64 devices in a mesh: dp: 4 (over x, y), sp: 16 (over z, core).
Axes of the slice: x: 2, y: 2, z: 8, core: 2. Of those that a mesh axis runs over, the one named last changes fastest.
The devices are a block of a 4x4x8 slice.
Arguments:
- x_in: bfloat16 [4, 2048, 1024], P('dp', 'sp'), parts along dimension 0
- grad_y: bfloat16 [4, 2048, 1024], P('dp', 'sp'), parts along dimension 0
- positions: int32 [8192], P(('dp', 'sp')), parts along dimension 0
- w_q: bfloat16 [1024, 2048], replicated
- w_k: bfloat16 [1024, 1024], replicated
- w_v: bfloat16 [1024, 1024], replicated
- w_o: bfloat16 [2048, 1024], replicated
- w_gate: bfloat16 [1024, 3072], replicated
- w_up: bfloat16 [1024, 3072], replicated
- w_down: bfloat16 [3072, 1024], replicated
- norm_gain: float32 [1024], replicated
- q_norm: float32 [16, 128], replicated
- k_norm: float32 [8, 128], replicated
Outputs:
- output 1: bfloat16 [4, 2048, 1024], P('dp', 'sp'), parts along dimension 0
- output 2: bfloat16 [4, 2048, 1024], P('dp', 'sp'), parts along dimension 0
- output 3: bfloat16 [4096, 2048], P('dp'), parts along dimension 0
- output 4: bfloat16 [4096, 1024], P('dp'), parts along dimension 0
- output 5: bfloat16 [4096, 1024], P('dp'), parts along dimension 0
- output 6: bfloat16 [8192, 1024], P('dp'), parts along dimension 0
- output 7: bfloat16 [4096, 3072], P('dp'), parts along dimension 0
- output 8: bfloat16 [4096, 3072], P('dp'), parts along dimension 0
- output 9: bfloat16 [12288, 1024], P('dp'), parts along dimension 0
- output 10: float32 [4096], P('dp'), parts along dimension 0
- output 11: float32 [64, 128], P('dp'), parts along dimension 0
- output 12: float32 [32, 128], P('dp'), parts along dimension 0
There are 4 independent parts. The reference program is written for one: setup_inputs(seed, part) draws one part's arguments, and reference() takes and returns one part's arrays. A program takes and returns all parts, laid end to end along the dimension named above; an argument that names none is the same for every part.
All inputs are finite; a program needn't handle non-finite values.
Results may differ from the reference program's by a relative error of at most 0.02.
Values are sent between devices in bfloat16 or wider.
A program may use at most 768 MiB of HBM per device.

```python
import jax
import jax.numpy as jnp
from jax import lax

BATCH_SIZE = 1
SEQ_LEN = 2048
MODEL_DIM = 1024
FFN_DIM = 3072
NUM_HEADS = 16
NUM_KV = 8
HEAD_DIM = 128

NORM_EPS = 1e-5
ROPE_THETA = 75.0e6


def setup_inputs(seed: int = 0, part: int = 0) -> dict:
    root_key = jax.random.key(seed)
    part_keys = jax.random.split(jax.random.fold_in(root_key, part), 4)
    weight_keys = jax.random.split(root_key, 10)
    q_width = NUM_HEADS * HEAD_DIM
    kv_width = NUM_KV * HEAD_DIM
    act_shape = (BATCH_SIZE, SEQ_LEN, MODEL_DIM)
    pos_steps = jax.random.randint(part_keys[2], (SEQ_LEN,), 1, 3)
    offset = jax.random.randint(part_keys[3], (), 0, SEQ_LEN)

    def normal_weight(slot_index, num_rows, num_cols, fan_in):
        raw_draw = jax.random.normal(weight_keys[slot_index], (num_rows, num_cols), jnp.float32)
        return (raw_draw * fan_in ** -0.5).astype(jnp.bfloat16)

    return {
        'x_in': jax.random.normal(part_keys[0], act_shape, jnp.float32).astype(jnp.bfloat16),
        'grad_y': jax.random.normal(part_keys[1], act_shape, jnp.float32).astype(jnp.bfloat16),
        'positions': (offset + jnp.cumsum(pos_steps) - pos_steps[0]).astype(jnp.int32),
        'w_q': normal_weight(0, MODEL_DIM, q_width, MODEL_DIM),
        'w_k': normal_weight(1, MODEL_DIM, kv_width, MODEL_DIM),
        'w_v': normal_weight(2, MODEL_DIM, kv_width, MODEL_DIM),
        'w_o': normal_weight(3, q_width, MODEL_DIM, q_width),
        'w_gate': normal_weight(4, MODEL_DIM, FFN_DIM, MODEL_DIM),
        'w_up': normal_weight(5, MODEL_DIM, FFN_DIM, MODEL_DIM),
        'w_down': normal_weight(6, FFN_DIM, MODEL_DIM, FFN_DIM),
        'norm_gain': jax.random.uniform(weight_keys[7], (MODEL_DIM,), jnp.float32, 0.5, 1.5),
        'q_norm': jax.random.uniform(weight_keys[8], (NUM_HEADS, HEAD_DIM), jnp.float32, 0.5, 2.0),
        'k_norm': jax.random.uniform(weight_keys[9], (NUM_KV, HEAD_DIM), jnp.float32, 0.5, 2.0),
    }


def input_norm(x_f32, norm_gain):
    row_mean = jnp.mean(x_f32, axis=-1, keepdims=True)
    centered = x_f32 - row_mean
    row_var = jnp.mean(centered * centered, axis=-1, keepdims=True)
    return (centered * lax.rsqrt(row_var + NORM_EPS) * norm_gain).astype(jnp.bfloat16)


def rope_tables(positions):
    inv_freq = ROPE_THETA ** (-(jnp.arange(HEAD_DIM // 2, dtype=jnp.float32) * 2.0) / HEAD_DIM)
    angles = positions.astype(jnp.float32)[:, None] * inv_freq[None, :]
    return jnp.cos(angles), jnp.sin(angles)


def head_prepare(proj_in, norm_weight, cos_t, sin_t):
    proj_f32 = proj_in.astype(jnp.float32)
    row_mean = jnp.mean(proj_f32, axis=-1, keepdims=True)
    centered = proj_f32 - row_mean
    row_var = jnp.mean(centered * centered, axis=-1, keepdims=True)
    normed = centered * lax.rsqrt(row_var + NORM_EPS) * norm_weight
    pair_view = normed.reshape(normed.shape[:-1] + (normed.shape[-1] // 2, 2))
    even_part = pair_view[..., 0]
    odd_part = pair_view[..., 1]
    cos_rows = cos_t[:, None, :]
    sin_rows = sin_t[:, None, :]
    rotated = jnp.stack([even_part * cos_rows - odd_part * sin_rows, even_part * sin_rows + odd_part * cos_rows], axis=-1)
    return rotated.reshape(normed.shape).astype(jnp.bfloat16)


def head_attention(operands):
    q_head, k_head, v_head = operands
    scores = jnp.einsum('bqd,bsd->bqs', q_head.astype(jnp.float32), k_head.astype(jnp.float32)) * HEAD_DIM ** -0.5
    causal = jnp.arange(SEQ_LEN)[:, None] >= jnp.arange(SEQ_LEN)[None, :]
    attn_probs = jax.nn.softmax(jnp.where(causal, scores, -1e30), axis=-1).astype(jnp.bfloat16)
    attended = jnp.einsum('bqs,bsd->bqd', attn_probs.astype(jnp.float32), v_head.astype(jnp.float32))
    return attended.astype(jnp.bfloat16)


def layer_forward(x_in, positions, weights):
    w_q, w_k, w_v, w_o, w_gate, w_up, w_down, norm_gain, q_norm, k_norm = weights
    tokens = BATCH_SIZE * SEQ_LEN
    head_shape = (BATCH_SIZE, SEQ_LEN, NUM_HEADS, HEAD_DIM)
    kv_shape = (BATCH_SIZE, SEQ_LEN, NUM_KV, HEAD_DIM)
    x_f32 = x_in.astype(jnp.float32)
    normed = input_norm(x_f32, norm_gain).reshape(tokens, MODEL_DIM)
    q_proj = jnp.dot(normed, w_q, preferred_element_type=jnp.float32).astype(jnp.bfloat16).reshape(head_shape)
    k_proj = jnp.dot(normed, w_k, preferred_element_type=jnp.float32).astype(jnp.bfloat16).reshape(kv_shape)
    v_proj = jnp.dot(normed, w_v, preferred_element_type=jnp.float32).astype(jnp.bfloat16).reshape(kv_shape)
    cos_t, sin_t = rope_tables(positions)
    q_rot = head_prepare(q_proj, q_norm, cos_t, sin_t)
    k_rot = head_prepare(k_proj, k_norm, cos_t, sin_t)
    group_size = NUM_HEADS // NUM_KV
    q_major = jnp.moveaxis(q_rot, 2, 0)
    k_major = jnp.repeat(jnp.moveaxis(k_rot, 2, 0), group_size, axis=0)
    v_major = jnp.repeat(jnp.moveaxis(v_proj, 2, 0), group_size, axis=0)
    attended = lax.map(jax.checkpoint(head_attention), (q_major, k_major, v_major))
    attn_flat = jnp.moveaxis(attended, 0, 2).reshape(tokens, NUM_HEADS * HEAD_DIM)
    attn_out = jnp.dot(attn_flat, w_o, preferred_element_type=jnp.float32).astype(jnp.bfloat16)
    gate_pre = jnp.dot(normed, w_gate, preferred_element_type=jnp.float32)
    up_proj = jnp.dot(normed, w_up, preferred_element_type=jnp.float32)
    hidden = (jax.nn.silu(gate_pre) * up_proj).astype(jnp.bfloat16)
    mlp_out = jnp.dot(hidden, w_down, preferred_element_type=jnp.float32).astype(jnp.bfloat16)
    summed = x_f32 + attn_out.astype(jnp.float32).reshape(x_in.shape) + mlp_out.astype(jnp.float32).reshape(x_in.shape)
    return summed.astype(jnp.bfloat16)


def reference(x_in, grad_y, positions, w_q, w_k, w_v, w_o, w_gate, w_up, w_down, norm_gain, q_norm, k_norm):
    weights = (w_q, w_k, w_v, w_o, w_gate, w_up, w_down, norm_gain, q_norm, k_norm)
    y_out, layer_back = jax.vjp(lambda x_arg, w_arg: layer_forward(x_arg, positions, w_arg), x_in, weights)
    grad_x, weight_grads = layer_back(grad_y)
    return (y_out, grad_x, weight_grads[0], weight_grads[1], weight_grads[2], weight_grads[3], weight_grads[4], weight_grads[5], weight_grads[6], weight_grads[7], weight_grads[8], weight_grads[9])
```

```python
import functools

import jax
import jax.numpy as jnp
from jax import lax
from jax.experimental import pallas as pl
from jax.experimental.pallas import tpu as pltpu
from jax.sharding import PartitionSpec as P

NORM_EPS = 1e-5
ROPE_THETA = 75.0e6
VMEM_LIMIT = 60 * 1024 * 1024
F32 = jnp.float32
BF16 = jnp.bfloat16


def input_norm(x_f32, norm_gain):
    row_mean = jnp.mean(x_f32, axis=-1, keepdims=True)
    centered = x_f32 - row_mean
    row_var = jnp.mean(centered * centered, axis=-1, keepdims=True)
    return (centered * lax.rsqrt(row_var + NORM_EPS) * norm_gain).astype(BF16)


def swiglu(gate_pre, up_proj):
    return (jax.nn.silu(gate_pre) * up_proj).astype(BF16)


def times_transposed(lhs_mat, rhs_mat):
    return lax.dot_general(lhs_mat, rhs_mat, (((1,), (1,)), ((), ())), preferred_element_type=F32)


def transposed_times(lhs_mat, rhs_mat):
    return lax.dot_general(lhs_mat, rhs_mat, (((0,), (0,)), ((), ())), preferred_element_type=F32)


def rope_lanes(positions, head_dim):
    pair_index = jnp.arange(head_dim, dtype=jnp.int32) // 2
    inv_freq = ROPE_THETA ** (-(pair_index.astype(F32) * 2.0) / head_dim)
    angles = positions.astype(F32)[:, None] * inv_freq[None, :]
    sign = jnp.where(jnp.arange(head_dim) % 2 == 0, -1.0, 1.0).astype(F32)
    return jnp.cos(angles), jnp.sin(angles) * sign[None, :]


def swap_pairs(rows):
    lane = lax.broadcasted_iota(jnp.int32, rows.shape, 1)
    width = rows.shape[1]
    return jnp.where(lane % 2 == 0, pltpu.roll(rows, width - 1, 1), pltpu.roll(rows, 1, 1))


def head_stats(proj_f32):
    row_mean = jnp.mean(proj_f32, axis=-1, keepdims=True)
    centered = proj_f32 - row_mean
    inv_std = lax.rsqrt(jnp.mean(centered * centered, axis=-1, keepdims=True) + NORM_EPS)
    return centered * inv_std, inv_std


def head_forward(proj_f32, weight, cos_t, sin_t):
    unit, _ = head_stats(proj_f32)
    normed = unit * weight
    return (normed * cos_t + swap_pairs(normed) * sin_t).astype(BF16)


def head_backward(d_rot, proj_f32, weight, cos_t, sin_t):
    unit, inv_std = head_stats(proj_f32)
    d_normed = d_rot * cos_t + swap_pairs(d_rot * sin_t)
    d_weight = jnp.sum(d_normed * unit, axis=0, keepdims=True)
    d_unit = d_normed * weight
    mean_d = jnp.mean(d_unit, axis=-1, keepdims=True)
    mean_du = jnp.mean(d_unit * unit, axis=-1, keepdims=True)
    return inv_std * (d_unit - mean_d - unit * mean_du), d_weight


def attention_kernel(block, idx_ref, n_ref, dy_ref, wq_ref, wk_ref, wv_ref, wo_ref, qn_ref, kn_ref, cos_ref, sin_ref,
                     o_ref, dq_ref, send_ref, keep_ref, kproj_ref, dwq_ref, dwo_ref, gq_ref,
                     q_s, k_s, v_s, do_s, qp_s, e_s, dk_s, dv_s, gq_s):
    seq_len, head_dim = o_ref.shape
    steps = seq_len // block
    scale = head_dim ** -0.5

    def project(i, carry):
        rows = pl.ds(pl.multiple_of(i * block, block), block)
        n_rows = n_ref[rows, :]
        q_proj = jnp.dot(n_rows, wq_ref[...], preferred_element_type=F32).astype(BF16)
        k_proj = jnp.dot(n_rows, wk_ref[...], preferred_element_type=F32).astype(BF16)
        qp_s[rows, :] = q_proj
        kproj_ref[rows, :] = k_proj
        v_s[rows, :] = jnp.dot(n_rows, wv_ref[...], preferred_element_type=F32).astype(BF16)
        do_s[rows, :] = times_transposed(dy_ref[rows, :], wo_ref[...]).astype(BF16)
        cos_t, sin_t = cos_ref[rows, :], sin_ref[rows, :]
        q_s[rows, :] = head_forward(q_proj.astype(F32), qn_ref[0], cos_t, sin_t)
        k_s[rows, :] = head_forward(k_proj.astype(F32), kn_ref[0], cos_t, sin_t)
        dk_s[rows, :] = jnp.zeros((block, head_dim), F32)
        dv_s[rows, :] = jnp.zeros((block, head_dim), F32)
        return carry

    lax.fori_loop(0, steps, project, 0)
    gq_s[...] = jnp.zeros_like(gq_s)
    causal = lax.broadcasted_iota(jnp.int32, (block, block), 0) >= lax.broadcasted_iota(jnp.int32, (block, block), 1)

    def lanes_max(tile):
        parts = [tile[:, c:c + 128] for c in range(0, block, 128)]
        return functools.reduce(jnp.maximum, parts)

    def lanes_sum(tile):
        parts = [tile[:, c:c + 128] for c in range(0, block, 128)]
        return functools.reduce(jnp.add, parts)

    def query_block(i, carry):
        rows = pl.ds(pl.multiple_of(i * block, block), block)
        q_rows, do_rows = q_s[rows, :], do_s[rows, :]

        def keys_of(j):
            return pl.ds(pl.multiple_of(j * block, block), block)

        def score(j, top):
            tile = times_transposed(q_rows, k_s[keys_of(j), :])
            e_s[:, keys_of(j)] = tile
            return jnp.maximum(top, lanes_max(tile))

        top = lax.fori_loop(0, i, score, jnp.full((block, 128), -1e30, F32))
        diag = jnp.where(causal, times_transposed(q_rows, k_s[rows, :]), -1e30)
        e_s[:, rows] = diag
        top = jnp.max(jnp.maximum(top, lanes_max(diag)), axis=-1, keepdims=True)

        def exponent(j, total):
            tile = jnp.exp((e_s[:, keys_of(j)] - top) * scale)
            e_s[:, keys_of(j)] = tile
            return total + lanes_sum(tile)

        total = lax.fori_loop(0, i + 1, exponent, jnp.zeros((block, 128), F32))
        inv_total = 1.0 / jnp.sum(total, axis=-1, keepdims=True)

        def attend(j, acc):
            probs = e_s[:, keys_of(j)] * inv_total
            e_s[:, keys_of(j)] = probs
            probs = probs.astype(BF16)
            dv_s[keys_of(j), :] += transposed_times(probs, do_rows)
            return acc + jnp.dot(probs, v_s[keys_of(j), :], preferred_element_type=F32)

        out = lax.fori_loop(0, i + 1, attend, jnp.zeros((block, head_dim), F32))
        o_ref[rows, :] = out.astype(BF16)
        delta = jnp.sum(out * do_rows.astype(F32), axis=-1, keepdims=True)

        def back(j, acc):
            d_probs = times_transposed(do_rows, v_s[keys_of(j), :]).astype(BF16).astype(F32)
            d_score = (e_s[:, keys_of(j)] * (d_probs - delta) * scale).astype(BF16)
            dk_s[keys_of(j), :] += transposed_times(d_score, q_rows)
            return acc + jnp.dot(d_score, k_s[keys_of(j), :], preferred_element_type=F32)

        dq = lax.fori_loop(0, i + 1, back, jnp.zeros((block, head_dim), F32)).astype(BF16).astype(F32)
        dq_proj, d_weight = head_backward(dq, qp_s[rows, :].astype(F32), qn_ref[0], cos_ref[rows, :], sin_ref[rows, :])
        dq_ref[rows, :] = dq_proj.astype(BF16)
        gq_s[...] += d_weight
        return carry

    lax.fori_loop(0, steps, query_block, 0)
    gq_ref[...] = gq_s[...]
    first = idx_ref[2] == 0
    dk_all, dv_all = dk_s[...].astype(BF16), dv_s[...].astype(BF16)

    @pl.when(first)
    def _():
        keep_ref[...] = dk_all
        send_ref[...] = dv_all

    @pl.when(jnp.logical_not(first))
    def _():
        keep_ref[...] = dv_all
        send_ref[...] = dk_all

    dwq_ref[...] = transposed_times(n_ref[...], dq_ref[...]).astype(BF16)
    dwo_ref[...] = transposed_times(o_ref[...], dy_ref[...]).astype(BF16)


def key_value_kernel(idx_ref, keep_ref, got_ref, kproj_ref, n_ref, kn_ref, cos_ref, sin_ref, dkv_ref, dwkv_ref, gk_ref):
    total = (keep_ref[...].astype(F32) + got_ref[...].astype(F32)).astype(BF16)
    first = idx_ref[2] == 0

    @pl.when(first)
    def _():
        dk_proj, d_weight = head_backward(total.astype(F32), kproj_ref[...].astype(F32), kn_ref[0], cos_ref[...], sin_ref[...])
        dkv_ref[...] = dk_proj.astype(BF16)
        gk_ref[...] = d_weight

    @pl.when(jnp.logical_not(first))
    def _():
        dkv_ref[...] = total
        gk_ref[...] = jnp.zeros_like(gk_ref)

    dwkv_ref[...] = transposed_times(n_ref[...], dkv_ref[...]).astype(BF16)


def mlp_kernel(chunk, idx_ref, n_ref, dy_ref, wg_ref, wu_ref, wd_ref,
               fg_ref, fu_ref, fd_ref, hg_ref, hu_ref, hd_ref, nt_s, hid_s, dg_s, du_s):
    seq_len = n_ref.shape[0]

    @pl.when(pl.program_id(0) == 0)
    def _():
        def turn(i, carry):
            rows = pl.ds(pl.multiple_of(i * chunk, chunk), chunk)
            nt_s[:, rows] = n_ref[rows, :].T
            return carry
        lax.fori_loop(0, seq_len // chunk, turn, 0)

    def forward(i, carry):
        rows = pl.ds(pl.multiple_of(i * chunk, chunk), chunk)
        n_rows, dy_rows = n_ref[rows, :], dy_ref[rows, :]
        gate = jnp.dot(n_rows, wg_ref[...], preferred_element_type=F32)
        up = jnp.dot(n_rows, wu_ref[...], preferred_element_type=F32)
        d_hidden = times_transposed(dy_rows, wd_ref[...]).astype(BF16).astype(F32)
        sig = jax.nn.sigmoid(gate)
        silu = gate * sig
        hid_s[rows, :] = (silu * up).astype(BF16)
        du_s[rows, :] = (d_hidden * silu).astype(BF16)
        dg_s[rows, :] = (d_hidden * up * (sig * (1.0 + gate * (1.0 - sig)))).astype(BF16)
        return carry

    lax.fori_loop(0, seq_len // chunk, forward, 0)

    rows_out = nt_s.shape[0]
    piece = rows_out // 4

    def weights(i, carry):
        rows = pl.ds(pl.multiple_of(i * piece, piece), piece)
        nt_rows = nt_s[rows, :]
        d_gate = jnp.dot(nt_rows, dg_s[...], preferred_element_type=F32).astype(BF16)
        d_up = jnp.dot(nt_rows, du_s[...], preferred_element_type=F32).astype(BF16)
        fg_ref[rows, :] = d_gate
        hg_ref[rows, :] = d_gate
        fu_ref[rows, :] = d_up
        hu_ref[rows, :] = d_up
        return carry

    lax.fori_loop(0, 4, weights, 0)
    d_down = transposed_times(hid_s[...], dy_ref[...]).astype(BF16)
    fd_ref[...] = d_down
    hd_ref[...] = d_down


def fill_kernel(idx_ref, hg_ref, hu_ref, hd_ref, ag_ref, au_ref, ad_ref, fg_ref, fu_ref, fd_ref):
    fg_ref[...] = hg_ref[...]
    fu_ref[...] = hu_ref[...]
    fd_ref[...] = hd_ref[...]


def whole(shape):
    return pl.BlockSpec(shape, lambda *_: (0,) * len(shape))


def solution(mesh):
    group_devices = mesh.shape['sp']
    seq_spec = P('dp', 'sp', None)
    grad_spec = P('dp', None)
    pair_swap = [(i, i ^ 1) for i in range(group_devices)]

    def layer_step(x_in, grad_y, positions, w_q, w_k, w_v, w_o, w_gate, w_up, w_down, norm_gain, q_norm, k_norm):
        batch_rows, local_len, model_dim = x_in.shape
        num_heads, head_dim = q_norm.shape
        num_kv = k_norm.shape[0]
        share = num_heads // num_kv
        ffn_dim = w_gate.shape[1]
        seq_len = local_len * group_devices
        me = lax.axis_index('sp')
        core = me % 2
        idx = jnp.stack([me, me // share, core]).astype(jnp.int32)

        all_pos = lax.all_gather(positions, 'sp', axis=0, tiled=True)
        x_f32 = x_in.reshape(local_len, model_dim).astype(F32)
        flat_norm, norm_back = jax.vjp(input_norm, x_f32, norm_gain)
        grad_flat = grad_y.reshape(local_len, model_dim)
        n_all = lax.all_gather(flat_norm, 'sp', axis=0, tiled=True)
        dy_all = lax.all_gather(grad_flat, 'sp', axis=0, tiled=True)
        cos_t, sin_t = rope_lanes(all_pos, head_dim)

        gate_pre = jnp.dot(flat_norm, w_gate, preferred_element_type=F32)
        up_proj = jnp.dot(flat_norm, w_up, preferred_element_type=F32)
        hidden, act_back = jax.vjp(swiglu, gate_pre, up_proj)
        mlp_out = jnp.dot(hidden, w_down, preferred_element_type=F32).astype(BF16)
        d_hidden = times_transposed(grad_flat, w_down).astype(BF16)
        d_gate, d_up = act_back(d_hidden)
        d_norm_mlp = times_transposed(d_gate.astype(BF16), w_gate) + times_transposed(d_up.astype(BF16), w_up)

        vec = jax.ShapeDtypeStruct((1, head_dim), F32)
        rows_bf = jax.ShapeDtypeStruct((seq_len, head_dim), BF16)
        block = 512
        qn3 = q_norm.reshape(num_heads, 1, head_dim)
        kn3 = k_norm.reshape(num_kv, 1, head_dim)
        o_h, dq_h, send, keep, k_proj, dwq_h, dwo_h, gq = pl.pallas_call(
            functools.partial(attention_kernel, block),
            out_shape=[rows_bf, rows_bf, rows_bf, rows_bf, rows_bf,
                       jax.ShapeDtypeStruct((model_dim, head_dim), BF16), jax.ShapeDtypeStruct((head_dim, model_dim), BF16), vec],
            grid_spec=pltpu.PrefetchScalarGridSpec(
                num_scalar_prefetch=1, grid=(1,),
                in_specs=[whole((seq_len, model_dim)), whole((seq_len, model_dim)),
                          pl.BlockSpec((model_dim, head_dim), lambda g, s: (0, s[0])),
                          pl.BlockSpec((model_dim, head_dim), lambda g, s: (0, s[1])),
                          pl.BlockSpec((model_dim, head_dim), lambda g, s: (0, s[1])),
                          pl.BlockSpec((head_dim, model_dim), lambda g, s: (s[0], 0)),
                          pl.BlockSpec((1, 1, head_dim), lambda g, s: (s[0], 0, 0)),
                          pl.BlockSpec((1, 1, head_dim), lambda g, s: (s[1], 0, 0)),
                          whole((seq_len, head_dim)), whole((seq_len, head_dim))],
                out_specs=[whole((seq_len, head_dim))] * 5 + [whole((model_dim, head_dim)), whole((head_dim, model_dim)), whole((1, head_dim))],
                scratch_shapes=[pltpu.VMEM((seq_len, head_dim), BF16)] * 5
                + [pltpu.VMEM((block, seq_len), F32), pltpu.VMEM((seq_len, head_dim), F32), pltpu.VMEM((seq_len, head_dim), F32),
                   pltpu.VMEM((1, head_dim), F32)]),
            compiler_params=pltpu.CompilerParams(vmem_limit_bytes=VMEM_LIMIT),
            cost_estimate=pl.CostEstimate(flops=20_000_000_000, bytes_accessed=20_000_000, transcendentals=0),
            name="attention",
        )(idx, n_all, dy_all, w_q, w_k, w_v, w_o, qn3, kn3, cos_t, sin_t)

        got = lax.ppermute(send, 'sp', pair_swap)
        dkv_h, dwkv_h, gk = pl.pallas_call(
            key_value_kernel,
            out_shape=[rows_bf, jax.ShapeDtypeStruct((model_dim, head_dim), BF16), vec],
            grid_spec=pltpu.PrefetchScalarGridSpec(
                num_scalar_prefetch=1, grid=(1,),
                in_specs=[whole((seq_len, head_dim))] * 3 + [whole((seq_len, model_dim)),
                          pl.BlockSpec((1, 1, head_dim), lambda g, s: (s[1], 0, 0)),
                          whole((seq_len, head_dim)), whole((seq_len, head_dim))],
                out_specs=[whole((seq_len, head_dim)), whole((model_dim, head_dim)), whole((1, head_dim))]),
            compiler_params=pltpu.CompilerParams(vmem_limit_bytes=VMEM_LIMIT),
            cost_estimate=pl.CostEstimate(flops=5_000_000_000, bytes_accessed=8_000_000, transcendentals=0),
            name="key_value",
        )(idx, keep, got, k_proj, n_all, kn3, cos_t, sin_t)

        dwo_all = lax.all_gather(dwo_h, 'sp', axis=0, tiled=True)
        dwq_all = lax.all_gather(dwq_h, 'sp', axis=0)
        dwkv_all = lax.all_gather(dwkv_h, 'sp', axis=0)

        tile = 256
        half = ffn_dim // 2
        tiles = half // tile
        full_in = jax.ShapeDtypeStruct((model_dim, ffn_dim), BF16)
        full_out = jax.ShapeDtypeStruct((ffn_dim, model_dim), BF16)
        half_in = jax.ShapeDtypeStruct((model_dim, half), BF16)
        half_out = jax.ShapeDtypeStruct((half, model_dim), BF16)
        col_here = pl.BlockSpec((model_dim, tile), lambda i, s: (0, s[2] * tiles + i))
        row_here = pl.BlockSpec((tile, model_dim), lambda i, s: (s[2] * tiles + i, 0))
        col_half = pl.BlockSpec((model_dim, tile), lambda i, s: (0, i))
        row_half = pl.BlockSpec((tile, model_dim), lambda i, s: (i, 0))
        part_g, part_u, part_d, half_g, half_u, half_d = pl.pallas_call(
            functools.partial(mlp_kernel, 256),
            out_shape=[full_in, full_in, full_out, half_in, half_in, half_out],
            grid_spec=pltpu.PrefetchScalarGridSpec(
                num_scalar_prefetch=1, grid=(tiles,),
                in_specs=[whole((seq_len, model_dim)), whole((seq_len, model_dim)), col_here, col_here, row_here],
                out_specs=[col_here, col_here, row_here, col_half, col_half, row_half],
                scratch_shapes=[pltpu.VMEM((model_dim, seq_len), BF16)] + [pltpu.VMEM((seq_len, tile), BF16)] * 3),
            compiler_params=pltpu.CompilerParams(vmem_limit_bytes=VMEM_LIMIT),
            cost_estimate=pl.CostEstimate(flops=12 * seq_len * model_dim * half, bytes_accessed=40_000_000, transcendentals=0),
            name="mlp",
        )(idx, n_all, dy_all, w_gate, w_up, w_down)
        got_g = lax.ppermute(half_g, 'sp', pair_swap)
        got_u = lax.ppermute(half_u, 'sp', pair_swap)
        got_d = lax.ppermute(half_d, 'sp', pair_swap)
        col_there = pl.BlockSpec((model_dim, tile), lambda i, s: (0, (1 - s[2]) * tiles + i))
        row_there = pl.BlockSpec((tile, model_dim), lambda i, s: ((1 - s[2]) * tiles + i, 0))
        hbm = pl.BlockSpec(memory_space=pl.ANY)
        dw_gate, dw_up, dw_down = pl.pallas_call(
            fill_kernel,
            out_shape=[full_in, full_in, full_out],
            grid_spec=pltpu.PrefetchScalarGridSpec(
                num_scalar_prefetch=1, grid=(tiles,),
                in_specs=[col_half, col_half, row_half, hbm, hbm, hbm],
                out_specs=[col_there, col_there, row_there]),
            input_output_aliases={4: 0, 5: 1, 6: 2},
            cost_estimate=pl.CostEstimate(flops=1_000_000_000, bytes_accessed=20_000_000, transcendentals=0),
            name="fill",
        )(idx, got_g, got_u, got_d, part_g, part_u, part_d)

        attn_flat = lax.all_to_all(o_h, 'sp', 0, 1, tiled=True)
        attn_out = jnp.dot(attn_flat, w_o, preferred_element_type=F32).astype(BF16)
        y_out = (x_f32 + attn_out.astype(F32) + mlp_out.astype(F32)).astype(BF16)

        d_rows = lax.all_to_all(jnp.concatenate([dq_h, dkv_h], axis=1), 'sp', 0, 1, tiled=True)
        d_rows = d_rows.reshape(local_len, num_kv, share, 2, head_dim)
        dq_flat = d_rows[:, :, :, 0].reshape(local_len, num_heads * head_dim)
        dk_flat = d_rows[:, :, 0, 1].reshape(local_len, num_kv * head_dim)
        dv_flat = d_rows[:, :, 1, 1].reshape(local_len, num_kv * head_dim)
        d_norm = (times_transposed(dq_flat, w_q) + times_transposed(dk_flat, w_k) + times_transposed(dv_flat, w_v) + d_norm_mlp).astype(BF16)
        dx_norm, grad_gain = norm_back(d_norm)
        grad_x = (grad_flat.astype(F32) + dx_norm).astype(BF16)

        small = jnp.concatenate([grad_gain.reshape(-1, head_dim), gq, gk], axis=0)
        small_all = lax.all_gather(small, 'sp', axis=0)
        gain_rows = model_dim // head_dim
        grad_gain = jnp.sum(small_all[:, :gain_rows], axis=0).reshape(model_dim)
        grad_q_norm = small_all[:, gain_rows]
        grad_k_norm = small_all[::share, gain_rows + 1]

        dw_q = dwq_all.transpose(1, 0, 2).reshape(model_dim, num_heads * head_dim)
        dwkv = dwkv_all.reshape(num_kv, share, model_dim, head_dim)
        dw_k = dwkv[:, 0].transpose(1, 0, 2).reshape(model_dim, num_kv * head_dim)
        dw_v = dwkv[:, 1].transpose(1, 0, 2).reshape(model_dim, num_kv * head_dim)
        return (y_out.reshape(x_in.shape), grad_x.reshape(x_in.shape), dw_q, dw_k, dw_v, dwo_all, dw_gate, dw_up, dw_down,
                grad_gain, grad_q_norm, grad_k_norm)

    in_specs = (seq_spec, seq_spec, P(('dp', 'sp'))) + (P(),) * 10
    out_specs = (seq_spec, seq_spec) + (grad_spec,) * 7 + (P('dp'), grad_spec, grad_spec)
    return jax.shard_map(layer_step, mesh=mesh, in_specs=in_specs, out_specs=out_specs, check_vma=False)
```

```python
import functools

import jax
import jax.numpy as jnp
from jax import lax
from jax.experimental import pallas as pl
from jax.experimental.pallas import tpu as pltpu
from jax.sharding import PartitionSpec as P

NORM_EPS = 1e-5
ROPE_THETA = 75.0e6
VMEM_LIMIT = 60 * 1024 * 1024
F32 = jnp.float32
BF16 = jnp.bfloat16
MESH = pl.DeviceIdType.MESH


def input_norm(x_f32, norm_gain):
    row_mean = jnp.mean(x_f32, axis=-1, keepdims=True)
    centered = x_f32 - row_mean
    row_var = jnp.mean(centered * centered, axis=-1, keepdims=True)
    return (centered * lax.rsqrt(row_var + NORM_EPS) * norm_gain).astype(BF16)


def swiglu(gate_pre, up_proj):
    return (jax.nn.silu(gate_pre) * up_proj).astype(BF16)


def times_transposed(lhs_mat, rhs_mat):
    return lax.dot_general(lhs_mat, rhs_mat, (((1,), (1,)), ((), ())), preferred_element_type=F32)


def transposed_times(lhs_mat, rhs_mat):
    return lax.dot_general(lhs_mat, rhs_mat, (((0,), (0,)), ((), ())), preferred_element_type=F32)


def rope_lanes(positions, head_dim):
    pair_index = jnp.arange(head_dim, dtype=jnp.int32) // 2
    inv_freq = ROPE_THETA ** (-(pair_index.astype(F32) * 2.0) / head_dim)
    angles = positions.astype(F32)[:, None] * inv_freq[None, :]
    sign = jnp.where(jnp.arange(head_dim) % 2 == 0, -1.0, 1.0).astype(F32)
    return jnp.cos(angles), jnp.sin(angles) * sign[None, :]


def swap_pairs(rows):
    lane = lax.broadcasted_iota(jnp.int32, rows.shape, 1)
    width = rows.shape[1]
    return jnp.where(lane % 2 == 0, pltpu.roll(rows, width - 1, 1), pltpu.roll(rows, 1, 1))


def head_stats(proj_f32):
    row_mean = jnp.mean(proj_f32, axis=-1, keepdims=True)
    centered = proj_f32 - row_mean
    inv_std = lax.rsqrt(jnp.mean(centered * centered, axis=-1, keepdims=True) + NORM_EPS)
    return centered * inv_std, inv_std


def head_forward(proj_f32, weight, cos_t, sin_t):
    unit, _ = head_stats(proj_f32)
    normed = unit * weight
    return (normed * cos_t + swap_pairs(normed) * sin_t).astype(BF16)


def head_backward(d_rot, proj_f32, weight, cos_t, sin_t):
    unit, inv_std = head_stats(proj_f32)
    d_normed = d_rot * cos_t + swap_pairs(d_rot * sin_t)
    d_weight = jnp.sum(d_normed * unit, axis=0, keepdims=True)
    d_unit = d_normed * weight
    mean_d = jnp.mean(d_unit, axis=-1, keepdims=True)
    mean_du = jnp.mean(d_unit * unit, axis=-1, keepdims=True)
    return inv_std * (d_unit - mean_d - unit * mean_du), d_weight


def forward_kernel(block, idx_ref, n_s, wq_ref, wk_ref, wv_ref, qn_ref, kn_ref, cos_ref, sin_ref,
                   o_ref, o32_ref, lse_ref, q_ref, k_ref, v_ref, qproj_ref, kproj_ref, e_s):
    seq_len, head_dim = o_ref.shape
    steps = seq_len // block
    scale = head_dim ** -0.5

    def project(i, carry):
        rows = pl.ds(pl.multiple_of(i * block, block), block)
        n_rows = n_s[rows, :]
        weights = jnp.concatenate([wq_ref[...], wk_ref[...], wv_ref[...]], axis=1)
        proj = jnp.dot(n_rows, weights, preferred_element_type=F32).astype(BF16)
        q_proj, k_proj = proj[:, :head_dim], proj[:, head_dim:2 * head_dim]
        qproj_ref[rows, :] = q_proj
        kproj_ref[rows, :] = k_proj
        v_ref[rows, :] = proj[:, 2 * head_dim:]
        cos_t, sin_t = cos_ref[rows, :], sin_ref[rows, :]
        q_ref[rows, :] = head_forward(q_proj.astype(F32), qn_ref[0], cos_t, sin_t)
        k_ref[rows, :] = head_forward(k_proj.astype(F32), kn_ref[0], cos_t, sin_t)
        return carry

    lax.fori_loop(0, steps, project, 0)
    causal = lax.broadcasted_iota(jnp.int32, (block, block), 0) >= lax.broadcasted_iota(jnp.int32, (block, block), 1)

    def lanes(op, tile):
        return functools.reduce(op, [tile[:, c:c + 128] for c in range(0, block, 128)])

    def keys_of(j):
        return pl.ds(pl.multiple_of(j * block, block), block)

    def query_block(i, carry):
        rows = keys_of(i)
        q_rows = q_ref[rows, :]

        def score(j, top):
            tile = times_transposed(q_rows, k_ref[keys_of(j), :])
            e_s[:, keys_of(j)] = tile
            return jnp.maximum(top, lanes(jnp.maximum, tile))

        top = lax.fori_loop(0, i, score, jnp.full((block, 128), -1e30, F32))
        diag = jnp.where(causal, times_transposed(q_rows, k_ref[rows, :]), -1e30)
        e_s[:, rows] = diag
        top = jnp.max(jnp.maximum(top, lanes(jnp.maximum, diag)), axis=-1, keepdims=True)

        def exponent(j, total):
            tile = jnp.exp((e_s[:, keys_of(j)] - top) * scale)
            e_s[:, keys_of(j)] = tile
            return total + lanes(jnp.add, tile)

        total = lax.fori_loop(0, i + 1, exponent, jnp.zeros((block, 128), F32))
        total = jnp.sum(total, axis=-1, keepdims=True)
        inv_total = 1.0 / total

        def attend(j, acc):
            probs = (e_s[:, keys_of(j)] * inv_total).astype(BF16)
            return acc + jnp.dot(probs, v_ref[keys_of(j), :], preferred_element_type=F32)

        out = lax.fori_loop(0, i + 1, attend, jnp.zeros((block, head_dim), F32))
        o_ref[rows, :] = out.astype(BF16)
        o32_ref[rows, :] = out
        lse_ref[rows, :] = jnp.broadcast_to(top * scale + jnp.log(total), (block, 128))
        return carry

    lax.fori_loop(0, steps, query_block, 0)


def output_grad_kernel(idx_ref, dy_s, wo_ref, o_ref, do_ref, dwo_ref):
    dwo_ref[...] = transposed_times(o_ref[...], dy_s[...]).astype(BF16)
    do_ref[...] = times_transposed(dy_s[...], wo_ref[...]).astype(BF16)


def backward_kernel(block, idx_ref, do_ref, o32_ref, lse_ref, q_ref, k_ref, v_ref, qproj_ref, qn_ref, cos_ref, sin_ref,
                    dq_ref, send_ref, keep_ref, gq_ref, dk_s, dv_s):
    seq_len, head_dim = do_ref.shape
    steps = seq_len // block
    scale = head_dim ** -0.5
    causal = lax.broadcasted_iota(jnp.int32, (block, block), 0) >= lax.broadcasted_iota(jnp.int32, (block, block), 1)
    dk_s[...] = jnp.zeros_like(dk_s)
    dv_s[...] = jnp.zeros_like(dv_s)
    gq_ref[...] = jnp.zeros_like(gq_ref)

    def query_block(i, carry):
        rows = pl.ds(pl.multiple_of(i * block, block), block)
        q_rows, do_rows = q_ref[rows, :], do_ref[rows, :]
        delta = jnp.sum(o32_ref[rows, :] * do_rows.astype(F32), axis=-1, keepdims=True)
        lse = lse_ref[rows, :][:, :1]

        def tile_back(keys, masked):
            k_rows, v_rows = k_ref[keys, :], v_ref[keys, :]
            probs = jnp.exp(times_transposed(q_rows, k_rows) * scale - lse)
            if masked:
                probs = jnp.where(causal, probs, 0.0)
            d_probs = times_transposed(do_rows, v_rows).astype(BF16).astype(F32)
            d_score = (probs * (d_probs - delta) * scale).astype(BF16)
            dv_s[keys, :] += transposed_times(probs.astype(BF16), do_rows)
            dk_s[keys, :] += transposed_times(d_score, q_rows)
            return jnp.dot(d_score, k_rows, preferred_element_type=F32)

        def back(j, acc):
            return acc + tile_back(pl.ds(pl.multiple_of(j * block, block), block), False)

        dq = lax.fori_loop(0, i, back, tile_back(rows, True)).astype(BF16).astype(F32)
        dq_proj, d_weight = head_backward(dq, qproj_ref[rows, :].astype(F32), qn_ref[0], cos_ref[rows, :], sin_ref[rows, :])
        dq_ref[rows, :] = dq_proj.astype(BF16)
        gq_ref[...] += d_weight
        return carry

    lax.fori_loop(0, steps, query_block, 0)
    first = idx_ref[2] == 0

    @pl.when(first)
    def _():
        keep_ref[...] = dk_s[...].astype(BF16)
        send_ref[...] = dv_s[...].astype(BF16)

    @pl.when(jnp.logical_not(first))
    def _():
        keep_ref[...] = dv_s[...].astype(BF16)
        send_ref[...] = dk_s[...].astype(BF16)


def projection_grad_kernel(idx_ref, n_s, dq_ref, keep_ref, got_ref, kproj_ref, kn_ref, cos_ref, sin_ref,
                           rows_ref, dw_ref, gk_ref):
    head_dim = dq_ref.shape[1]
    total = (keep_ref[...].astype(F32) + got_ref[...].astype(F32)).astype(BF16)
    rows_ref[:, :head_dim] = dq_ref[...]
    first = idx_ref[2] == 0

    @pl.when(first)
    def _():
        dk_proj, d_weight = head_backward(total.astype(F32), kproj_ref[...].astype(F32), kn_ref[0], cos_ref[...], sin_ref[...])
        rows_ref[:, head_dim:] = dk_proj.astype(BF16)
        gk_ref[...] = d_weight

    @pl.when(jnp.logical_not(first))
    def _():
        rows_ref[:, head_dim:] = total
        gk_ref[...] = jnp.zeros_like(gk_ref)

    dw_ref[...] = transposed_times(n_s[...], rows_ref[...]).astype(BF16)


class Ring:
    def __init__(self, devices):
        self.chips = devices // 2
        self.me = lax.axis_index('sp')
        self.z, self.core = self.me // 2, self.me % 2
        self.turn = 1 - 2 * self.core
        self.partner = self.me + self.turn
        self.after = self.device(self.z + self.turn, self.core)
        self.before = self.device(self.z - self.turn, self.core)

    def device(self, z, core):
        return 2 * lax.rem(z + 2 * self.chips, self.chips) + core

    def own_slot(self, step):
        return self.device(self.z - self.turn * step, self.core)

    def other_slot(self, step):
        return self.device(self.z + self.turn * step, 1 - self.core)

    def barrier(self):
        sem = pltpu.get_barrier_semaphore()
        for device in (self.after, self.before, self.partner):
            pl.semaphore_signal(sem, inc=1, device_id={'sp': device}, device_id_type=MESH)
        pl.semaphore_wait(sem, 3)

    def forward(self, buf, sems, lane, step):
        slot = buf.at[self.own_slot(step)]
        return pltpu.make_async_remote_copy(slot, slot, sems[0].at[lane, step], sems[1].at[lane, step + 1],
                                            device_id={'sp': self.after}, device_id_type=MESH)

    def share(self, buf, sems, lane, step):
        slot = buf.at[self.own_slot(step)]
        return pltpu.make_async_remote_copy(slot, slot, sems[2].at[lane, step], sems[3].at[lane, step],
                                            device_id={'sp': self.partner}, device_id_type=MESH)

    def arrived(self, buf, sems, lane, step):
        slot = buf.at[self.own_slot(step)]
        return pltpu.make_async_remote_copy(slot, slot, sems[0].at[lane, step], sems[1].at[lane, step],
                                            device_id={'sp': self.before}, device_id_type=MESH)

    def shared(self, buf, sems, lane, step):
        slot = buf.at[self.other_slot(step)]
        return pltpu.make_async_remote_copy(slot, slot, sems[2].at[lane, step], sems[3].at[lane, step],
                                            device_id={'sp': self.partner}, device_id_type=MESH)

    def take(self, buf, sems, lane, step):
        @pl.when(step > 0)
        def _():
            self.arrived(buf, sems, lane, step).wait_recv()

        @pl.when(step < self.chips - 1)
        def _():
            self.forward(buf, sems, lane, step).start()
        self.share(buf, sems, lane, step).start()
        self.shared(buf, sems, lane, step).wait_recv()

    def finish(self, buf, sems, lane):
        def body(step, carry):
            @pl.when(step < self.chips - 1)
            def _():
                self.forward(buf, sems, lane, step).wait_send()
            self.share(buf, sems, lane, step).wait_send()
            return carry
        lax.fori_loop(0, self.chips, body, 0)


def gather_kernel(devices, n_ref, dy_ref, pos_ref, wg_ref, wu_ref, wd_ref,
                  n_out, dy_out, pos_out, hid_out, dg_out, du_out, mlp_out, dn_out,
                  n_s, dy_s, pos_s, wg_s, wu_s, wd_s, hid_s, dg_s, du_s, gate_s, up_s, part_s, got_s,
                  load_sem, weight_sem, ring_send, ring_recv, pair_send, pair_recv, out_sem, act_sem, swap_send, swap_recv):
    ring = Ring(devices)
    sems = (ring_send, ring_recv, pair_send, pair_recv)
    half = wg_s.shape[1]
    lanes = ((pos_s, pos_ref, pos_out), (n_s, n_ref, n_out), (dy_s, dy_ref, dy_out))
    loads = [pltpu.make_async_copy(src, buf.at[ring.me], load_sem.at[i]) for i, (buf, src, _) in enumerate(lanes)]
    columns = pl.ds(pl.multiple_of(ring.core * half, half), half)
    weights = [pltpu.make_async_copy(wg_ref.at[:, columns], wg_s, weight_sem.at[0]),
               pltpu.make_async_copy(wu_ref.at[:, columns], wu_s, weight_sem.at[1]),
               pltpu.make_async_copy(wd_ref.at[columns, :], wd_s, weight_sem.at[2])]
    for copy in loads + weights:
        copy.start()
    ring.barrier()
    for copy in loads:
        copy.wait()

    tile = 512
    acts = ((hid_s, hid_out), (dg_s, dg_out), (du_s, du_out))

    def put(lane, slot):
        buf, _, out = lanes[lane]
        return pltpu.make_async_copy(buf.at[slot], out.at[slot], out_sem.at[lane, slot])

    def put_act(i, slot):
        return pltpu.make_async_copy(acts[i][0].at[slot], acts[i][1].at[slot], act_sem.at[i, slot])

    def step_body(step, carry):
        mine, other = ring.own_slot(step), ring.other_slot(step)
        ring.take(n_s, sems, 1, step)
        ring.take(pos_s, sems, 0, step)

        @pl.when(step == 0)
        def _():
            weights[0].wait()
            weights[1].wait()

        def gate_up(j, inner):
            cols = pl.ds(pl.multiple_of(j * tile, tile), tile)
            n_rows = jnp.concatenate([n_s[mine], n_s[other]], axis=0)
            gate_s[:, cols] = jnp.dot(n_rows, wg_s[:, cols], preferred_element_type=F32)
            up_s[:, cols] = jnp.dot(n_rows, wu_s[:, cols], preferred_element_type=F32)
            return inner
        lax.fori_loop(0, half // tile, gate_up, 0)
        ring.take(dy_s, sems, 2, step)
        for lane in range(3):
            put(lane, mine).start()
            put(lane, other).start()

        @pl.when(step == 0)
        def _():
            weights[2].wait()

        def hidden(j, inner):
            cols = pl.ds(pl.multiple_of(j * tile, tile), tile)
            dy_rows = jnp.concatenate([dy_s[mine], dy_s[other]], axis=0)
            d_hidden = times_transposed(dy_rows, wd_s[cols, :]).astype(BF16).astype(F32)
            gate, up = gate_s[:, cols], up_s[:, cols]
            sig = jax.nn.sigmoid(gate)
            silu = gate * sig
            hid = (silu * up).astype(BF16)
            d_up = (d_hidden * silu).astype(BF16)
            d_gate = (d_hidden * up * (sig * (1.0 + gate * (1.0 - sig)))).astype(BF16)
            rows = hid.shape[0] // 2
            for buf, value in ((hid_s, hid), (dg_s, d_gate), (du_s, d_up)):
                buf[mine, :, cols] = value[:rows]
                buf[other, :, cols] = value[rows:]
            return inner
        lax.fori_loop(0, half // tile, hidden, 0)

        @pl.when(step > 0)
        def _():
            for i in range(3):
                put_act(i, ring.own_slot(step - 1)).start()
                put_act(i, ring.other_slot(step - 1)).start()
        return carry

    lax.fori_loop(0, ring.chips, step_body, 0)
    last = ring.chips - 1
    for i in range(3):
        put_act(i, ring.own_slot(last)).start()
        put_act(i, ring.other_slot(last)).start()

    def partial(slot):
        return (jnp.dot(hid_s[slot], wd_s[...], preferred_element_type=F32),
                times_transposed(dg_s[slot], wg_s[...]) + times_transposed(du_s[slot], wu_s[...]))

    part_s[0], part_s[1] = partial(ring.partner)
    mine_m, mine_n = partial(ring.me)
    dn_out[...] = mine_n
    swap = pltpu.make_async_remote_copy(part_s, got_s, swap_send, swap_recv, device_id={'sp': ring.partner}, device_id_type=MESH)
    swap.start()
    for lane in range(3):
        ring.finish(lanes[lane][0], sems, lane)

    def drain(slot, carry):
        for lane in range(3):
            put(lane, slot).wait()
            put_act(lane, slot).wait()
        return carry
    lax.fori_loop(0, devices, drain, 0)
    swap.wait()
    mlp_out[...] = (mine_m + got_s[0]).astype(BF16)
    dn_out[...] += got_s[1]


def weight_kernel(devices, dwo_ref, dwqkv_ref, n_ref, dy_ref, hid_ref, dg_ref, du_ref,
                  q_out, k_out, v_out, o_out, g_out, u_out, d_out,
                  wo_s, wqkv_s, n_s, dy_s, nt_s, hid_s, dg_s, du_s, st_g, st_u, st_d,
                  load_sem, tile_sem, ring_send, ring_recv, pair_send, pair_recv, out_sem, kv_sem,
                  put_sem, swap_send, swap_recv):
    ring = Ring(devices)
    sems = (ring_send, ring_recv, pair_send, pair_recv)
    head_dim, model_dim = dwo_ref.shape
    half = hid_ref.shape[1]
    tile = st_g.shape[2]
    tiles = half // tile
    loads = [pltpu.make_async_copy(dwo_ref, wo_s.at[ring.me], load_sem.at[0]),
             pltpu.make_async_copy(dwqkv_ref, wqkv_s.at[ring.me], load_sem.at[1]),
             pltpu.make_async_copy(n_ref, n_s, load_sem.at[2]),
             pltpu.make_async_copy(dy_ref, dy_s, load_sem.at[3])]
    tile_bufs = ((hid_ref, hid_s), (dg_ref, dg_s), (du_ref, du_s))

    def fetch(i, t):
        cols = pl.ds(pl.multiple_of(t * tile, tile), tile)
        return pltpu.make_async_copy(tile_bufs[i][0].at[:, cols], tile_bufs[i][1].at[t % 2], tile_sem.at[i, t % 2])

    for copy in loads:
        copy.start()
    for i in range(3):
        fetch(i, 0).start()
    ring.barrier()
    loads[0].wait()
    loads[1].wait()

    def put_o(slot):
        rows = pl.ds(pl.multiple_of(slot * head_dim, head_dim), head_dim)
        return pltpu.make_async_copy(wo_s.at[slot], o_out.at[rows, :], out_sem.at[0, slot])

    def put_q(slot):
        cols = pl.ds(pl.multiple_of(slot * head_dim, head_dim), head_dim)
        return pltpu.make_async_copy(wqkv_s.at[slot, :, pl.ds(0, head_dim)], q_out.at[:, cols], out_sem.at[1, slot])

    def put_kv(slot, out):
        cols = pl.ds(pl.multiple_of(slot // 2 * head_dim, head_dim), head_dim)
        return pltpu.make_async_copy(wqkv_s.at[slot, :, pl.ds(head_dim, head_dim)], out.at[:, cols], kv_sem.at[slot])

    def store(t, i, core):
        st, out = ((st_g, g_out), (st_u, u_out), (st_d, d_out))[i]
        span = pl.ds(pl.multiple_of(core * half + t * tile, tile), tile)
        return st.at[t], (out.at[span, :] if i == 2 else out.at[:, span])

    def put_tile(t, i):
        src, dst = store(t, i, ring.core)
        return pltpu.make_async_copy(src, dst, put_sem.at[i, t])

    def send_tile(t, i, core):
        src, dst = store(t, i, core)
        return pltpu.make_async_remote_copy(src, dst, swap_send.at[i, t], swap_recv.at[i, t],
                                            device_id={'sp': ring.partner}, device_id_type=MESH)

    def step_body(step, carry):
        ring.take(wo_s, sems, 0, step)

        @pl.when(step == 0)
        def _():
            loads[2].wait()

            def turn(i, inner):
                rows = pl.ds(pl.multiple_of(i * 256, 256), 256)
                nt_s[:, rows] = n_s[rows, :].T
                return inner
            lax.fori_loop(0, n_s.shape[0] // 256, turn, 0)
            loads[3].wait()

        piece = model_dim // 4

        @pl.when(step < tiles)
        def _():
            for i in range(3):
                fetch(i, step).wait()

            @pl.when(step + 1 < tiles)
            def _():
                for i in range(3):
                    fetch(i, step + 1).start()

            def in_weights(i, inner):
                rows = pl.ds(pl.multiple_of(i * piece, piece), piece)
                st_g[step, rows, :] = jnp.dot(nt_s[rows, :], dg_s[step % 2], preferred_element_type=F32).astype(BF16)
                st_u[step, rows, :] = jnp.dot(nt_s[rows, :], du_s[step % 2], preferred_element_type=F32).astype(BF16)
                return inner
            lax.fori_loop(0, 4, in_weights, 0)

        ring.take(wqkv_s, sems, 1, step)
        for slot in (ring.own_slot(step), ring.other_slot(step)):
            put_o(slot).start()
            put_q(slot).start()

            @pl.when(slot % 2 == 0)
            def _():
                put_kv(slot, k_out).start()

            @pl.when(slot % 2 == 1)
            def _():
                put_kv(slot, v_out).start()

        @pl.when(step < tiles)
        def _():
            st_d[step] = transposed_times(hid_s[step % 2], dy_s[...]).astype(BF16)

        @pl.when(jnp.logical_and(step > 0, step <= tiles))
        def _():
            for i in range(3):
                put_tile(step - 1, i).start()
                send_tile(step - 1, i, ring.core).start()
        return carry

    lax.fori_loop(0, ring.chips, step_body, 0)
    ring.finish(wo_s, sems, 0)
    ring.finish(wqkv_s, sems, 1)

    def drain(slot, carry):
        put_o(slot).wait()
        put_q(slot).wait()
        put_kv(slot, k_out).wait()
        return carry
    lax.fori_loop(0, devices, drain, 0)

    def drain_tiles(t, carry):
        for i in range(3):
            put_tile(t, i).wait()
            send_tile(t, i, ring.core).wait_send()
            send_tile(t, i, 1 - ring.core).wait_recv()
        return carry
    lax.fori_loop(0, tiles, drain_tiles, 0)


def whole(shape):
    return pl.BlockSpec(shape, lambda *_: (0,) * len(shape))


def solution(mesh):
    group_devices = mesh.shape['sp']
    seq_spec = P('dp', 'sp', None)
    grad_spec = P('dp', None)
    pair_swap = [(i, i ^ 1) for i in range(group_devices)]
    def spread(piece):
        copies = jnp.broadcast_to(piece[None], (group_devices,) + piece.shape)
        return lax.all_to_all(copies, 'sp', 0, 0, tiled=True)

    def layer_step(x_in, grad_y, positions, w_q, w_k, w_v, w_o, w_gate, w_up, w_down, norm_gain, q_norm, k_norm):
        batch_rows, local_len, model_dim = x_in.shape
        num_heads, head_dim = q_norm.shape
        num_kv = k_norm.shape[0]
        share = num_heads // num_kv
        ffn_dim = w_gate.shape[1]
        seq_len = local_len * group_devices
        me = lax.axis_index('sp')
        idx = jnp.stack([me, me // share, me % 2]).astype(jnp.int32)
        params = pltpu.CompilerParams(vmem_limit_bytes=VMEM_LIMIT)
        hbm = pl.BlockSpec(memory_space=pl.ANY)

        def call(kernel, name, flops, bytes_accessed, grid, in_specs, out_specs, out_shape, scratch, aliases=None):
            return pl.pallas_call(
                kernel, out_shape=out_shape, name=name, compiler_params=params, input_output_aliases=aliases or {},
                cost_estimate=pl.CostEstimate(flops=flops, bytes_accessed=bytes_accessed, transcendentals=0),
                grid_spec=pltpu.PrefetchScalarGridSpec(num_scalar_prefetch=1, grid=grid, in_specs=in_specs, out_specs=out_specs,
                                                       scratch_shapes=scratch))

        x_f32 = x_in.reshape(local_len, model_dim).astype(F32)
        flat_norm, norm_back = jax.vjp(input_norm, x_f32, norm_gain)
        grad_flat = grad_y.reshape(local_len, model_dim)
        half = ffn_dim // 2
        dma = pltpu.SemaphoreType.DMA
        chips = group_devices // 2
        ring_sems = lambda lanes: [dma((lanes, chips))] * 4
        struct = jax.ShapeDtypeStruct
        vmem = pltpu.VMEM
        in_vmem = pl.BlockSpec(memory_space=pltpu.VMEM)
        acts = (group_devices, local_len, half)
        blocks = (group_devices, local_len, model_dim)
        pos_rows = jnp.broadcast_to(positions.reshape(1, local_len), (8, local_len))
        n_all, dy_all, pos_all, hid, d_gate, d_up, mlp_out, d_norm_mlp = pl.pallas_call(
            functools.partial(gather_kernel, group_devices), name="gather_tokens",
            out_shape=[struct(blocks, BF16), struct(blocks, BF16), struct((group_devices, 8, local_len), jnp.int32)]
            + [struct(acts, BF16)] * 3 + [struct((local_len, model_dim), BF16), struct((local_len, model_dim), F32)],
            in_specs=[hbm] * 6, out_specs=[hbm] * 6 + [in_vmem] * 2,
            scratch_shapes=[vmem(blocks, BF16), vmem(blocks, BF16), vmem((group_devices, 8, local_len), jnp.int32),
                            vmem((model_dim, half), BF16), vmem((model_dim, half), BF16), vmem((half, model_dim), BF16)]
            + [vmem(acts, BF16)] * 3 + [vmem((2 * local_len, half), F32)] * 2 + [vmem((2, local_len, model_dim), F32)] * 2
            + [dma((3,)), dma((3,))] + ring_sems(3) + [dma((3, group_devices)), dma((3, group_devices)), dma(()), dma(())],
            compiler_params=pltpu.CompilerParams(collective_id=0, has_side_effects=True, vmem_limit_bytes=VMEM_LIMIT),
            cost_estimate=pl.CostEstimate(flops=40_000_000_000, bytes_accessed=40_000_000, transcendentals=0),
        )(flat_norm, grad_flat, pos_rows, w_gate, w_up, w_down)
        n_all, dy_all = n_all.reshape(seq_len, model_dim), dy_all.reshape(seq_len, model_dim)
        hid, d_gate, d_up = (act.reshape(seq_len, half) for act in (hid, d_gate, d_up))
        cos_t, sin_t = rope_lanes(pos_all[:, 0].reshape(seq_len), head_dim)

        vec = jax.ShapeDtypeStruct((1, head_dim), F32)
        rows_bf = jax.ShapeDtypeStruct((seq_len, head_dim), BF16)
        rows_f32 = jax.ShapeDtypeStruct((seq_len, head_dim), F32)
        rows = whole((seq_len, head_dim))
        head_cols = pl.BlockSpec((model_dim, head_dim), lambda g, s: (0, s[0]))
        kv_cols = pl.BlockSpec((model_dim, head_dim), lambda g, s: (0, s[1]))
        head_rows = pl.BlockSpec((head_dim, model_dim), lambda g, s: (s[0], 0))
        head_vec = pl.BlockSpec((1, 1, head_dim), lambda g, s: (s[0], 0, 0))
        kv_vec = pl.BlockSpec((1, 1, head_dim), lambda g, s: (s[1], 0, 0))
        tokens = whole((seq_len, model_dim))
        block = 512
        qn3 = q_norm.reshape(num_heads, 1, head_dim)
        kn3 = k_norm.reshape(num_kv, 1, head_dim)

        o_h, o32, lse, q_rot, k_rot, v_h, q_proj, k_proj = call(
            functools.partial(forward_kernel, block), "attention_fwd", 10_000_000_000, 12_000_000, (1,),
            [tokens, head_cols, kv_cols, kv_cols, head_vec, kv_vec, rows, rows], [rows] * 8,
            [rows_bf, rows_f32, rows_f32] + [rows_bf] * 5, [pltpu.VMEM((block, seq_len), F32)],
        )(idx, n_all, w_q, w_k, w_v, qn3, kn3, cos_t, sin_t)

        d_o, dwo_h = call(
            output_grad_kernel, "output_grad", 3_000_000_000, 6_000_000, (1,), [tokens, head_rows, rows], [rows, whole((head_dim, model_dim))],
            [rows_bf, jax.ShapeDtypeStruct((head_dim, model_dim), BF16)], [],
        )(idx, dy_all, w_o, o_h)

        dq_h, send, keep, gq = call(
            functools.partial(backward_kernel, block), "attention_bwd", 14_000_000_000, 8_000_000, (1,),
            [rows] * 7 + [head_vec, rows, rows], [rows] * 3 + [whole((1, head_dim))], [rows_bf] * 3 + [vec],
            [pltpu.VMEM((seq_len, head_dim), F32)] * 2,
        )(idx, d_o, o32, lse, q_rot, k_rot, v_h, q_proj, qn3, cos_t, sin_t)

        got = lax.ppermute(send, 'sp', pair_swap)
        d_rows, dwqkv_h, gk = call(
            projection_grad_kernel, "projection_grad", 4_000_000_000, 8_000_000, (1,),
            [tokens] + [rows] * 4 + [kv_vec, rows, rows],
            [whole((seq_len, 2 * head_dim)), whole((model_dim, 2 * head_dim)), whole((1, head_dim))],
            [jax.ShapeDtypeStruct((seq_len, 2 * head_dim), BF16), jax.ShapeDtypeStruct((model_dim, 2 * head_dim), BF16), vec],
            [],
        )(idx, n_all, dq_h, keep, got, k_proj, kn3, cos_t, sin_t)

        tile = 256
        tiles = half // tile
        tile_in = (tiles, model_dim, tile)
        dw_q, dw_k, dw_v, dw_o, dw_gate, dw_up, dw_down = pl.pallas_call(
            functools.partial(weight_kernel, group_devices), name="gather_weights",
            out_shape=[struct(w.shape, BF16) for w in (w_q, w_k, w_v, w_o, w_gate, w_up, w_down)],
            in_specs=[hbm] * 7, out_specs=[hbm] * 7,
            scratch_shapes=[vmem((group_devices, head_dim, model_dim), BF16), vmem((group_devices, model_dim, 2 * head_dim), BF16),
                            vmem((seq_len, model_dim), BF16), vmem((seq_len, model_dim), BF16), vmem((model_dim, seq_len), BF16)]
            + [vmem((2, seq_len, tile), BF16)] * 3 + [vmem(tile_in, BF16), vmem(tile_in, BF16), vmem((tiles, tile, model_dim), BF16)]
            + [dma((4,)), dma((3, 2))] + ring_sems(2) + [dma((2, group_devices)), dma((group_devices,))] + [dma((3, tiles))] * 3,
            compiler_params=pltpu.CompilerParams(collective_id=1, has_side_effects=True, vmem_limit_bytes=VMEM_LIMIT),
            cost_estimate=pl.CostEstimate(flops=60_000_000_000, bytes_accessed=60_000_000, transcendentals=0),
        )(dwo_h, dwqkv_h, n_all, dy_all, hid, d_gate, d_up)

        attn_flat = lax.all_to_all(o_h, 'sp', 0, 1, tiled=True)
        attn_out = jnp.dot(attn_flat, w_o, preferred_element_type=F32).astype(BF16)
        y_out = (x_f32 + attn_out.astype(F32) + mlp_out.astype(F32)).astype(BF16)

        d_rows = lax.all_to_all(d_rows, 'sp', 0, 1, tiled=True)
        d_rows = d_rows.reshape(local_len, num_kv, share, 2, head_dim)
        dq_flat = d_rows[:, :, :, 0].reshape(local_len, num_heads * head_dim)
        dk_flat = d_rows[:, :, 0, 1].reshape(local_len, num_kv * head_dim)
        dv_flat = d_rows[:, :, 1, 1].reshape(local_len, num_kv * head_dim)
        d_norm = (times_transposed(dq_flat, w_q) + times_transposed(dk_flat, w_k) + times_transposed(dv_flat, w_v) + d_norm_mlp).astype(BF16)
        dx_norm, grad_gain = norm_back(d_norm)
        grad_x = (grad_flat.astype(F32) + dx_norm).astype(BF16)

        gain_rows = model_dim // head_dim
        small = jnp.concatenate([grad_gain.reshape(gain_rows, head_dim), gq, gk], axis=0)
        small_all = spread(small)
        grad_gain = jnp.sum(small_all[:, :gain_rows], axis=0).reshape(model_dim)
        grad_q_norm = small_all[:, gain_rows]
        grad_k_norm = small_all[::share, gain_rows + 1]

        return (y_out.reshape(x_in.shape), grad_x.reshape(x_in.shape), dw_q, dw_k, dw_v, dw_o, dw_gate, dw_up, dw_down,
                grad_gain, grad_q_norm, grad_k_norm)

    in_specs = (seq_spec, seq_spec, P(('dp', 'sp'))) + (P(),) * 10
    out_specs = (seq_spec, seq_spec) + (grad_spec,) * 7 + (P('dp'), grad_spec, grad_spec)
    return jax.shard_map(layer_step, mesh=mesh, in_specs=in_specs, out_specs=out_specs, check_vma=False)
```

```python
import functools

import jax
import jax.numpy as jnp
from jax import lax
from jax.experimental import pallas as pl
from jax.experimental.pallas import tpu as pltpu
from jax.sharding import PartitionSpec as P

NORM_EPS = 1e-5
ROPE_THETA = 75.0e6
VMEM_LIMIT = 60 * 1024 * 1024
F32 = jnp.float32
BF16 = jnp.bfloat16
MESH = pl.DeviceIdType.MESH


def input_norm(x_f32, norm_gain):
    row_mean = jnp.mean(x_f32, axis=-1, keepdims=True)
    centered = x_f32 - row_mean
    row_var = jnp.mean(centered * centered, axis=-1, keepdims=True)
    return (centered * lax.rsqrt(row_var + NORM_EPS) * norm_gain).astype(BF16)


def swiglu(gate_pre, up_proj):
    return (jax.nn.silu(gate_pre) * up_proj).astype(BF16)


def times_transposed(lhs_mat, rhs_mat):
    return lax.dot_general(lhs_mat, rhs_mat, (((1,), (1,)), ((), ())), preferred_element_type=F32)


def transposed_times(lhs_mat, rhs_mat):
    return lax.dot_general(lhs_mat, rhs_mat, (((0,), (0,)), ((), ())), preferred_element_type=F32)


def rope_lanes(positions, head_dim):
    pair_index = jnp.arange(head_dim, dtype=jnp.int32) // 2
    inv_freq = ROPE_THETA ** (-(pair_index.astype(F32) * 2.0) / head_dim)
    angles = positions.astype(F32)[:, None] * inv_freq[None, :]
    sign = jnp.where(jnp.arange(head_dim) % 2 == 0, -1.0, 1.0).astype(F32)
    return jnp.cos(angles), jnp.sin(angles) * sign[None, :]


def swap_pairs(rows):
    lane = lax.broadcasted_iota(jnp.int32, rows.shape, 1)
    width = rows.shape[1]
    return jnp.where(lane % 2 == 0, pltpu.roll(rows, width - 1, 1), pltpu.roll(rows, 1, 1))


def head_stats(proj_f32):
    row_mean = jnp.mean(proj_f32, axis=-1, keepdims=True)
    centered = proj_f32 - row_mean
    inv_std = lax.rsqrt(jnp.mean(centered * centered, axis=-1, keepdims=True) + NORM_EPS)
    return centered * inv_std, inv_std


def head_forward(proj_f32, weight, cos_t, sin_t):
    unit, _ = head_stats(proj_f32)
    normed = unit * weight
    return (normed * cos_t + swap_pairs(normed) * sin_t).astype(BF16)


def head_backward(d_rot, proj_f32, weight, cos_t, sin_t):
    unit, inv_std = head_stats(proj_f32)
    d_normed = d_rot * cos_t + swap_pairs(d_rot * sin_t)
    d_weight = jnp.sum(d_normed * unit, axis=0, keepdims=True)
    d_unit = d_normed * weight
    mean_d = jnp.mean(d_unit, axis=-1, keepdims=True)
    mean_du = jnp.mean(d_unit * unit, axis=-1, keepdims=True)
    return inv_std * (d_unit - mean_d - unit * mean_du), d_weight


def forward_kernel(block, idx_ref, n_s, wq_ref, wk_ref, wv_ref, qn_ref, kn_ref, cos_ref, sin_ref,
                   o_ref, o32_ref, lse_ref, q_ref, k_ref, v_ref, qproj_ref, kproj_ref, e_s):
    seq_len, head_dim = o_ref.shape
    steps = seq_len // block
    scale = head_dim ** -0.5

    def project(i, carry):
        rows = pl.ds(pl.multiple_of(i * block, block), block)
        n_rows = n_s[rows, :]
        weights = jnp.concatenate([wq_ref[...], wk_ref[...], wv_ref[...]], axis=1)
        proj = jnp.dot(n_rows, weights, preferred_element_type=F32).astype(BF16)
        q_proj, k_proj = proj[:, :head_dim], proj[:, head_dim:2 * head_dim]
        qproj_ref[rows, :] = q_proj
        kproj_ref[rows, :] = k_proj
        v_ref[rows, :] = proj[:, 2 * head_dim:]
        cos_t, sin_t = cos_ref[rows, :], sin_ref[rows, :]
        q_ref[rows, :] = head_forward(q_proj.astype(F32), qn_ref[0], cos_t, sin_t)
        k_ref[rows, :] = head_forward(k_proj.astype(F32), kn_ref[0], cos_t, sin_t)
        return carry

    lax.fori_loop(0, steps, project, 0)
    causal = lax.broadcasted_iota(jnp.int32, (block, block), 0) >= lax.broadcasted_iota(jnp.int32, (block, block), 1)

    def lanes(op, tile):
        return functools.reduce(op, [tile[:, c:c + 128] for c in range(0, block, 128)])

    def keys_of(j):
        return pl.ds(pl.multiple_of(j * block, block), block)

    def query_block(i, carry):
        rows = keys_of(i)
        q_rows = q_ref[rows, :]

        def score(j, top):
            tile = times_transposed(q_rows, k_ref[keys_of(j), :])
            e_s[:, keys_of(j)] = tile
            return jnp.maximum(top, lanes(jnp.maximum, tile))

        top = lax.fori_loop(0, i, score, jnp.full((block, 128), -1e30, F32))
        diag = jnp.where(causal, times_transposed(q_rows, k_ref[rows, :]), -1e30)
        e_s[:, rows] = diag
        top = jnp.max(jnp.maximum(top, lanes(jnp.maximum, diag)), axis=-1, keepdims=True)

        def exponent(j, total):
            tile = jnp.exp((e_s[:, keys_of(j)] - top) * scale)
            e_s[:, keys_of(j)] = tile
            return total + lanes(jnp.add, tile)

        total = lax.fori_loop(0, i + 1, exponent, jnp.zeros((block, 128), F32))
        total = jnp.sum(total, axis=-1, keepdims=True)
        inv_total = 1.0 / total

        def attend(j, acc):
            probs = (e_s[:, keys_of(j)] * inv_total).astype(BF16)
            return acc + jnp.dot(probs, v_ref[keys_of(j), :], preferred_element_type=F32)

        out = lax.fori_loop(0, i + 1, attend, jnp.zeros((block, head_dim), F32))
        o_ref[rows, :] = out.astype(BF16)
        o32_ref[rows, :] = out
        lse_ref[rows, :] = jnp.broadcast_to(top * scale + jnp.log(total), (block, 128))
        return carry

    lax.fori_loop(0, steps, query_block, 0)


def output_grad_kernel(idx_ref, dy_s, wo_ref, o_ref, do_ref, dwo_ref):
    dwo_ref[...] = transposed_times(o_ref[...], dy_s[...]).astype(BF16)
    do_ref[...] = times_transposed(dy_s[...], wo_ref[...]).astype(BF16)


def backward_kernel(block, idx_ref, do_ref, o32_ref, lse_ref, q_ref, k_ref, v_ref, qproj_ref, qn_ref, cos_ref, sin_ref,
                    dq_ref, send_ref, keep_ref, gq_ref, dk_s, dv_s):
    seq_len, head_dim = do_ref.shape
    steps = seq_len // block
    scale = head_dim ** -0.5
    causal = lax.broadcasted_iota(jnp.int32, (block, block), 0) >= lax.broadcasted_iota(jnp.int32, (block, block), 1)
    dk_s[...] = jnp.zeros_like(dk_s)
    dv_s[...] = jnp.zeros_like(dv_s)
    gq_ref[...] = jnp.zeros_like(gq_ref)

    def query_block(i, carry):
        rows = pl.ds(pl.multiple_of(i * block, block), block)
        q_rows, do_rows = q_ref[rows, :], do_ref[rows, :]
        delta = jnp.sum(o32_ref[rows, :] * do_rows.astype(F32), axis=-1, keepdims=True)
        lse = lse_ref[rows, :][:, :1]

        def tile_back(keys, masked):
            k_rows, v_rows = k_ref[keys, :], v_ref[keys, :]
            probs = jnp.exp(times_transposed(q_rows, k_rows) * scale - lse)
            if masked:
                probs = jnp.where(causal, probs, 0.0)
            d_probs = times_transposed(do_rows, v_rows).astype(BF16).astype(F32)
            d_score = (probs * (d_probs - delta) * scale).astype(BF16)
            dv_s[keys, :] += transposed_times(probs.astype(BF16), do_rows)
            dk_s[keys, :] += transposed_times(d_score, q_rows)
            return jnp.dot(d_score, k_rows, preferred_element_type=F32)

        def back(j, acc):
            return acc + tile_back(pl.ds(pl.multiple_of(j * block, block), block), False)

        dq = lax.fori_loop(0, i, back, tile_back(rows, True)).astype(BF16).astype(F32)
        dq_proj, d_weight = head_backward(dq, qproj_ref[rows, :].astype(F32), qn_ref[0], cos_ref[rows, :], sin_ref[rows, :])
        dq_ref[rows, :] = dq_proj.astype(BF16)
        gq_ref[...] += d_weight
        return carry

    lax.fori_loop(0, steps, query_block, 0)
    first = idx_ref[2] == 0

    @pl.when(first)
    def _():
        keep_ref[...] = dk_s[...].astype(BF16)
        send_ref[...] = dv_s[...].astype(BF16)

    @pl.when(jnp.logical_not(first))
    def _():
        keep_ref[...] = dv_s[...].astype(BF16)
        send_ref[...] = dk_s[...].astype(BF16)


def projection_grad_kernel(idx_ref, n_s, dq_ref, keep_ref, got_ref, kproj_ref, kn_ref, cos_ref, sin_ref,
                           rows_ref, dw_ref, gk_ref):
    head_dim = dq_ref.shape[1]
    total = (keep_ref[...].astype(F32) + got_ref[...].astype(F32)).astype(BF16)
    rows_ref[:, :head_dim] = dq_ref[...]
    first = idx_ref[2] == 0

    @pl.when(first)
    def _():
        dk_proj, d_weight = head_backward(total.astype(F32), kproj_ref[...].astype(F32), kn_ref[0], cos_ref[...], sin_ref[...])
        rows_ref[:, head_dim:] = dk_proj.astype(BF16)
        gk_ref[...] = d_weight

    @pl.when(jnp.logical_not(first))
    def _():
        rows_ref[:, head_dim:] = total
        gk_ref[...] = jnp.zeros_like(gk_ref)

    dw_ref[...] = transposed_times(n_s[...], rows_ref[...]).astype(BF16)


class Ring:
    def __init__(self, devices):
        self.chips = devices // 2
        self.me = lax.axis_index('sp')
        self.z, self.core = self.me // 2, self.me % 2
        self.turn = 1 - 2 * self.core
        self.partner = self.me + self.turn
        self.after = self.device(self.z + self.turn, self.core)
        self.before = self.device(self.z - self.turn, self.core)

    def device(self, z, core):
        return 2 * lax.rem(z + 2 * self.chips, self.chips) + core

    def own_slot(self, step):
        return self.device(self.z - self.turn * step, self.core)

    def other_slot(self, step):
        return self.device(self.z + self.turn * step, 1 - self.core)

    def barrier(self):
        sem = pltpu.get_barrier_semaphore()
        for device in (self.after, self.before, self.partner):
            pl.semaphore_signal(sem, inc=1, device_id={'sp': device}, device_id_type=MESH)
        pl.semaphore_wait(sem, 3)

    def forward(self, buf, sems, lane, step):
        slot = buf.at[self.own_slot(step)]
        return pltpu.make_async_remote_copy(slot, slot, sems[0].at[lane, step], sems[1].at[lane, step + 1],
                                            device_id={'sp': self.after}, device_id_type=MESH)

    def share(self, buf, sems, lane, step):
        slot = buf.at[self.own_slot(step)]
        return pltpu.make_async_remote_copy(slot, slot, sems[2].at[lane, step], sems[3].at[lane, step],
                                            device_id={'sp': self.partner}, device_id_type=MESH)

    def arrived(self, buf, sems, lane, step):
        slot = buf.at[self.own_slot(step)]
        return pltpu.make_async_remote_copy(slot, slot, sems[0].at[lane, step], sems[1].at[lane, step],
                                            device_id={'sp': self.before}, device_id_type=MESH)

    def shared(self, buf, sems, lane, step):
        slot = buf.at[self.other_slot(step)]
        return pltpu.make_async_remote_copy(slot, slot, sems[2].at[lane, step], sems[3].at[lane, step],
                                            device_id={'sp': self.partner}, device_id_type=MESH)

    def take(self, buf, sems, lane, step):
        @pl.when(step > 0)
        def _():
            self.arrived(buf, sems, lane, step).wait_recv()

        @pl.when(step < self.chips - 1)
        def _():
            self.forward(buf, sems, lane, step).start()
        self.share(buf, sems, lane, step).start()

    def finish(self, buf, sems, lane):
        def body(step, carry):
            @pl.when(step < self.chips - 1)
            def _():
                self.forward(buf, sems, lane, step).wait_send()
            self.share(buf, sems, lane, step).wait_send()
            return carry
        lax.fori_loop(0, self.chips, body, 0)


def gather_kernel(devices, n_ref, dy_ref, pos_ref, wg_ref, wu_ref, wd_ref,
                  n_out, dy_out, pos_out, hid_out, dg_out, du_out, mlp_out, dn_out,
                  n_s, dy_s, pos_s, wg_s, wu_s, wd_s, hid_s, dg_s, du_s, gate_s, up_s, part_s, got_s, mine_s,
                  load_sem, weight_sem, ring_send, ring_recv, pair_send, pair_recv, out_sem, act_sem, swap_send, swap_recv):
    ring = Ring(devices)
    sems = (ring_send, ring_recv, pair_send, pair_recv)
    half = wg_s.shape[1]
    lanes = ((pos_s, pos_ref, pos_out), (n_s, n_ref, n_out), (dy_s, dy_ref, dy_out))
    loads = [pltpu.make_async_copy(src, buf.at[ring.me], load_sem.at[i]) for i, (buf, src, _) in enumerate(lanes)]
    columns = pl.ds(pl.multiple_of(ring.core * half, half), half)
    weights = [pltpu.make_async_copy(wg_ref.at[:, columns], wg_s, weight_sem.at[0]),
               pltpu.make_async_copy(wu_ref.at[:, columns], wu_s, weight_sem.at[1]),
               pltpu.make_async_copy(wd_ref.at[columns, :], wd_s, weight_sem.at[2])]
    for copy in loads + weights:
        copy.start()
    ring.barrier()
    for copy in loads:
        copy.wait()

    tile = 512
    acts = ((hid_s, hid_out), (dg_s, dg_out), (du_s, du_out))

    def put(lane, slot):
        buf, _, out = lanes[lane]
        return pltpu.make_async_copy(buf.at[slot], out.at[slot], out_sem.at[lane, slot])

    def put_act(i, slot):
        return pltpu.make_async_copy(acts[i][0].at[slot], acts[i][1].at[slot], act_sem.at[i, slot])

    def gate_up(step):
        mine, other = ring.own_slot(step), ring.other_slot(step)

        def body(j, inner):
            cols = pl.ds(pl.multiple_of(j * tile, tile), tile)
            n_rows = jnp.concatenate([n_s[mine], n_s[other]], axis=0)
            gate_s[:, cols] = jnp.dot(n_rows, wg_s[:, cols], preferred_element_type=F32)
            up_s[:, cols] = jnp.dot(n_rows, wu_s[:, cols], preferred_element_type=F32)
            return inner
        lax.fori_loop(0, half // tile, body, 0)

    def hidden(step):
        mine, other = ring.own_slot(step), ring.other_slot(step)

        def body(j, inner):
            cols = pl.ds(pl.multiple_of(j * tile, tile), tile)
            dy_rows = jnp.concatenate([dy_s[mine], dy_s[other]], axis=0)
            d_hidden = times_transposed(dy_rows, wd_s[cols, :]).astype(BF16).astype(F32)
            gate, up = gate_s[:, cols], up_s[:, cols]
            sig = jax.nn.sigmoid(gate)
            silu = gate * sig
            hid = (silu * up).astype(BF16)
            d_up = (d_hidden * silu).astype(BF16)
            d_gate = (d_hidden * up * (sig * (1.0 + gate * (1.0 - sig)))).astype(BF16)
            rows = hid.shape[0] // 2
            for buf, value in ((hid_s, hid), (dg_s, d_gate), (du_s, d_up)):
                buf[mine, :, cols] = value[:rows]
                buf[other, :, cols] = value[rows:]
            return inner
        lax.fori_loop(0, half // tile, body, 0)

    def put_acts(step):
        for i in range(3):
            put_act(i, ring.own_slot(step)).start()
            put_act(i, ring.other_slot(step)).start()

    swap = pltpu.make_async_remote_copy(part_s, got_s, swap_send, swap_recv, device_id={'sp': ring.partner}, device_id_type=MESH)

    def own_tokens(step):
        for k, (slot, keep) in enumerate(((ring.partner, part_s), (ring.me, mine_s))):
            @pl.when(step == 3 * k + 2)
            def _():
                keep[0] = jnp.dot(hid_s[slot], wd_s[...], preferred_element_type=F32)

            @pl.when(step == 3 * k + 3)
            def _():
                keep[1] = times_transposed(dg_s[slot], wg_s[...])

            @pl.when(step == 3 * k + 4)
            def _():
                keep[1] += times_transposed(du_s[slot], wu_s[...])

        @pl.when(step == 5)
        def _():
            swap.start()

    def step_body(step, carry):
        ring.take(n_s, sems, 1, step)
        ring.take(pos_s, sems, 0, step)

        @pl.when(step == 1)
        def _():
            weights[0].wait()
            weights[1].wait()

        @pl.when(step > 0)
        def _():
            gate_up(step - 1)
        ring.take(dy_s, sems, 2, step)

        @pl.when(step == 1)
        def _():
            weights[2].wait()

        @pl.when(step > 0)
        def _():
            hidden(step - 1)

        @pl.when(step > 1)
        def _():
            put_acts(step - 2)
        own_tokens(step)
        for lane in range(3):
            ring.shared(lanes[lane][0], sems, lane, step).wait_recv()
            put(lane, ring.own_slot(step)).start()
            put(lane, ring.other_slot(step)).start()
        return carry

    lax.fori_loop(0, ring.chips, step_body, 0)
    last = ring.chips - 1
    gate_up(last)
    put_acts(last - 1)
    hidden(last)
    own_tokens(last + 1)
    put_acts(last)
    for lane in range(3):
        ring.finish(lanes[lane][0], sems, lane)

    def drain(slot, carry):
        for lane in range(3):
            put(lane, slot).wait()
            put_act(lane, slot).wait()
        return carry
    lax.fori_loop(0, devices, drain, 0)
    swap.wait()
    mlp_out[...] = (mine_s[0] + got_s[0]).astype(BF16)
    dn_out[...] = mine_s[1] + got_s[1]


def weight_kernel(devices, dwo_ref, dwqkv_ref, n_ref, dy_ref, hid_ref, dg_ref, du_ref,
                  q_out, k_out, v_out, o_out, g_out, u_out, d_out,
                  wo_s, wqkv_s, n_s, dy_s, nt_s, hid_s, dg_s, du_s, st_g, st_u, st_d,
                  load_sem, tile_sem, ring_send, ring_recv, pair_send, pair_recv, out_sem, kv_sem,
                  put_sem, swap_send, swap_recv):
    ring = Ring(devices)
    sems = (ring_send, ring_recv, pair_send, pair_recv)
    head_dim, model_dim = dwo_ref.shape
    half = hid_ref.shape[1]
    tile = st_g.shape[2]
    tiles = half // tile
    loads = [pltpu.make_async_copy(dwo_ref, wo_s.at[ring.me], load_sem.at[0]),
             pltpu.make_async_copy(dwqkv_ref, wqkv_s.at[ring.me], load_sem.at[1]),
             pltpu.make_async_copy(n_ref, n_s, load_sem.at[2]),
             pltpu.make_async_copy(dy_ref, dy_s, load_sem.at[3])]
    tile_bufs = ((hid_ref, hid_s), (dg_ref, dg_s), (du_ref, du_s))

    def fetch(i, t):
        cols = pl.ds(pl.multiple_of(t * tile, tile), tile)
        return pltpu.make_async_copy(tile_bufs[i][0].at[:, cols], tile_bufs[i][1].at[t % 2], tile_sem.at[i, t % 2])

    for copy in loads:
        copy.start()
    for i in range(3):
        fetch(i, 0).start()
    ring.barrier()
    loads[0].wait()
    loads[1].wait()

    def put_o(slot):
        rows = pl.ds(pl.multiple_of(slot * head_dim, head_dim), head_dim)
        return pltpu.make_async_copy(wo_s.at[slot], o_out.at[rows, :], out_sem.at[0, slot])

    def put_q(slot):
        cols = pl.ds(pl.multiple_of(slot * head_dim, head_dim), head_dim)
        return pltpu.make_async_copy(wqkv_s.at[slot, :, pl.ds(0, head_dim)], q_out.at[:, cols], out_sem.at[1, slot])

    def put_kv(slot, out):
        cols = pl.ds(pl.multiple_of(slot // 2 * head_dim, head_dim), head_dim)
        return pltpu.make_async_copy(wqkv_s.at[slot, :, pl.ds(head_dim, head_dim)], out.at[:, cols], kv_sem.at[slot])

    def store(t, i, core):
        st, out = ((st_g, g_out), (st_u, u_out), (st_d, d_out))[i]
        span = pl.ds(pl.multiple_of(core * half + t * tile, tile), tile)
        return st.at[t], (out.at[span, :] if i == 2 else out.at[:, span])

    def put_tile(t, i):
        src, dst = store(t, i, ring.core)
        return pltpu.make_async_copy(src, dst, put_sem.at[i, t])

    def send_tile(t, i, core):
        src, dst = store(t, i, core)
        return pltpu.make_async_remote_copy(src, dst, swap_send.at[i, t], swap_recv.at[i, t],
                                            device_id={'sp': ring.partner}, device_id_type=MESH)

    def step_body(step, carry):
        ring.take(wo_s, sems, 0, step)

        @pl.when(step == 0)
        def _():
            loads[2].wait()

            def turn(i, inner):
                rows = pl.ds(pl.multiple_of(i * 256, 256), 256)
                nt_s[:, rows] = n_s[rows, :].T
                return inner
            lax.fori_loop(0, n_s.shape[0] // 256, turn, 0)
            loads[3].wait()

        piece = model_dim // 4

        @pl.when(step < tiles)
        def _():
            for i in range(3):
                fetch(i, step).wait()

            @pl.when(step + 1 < tiles)
            def _():
                for i in range(3):
                    fetch(i, step + 1).start()

            def in_weights(i, inner):
                rows = pl.ds(pl.multiple_of(i * piece, piece), piece)
                st_g[step, rows, :] = jnp.dot(nt_s[rows, :], dg_s[step % 2], preferred_element_type=F32).astype(BF16)
                st_u[step, rows, :] = jnp.dot(nt_s[rows, :], du_s[step % 2], preferred_element_type=F32).astype(BF16)
                return inner
            lax.fori_loop(0, 4, in_weights, 0)

        ring.take(wqkv_s, sems, 1, step)

        @pl.when(step < tiles)
        def _():
            st_d[step] = transposed_times(hid_s[step % 2], dy_s[...]).astype(BF16)

        ring.shared(wo_s, sems, 0, step).wait_recv()
        ring.shared(wqkv_s, sems, 1, step).wait_recv()
        for slot in (ring.own_slot(step), ring.other_slot(step)):
            put_o(slot).start()
            put_q(slot).start()

            @pl.when(slot % 2 == 0)
            def _():
                put_kv(slot, k_out).start()

            @pl.when(slot % 2 == 1)
            def _():
                put_kv(slot, v_out).start()

        @pl.when(jnp.logical_and(step > 0, step <= tiles))
        def _():
            for i in range(3):
                put_tile(step - 1, i).start()
                send_tile(step - 1, i, ring.core).start()
        return carry

    lax.fori_loop(0, ring.chips, step_body, 0)
    ring.finish(wo_s, sems, 0)
    ring.finish(wqkv_s, sems, 1)

    def drain(slot, carry):
        put_o(slot).wait()
        put_q(slot).wait()
        put_kv(slot, k_out).wait()
        return carry
    lax.fori_loop(0, devices, drain, 0)

    def drain_tiles(t, carry):
        for i in range(3):
            put_tile(t, i).wait()
            send_tile(t, i, ring.core).wait_send()
            send_tile(t, i, 1 - ring.core).wait_recv()
        return carry
    lax.fori_loop(0, tiles, drain_tiles, 0)


def whole(shape):
    return pl.BlockSpec(shape, lambda *_: (0,) * len(shape))


def solution(mesh):
    group_devices = mesh.shape['sp']
    seq_spec = P('dp', 'sp', None)
    grad_spec = P('dp', None)
    pair_swap = [(i, i ^ 1) for i in range(group_devices)]
    def spread(piece):
        copies = jnp.broadcast_to(piece[None], (group_devices,) + piece.shape)
        return lax.all_to_all(copies, 'sp', 0, 0, tiled=True)

    def layer_step(x_in, grad_y, positions, w_q, w_k, w_v, w_o, w_gate, w_up, w_down, norm_gain, q_norm, k_norm):
        batch_rows, local_len, model_dim = x_in.shape
        num_heads, head_dim = q_norm.shape
        num_kv = k_norm.shape[0]
        share = num_heads // num_kv
        ffn_dim = w_gate.shape[1]
        seq_len = local_len * group_devices
        me = lax.axis_index('sp')
        idx = jnp.stack([me, me // share, me % 2]).astype(jnp.int32)
        params = pltpu.CompilerParams(vmem_limit_bytes=VMEM_LIMIT)
        hbm = pl.BlockSpec(memory_space=pl.ANY)

        def call(kernel, name, flops, bytes_accessed, grid, in_specs, out_specs, out_shape, scratch, aliases=None):
            return pl.pallas_call(
                kernel, out_shape=out_shape, name=name, compiler_params=params, input_output_aliases=aliases or {},
                cost_estimate=pl.CostEstimate(flops=flops, bytes_accessed=bytes_accessed, transcendentals=0),
                grid_spec=pltpu.PrefetchScalarGridSpec(num_scalar_prefetch=1, grid=grid, in_specs=in_specs, out_specs=out_specs,
                                                       scratch_shapes=scratch))

        x_f32 = x_in.reshape(local_len, model_dim).astype(F32)
        flat_norm, norm_back = jax.vjp(input_norm, x_f32, norm_gain)
        grad_flat = grad_y.reshape(local_len, model_dim)
        half = ffn_dim // 2
        dma = pltpu.SemaphoreType.DMA
        chips = group_devices // 2
        ring_sems = lambda lanes: [dma((lanes, chips))] * 4
        struct = jax.ShapeDtypeStruct
        vmem = pltpu.VMEM
        in_vmem = pl.BlockSpec(memory_space=pltpu.VMEM)
        acts = (group_devices, local_len, half)
        blocks = (group_devices, local_len, model_dim)
        pos_rows = jnp.broadcast_to(positions.reshape(1, local_len), (8, local_len))
        n_all, dy_all, pos_all, hid, d_gate, d_up, mlp_out, d_norm_mlp = pl.pallas_call(
            functools.partial(gather_kernel, group_devices), name="gather_tokens",
            out_shape=[struct(blocks, BF16), struct(blocks, BF16), struct((group_devices, 8, local_len), jnp.int32)]
            + [struct(acts, BF16)] * 3 + [struct((local_len, model_dim), BF16), struct((local_len, model_dim), F32)],
            in_specs=[hbm] * 6, out_specs=[hbm] * 6 + [in_vmem] * 2,
            scratch_shapes=[vmem(blocks, BF16), vmem(blocks, BF16), vmem((group_devices, 8, local_len), jnp.int32),
                            vmem((model_dim, half), BF16), vmem((model_dim, half), BF16), vmem((half, model_dim), BF16)]
            + [vmem(acts, BF16)] * 3 + [vmem((2 * local_len, half), F32)] * 2 + [vmem((2, local_len, model_dim), F32)] * 3
            + [dma((3,)), dma((3,))] + ring_sems(3) + [dma((3, group_devices)), dma((3, group_devices)), dma(()), dma(())],
            compiler_params=pltpu.CompilerParams(collective_id=0, has_side_effects=True, vmem_limit_bytes=VMEM_LIMIT),
            cost_estimate=pl.CostEstimate(flops=40_000_000_000, bytes_accessed=40_000_000, transcendentals=0),
        )(flat_norm, grad_flat, pos_rows, w_gate, w_up, w_down)
        n_all, dy_all = n_all.reshape(seq_len, model_dim), dy_all.reshape(seq_len, model_dim)
        hid, d_gate, d_up = (act.reshape(seq_len, half) for act in (hid, d_gate, d_up))
        cos_t, sin_t = rope_lanes(pos_all[:, 0].reshape(seq_len), head_dim)

        vec = jax.ShapeDtypeStruct((1, head_dim), F32)
        rows_bf = jax.ShapeDtypeStruct((seq_len, head_dim), BF16)
        rows_f32 = jax.ShapeDtypeStruct((seq_len, head_dim), F32)
        rows = whole((seq_len, head_dim))
        head_cols = pl.BlockSpec((model_dim, head_dim), lambda g, s: (0, s[0]))
        kv_cols = pl.BlockSpec((model_dim, head_dim), lambda g, s: (0, s[1]))
        head_rows = pl.BlockSpec((head_dim, model_dim), lambda g, s: (s[0], 0))
        head_vec = pl.BlockSpec((1, 1, head_dim), lambda g, s: (s[0], 0, 0))
        kv_vec = pl.BlockSpec((1, 1, head_dim), lambda g, s: (s[1], 0, 0))
        tokens = whole((seq_len, model_dim))
        block = 512
        qn3 = q_norm.reshape(num_heads, 1, head_dim)
        kn3 = k_norm.reshape(num_kv, 1, head_dim)

        o_h, o32, lse, q_rot, k_rot, v_h, q_proj, k_proj = call(
            functools.partial(forward_kernel, block), "attention_fwd", 10_000_000_000, 12_000_000, (1,),
            [tokens, head_cols, kv_cols, kv_cols, head_vec, kv_vec, rows, rows], [rows] * 8,
            [rows_bf, rows_f32, rows_f32] + [rows_bf] * 5, [pltpu.VMEM((block, seq_len), F32)],
        )(idx, n_all, w_q, w_k, w_v, qn3, kn3, cos_t, sin_t)

        d_o, dwo_h = call(
            output_grad_kernel, "output_grad", 3_000_000_000, 6_000_000, (1,), [tokens, head_rows, rows], [rows, whole((head_dim, model_dim))],
            [rows_bf, jax.ShapeDtypeStruct((head_dim, model_dim), BF16)], [],
        )(idx, dy_all, w_o, o_h)

        dq_h, send, keep, gq = call(
            functools.partial(backward_kernel, block), "attention_bwd", 14_000_000_000, 8_000_000, (1,),
            [rows] * 7 + [head_vec, rows, rows], [rows] * 3 + [whole((1, head_dim))], [rows_bf] * 3 + [vec],
            [pltpu.VMEM((seq_len, head_dim), F32)] * 2,
        )(idx, d_o, o32, lse, q_rot, k_rot, v_h, q_proj, qn3, cos_t, sin_t)

        got = lax.ppermute(send, 'sp', pair_swap)
        d_rows, dwqkv_h, gk = call(
            projection_grad_kernel, "projection_grad", 4_000_000_000, 8_000_000, (1,),
            [tokens] + [rows] * 4 + [kv_vec, rows, rows],
            [whole((seq_len, 2 * head_dim)), whole((model_dim, 2 * head_dim)), whole((1, head_dim))],
            [jax.ShapeDtypeStruct((seq_len, 2 * head_dim), BF16), jax.ShapeDtypeStruct((model_dim, 2 * head_dim), BF16), vec],
            [],
        )(idx, n_all, dq_h, keep, got, k_proj, kn3, cos_t, sin_t)

        tile = 256
        tiles = half // tile
        tile_in = (tiles, model_dim, tile)
        dw_q, dw_k, dw_v, dw_o, dw_gate, dw_up, dw_down = pl.pallas_call(
            functools.partial(weight_kernel, group_devices), name="gather_weights",
            out_shape=[struct(w.shape, BF16) for w in (w_q, w_k, w_v, w_o, w_gate, w_up, w_down)],
            in_specs=[hbm] * 7, out_specs=[hbm] * 7,
            scratch_shapes=[vmem((group_devices, head_dim, model_dim), BF16), vmem((group_devices, model_dim, 2 * head_dim), BF16),
                            vmem((seq_len, model_dim), BF16), vmem((seq_len, model_dim), BF16), vmem((model_dim, seq_len), BF16)]
            + [vmem((2, seq_len, tile), BF16)] * 3 + [vmem(tile_in, BF16), vmem(tile_in, BF16), vmem((tiles, tile, model_dim), BF16)]
            + [dma((4,)), dma((3, 2))] + ring_sems(2) + [dma((2, group_devices)), dma((group_devices,))] + [dma((3, tiles))] * 3,
            compiler_params=pltpu.CompilerParams(collective_id=1, has_side_effects=True, vmem_limit_bytes=VMEM_LIMIT),
            cost_estimate=pl.CostEstimate(flops=60_000_000_000, bytes_accessed=60_000_000, transcendentals=0),
        )(dwo_h, dwqkv_h, n_all, dy_all, hid, d_gate, d_up)

        attn_flat = lax.all_to_all(o_h, 'sp', 0, 1, tiled=True)
        attn_out = jnp.dot(attn_flat, w_o, preferred_element_type=F32).astype(BF16)
        y_out = (x_f32 + attn_out.astype(F32) + mlp_out.astype(F32)).astype(BF16)

        d_rows = lax.all_to_all(d_rows, 'sp', 0, 1, tiled=True)
        d_rows = d_rows.reshape(local_len, num_kv, share, 2, head_dim)
        dq_flat = d_rows[:, :, :, 0].reshape(local_len, num_heads * head_dim)
        dk_flat = d_rows[:, :, 0, 1].reshape(local_len, num_kv * head_dim)
        dv_flat = d_rows[:, :, 1, 1].reshape(local_len, num_kv * head_dim)
        d_norm = (times_transposed(dq_flat, w_q) + times_transposed(dk_flat, w_k) + times_transposed(dv_flat, w_v) + d_norm_mlp).astype(BF16)
        dx_norm, grad_gain = norm_back(d_norm)
        grad_x = (grad_flat.astype(F32) + dx_norm).astype(BF16)

        gain_rows = model_dim // head_dim
        small = jnp.concatenate([grad_gain.reshape(gain_rows, head_dim), gq, gk], axis=0)
        small_all = spread(small)
        grad_gain = jnp.sum(small_all[:, :gain_rows], axis=0).reshape(model_dim)
        grad_q_norm = small_all[:, gain_rows]
        grad_k_norm = small_all[::share, gain_rows + 1]

        return (y_out.reshape(x_in.shape), grad_x.reshape(x_in.shape), dw_q, dw_k, dw_v, dw_o, dw_gate, dw_up, dw_down,
                grad_gain, grad_q_norm, grad_k_norm)

    in_specs = (seq_spec, seq_spec, P(('dp', 'sp'))) + (P(),) * 10
    out_specs = (seq_spec, seq_spec) + (grad_spec,) * 7 + (P('dp'), grad_spec, grad_spec)
    return jax.shard_map(layer_step, mesh=mesh, in_specs=in_specs, out_specs=out_specs, check_vma=False)
```

```python
import functools

import jax
import jax.numpy as jnp
from jax import lax
from jax.experimental import pallas as pl
from jax.experimental.pallas import tpu as pltpu
from jax.sharding import PartitionSpec as P

NORM_EPS = 1e-5
ROPE_THETA = 75.0e6
VMEM_LIMIT = 63 * 1024 * 1024
F32 = jnp.float32
BF16 = jnp.bfloat16
MESH = pl.DeviceIdType.MESH


def input_norm(x_f32, norm_gain):
    row_mean = jnp.mean(x_f32, axis=-1, keepdims=True)
    centered = x_f32 - row_mean
    row_var = jnp.mean(centered * centered, axis=-1, keepdims=True)
    return (centered * lax.rsqrt(row_var + NORM_EPS) * norm_gain).astype(BF16)


def swiglu(gate_pre, up_proj):
    return (jax.nn.silu(gate_pre) * up_proj).astype(BF16)


def times_transposed(lhs_mat, rhs_mat):
    return lax.dot_general(lhs_mat, rhs_mat, (((1,), (1,)), ((), ())), preferred_element_type=F32)


def transposed_times(lhs_mat, rhs_mat):
    return lax.dot_general(lhs_mat, rhs_mat, (((0,), (0,)), ((), ())), preferred_element_type=F32)


def rope_lanes(positions, head_dim):
    pair_index = jnp.arange(head_dim, dtype=jnp.int32) // 2
    inv_freq = ROPE_THETA ** (-(pair_index.astype(F32) * 2.0) / head_dim)
    angles = positions.astype(F32)[:, None] * inv_freq[None, :]
    sign = jnp.where(jnp.arange(head_dim) % 2 == 0, -1.0, 1.0).astype(F32)
    return jnp.cos(angles), jnp.sin(angles) * sign[None, :]


def swap_pairs(rows):
    lane = lax.broadcasted_iota(jnp.int32, rows.shape, 1)
    width = rows.shape[1]
    return jnp.where(lane % 2 == 0, pltpu.roll(rows, width - 1, 1), pltpu.roll(rows, 1, 1))


def head_stats(proj_f32):
    row_mean = jnp.mean(proj_f32, axis=-1, keepdims=True)
    centered = proj_f32 - row_mean
    inv_std = lax.rsqrt(jnp.mean(centered * centered, axis=-1, keepdims=True) + NORM_EPS)
    return centered * inv_std, inv_std


def head_forward(proj_f32, weight, cos_t, sin_t):
    unit, _ = head_stats(proj_f32)
    normed = unit * weight
    return (normed * cos_t + swap_pairs(normed) * sin_t).astype(BF16)


def head_backward(d_rot, proj_f32, weight, cos_t, sin_t):
    unit, inv_std = head_stats(proj_f32)
    d_normed = d_rot * cos_t + swap_pairs(d_rot * sin_t)
    d_weight = jnp.sum(d_normed * unit, axis=0, keepdims=True)
    d_unit = d_normed * weight
    mean_d = jnp.mean(d_unit, axis=-1, keepdims=True)
    mean_du = jnp.mean(d_unit * unit, axis=-1, keepdims=True)
    return inv_std * (d_unit - mean_d - unit * mean_du), d_weight


def forward_kernel(block, idx_ref, n_s, wq_ref, wk_ref, wv_ref, qn_ref, kn_ref, cos_ref, sin_ref,
                   o_ref, o32_ref, lse_ref, q_ref, k_ref, v_ref, qproj_ref, kproj_ref, e_s):
    seq_len, head_dim = o_ref.shape
    steps = seq_len // block
    scale = head_dim ** -0.5

    def project(i, carry):
        rows = pl.ds(pl.multiple_of(i * block, block), block)
        n_rows = n_s[rows, :]
        weights = jnp.concatenate([wq_ref[...], wk_ref[...], wv_ref[...]], axis=1)
        proj = jnp.dot(n_rows, weights, preferred_element_type=F32).astype(BF16)
        q_proj, k_proj = proj[:, :head_dim], proj[:, head_dim:2 * head_dim]
        qproj_ref[rows, :] = q_proj
        kproj_ref[rows, :] = k_proj
        v_ref[rows, :] = proj[:, 2 * head_dim:]
        cos_t, sin_t = cos_ref[rows, :], sin_ref[rows, :]
        q_ref[rows, :] = head_forward(q_proj.astype(F32), qn_ref[0], cos_t, sin_t)
        k_ref[rows, :] = head_forward(k_proj.astype(F32), kn_ref[0], cos_t, sin_t)
        return carry

    lax.fori_loop(0, steps, project, 0)
    causal = lax.broadcasted_iota(jnp.int32, (block, block), 0) >= lax.broadcasted_iota(jnp.int32, (block, block), 1)

    def lanes(op, tile):
        return functools.reduce(op, [tile[:, c:c + 128] for c in range(0, block, 128)])

    def keys_of(j):
        return pl.ds(pl.multiple_of(j * block, block), block)

    def query_block(i, carry):
        rows = keys_of(i)
        q_rows = q_ref[rows, :]

        def score(j, top):
            tile = times_transposed(q_rows, k_ref[keys_of(j), :])
            e_s[:, keys_of(j)] = tile
            return jnp.maximum(top, lanes(jnp.maximum, tile))

        top = lax.fori_loop(0, i, score, jnp.full((block, 128), -1e30, F32))
        diag = jnp.where(causal, times_transposed(q_rows, k_ref[rows, :]), -1e30)
        e_s[:, rows] = diag
        top = jnp.max(jnp.maximum(top, lanes(jnp.maximum, diag)), axis=-1, keepdims=True)

        def exponent(j, total):
            tile = jnp.exp((e_s[:, keys_of(j)] - top) * scale)
            e_s[:, keys_of(j)] = tile
            return total + lanes(jnp.add, tile)

        total = lax.fori_loop(0, i + 1, exponent, jnp.zeros((block, 128), F32))
        total = jnp.sum(total, axis=-1, keepdims=True)
        inv_total = 1.0 / total

        def attend(j, acc):
            probs = (e_s[:, keys_of(j)] * inv_total).astype(BF16)
            return acc + jnp.dot(probs, v_ref[keys_of(j), :], preferred_element_type=F32)

        out = lax.fori_loop(0, i + 1, attend, jnp.zeros((block, head_dim), F32))
        o_ref[rows, :] = out.astype(BF16)
        o32_ref[rows, :] = out
        lse_ref[rows, :] = jnp.broadcast_to(top * scale + jnp.log(total), (block, 128))
        return carry

    lax.fori_loop(0, steps, query_block, 0)


class Ring:
    def __init__(self, devices):
        self.chips = devices // 2
        self.me = lax.axis_index('sp')
        self.z, self.core = self.me // 2, self.me % 2
        self.turn = 1 - 2 * self.core
        self.partner = self.me + self.turn
        self.after = self.device(self.z + self.turn, self.core)
        self.before = self.device(self.z - self.turn, self.core)

    def device(self, z, core):
        return 2 * lax.rem(z + 2 * self.chips, self.chips) + core

    def own_slot(self, step):
        return self.device(self.z - self.turn * step, self.core)

    def other_slot(self, step):
        return self.device(self.z + self.turn * step, 1 - self.core)

    def barrier(self):
        sem = pltpu.get_barrier_semaphore()
        for device in (self.after, self.before, self.partner):
            pl.semaphore_signal(sem, inc=1, device_id={'sp': device}, device_id_type=MESH)
        pl.semaphore_wait(sem, 3)

    def barrier_all(self):
        sem = pltpu.get_barrier_semaphore()

        def signal(hop, carry):
            pl.semaphore_signal(sem, inc=1, device_id={'sp': self.peer(hop)}, device_id_type=MESH)
            return carry
        lax.fori_loop(1, 2 * self.chips, signal, 0)
        pl.semaphore_wait(sem, 2 * self.chips - 1)

    def peer(self, hop):
        return lax.rem(self.me + hop, 2 * self.chips)

    def direct(self, src, dst, send, recv, hop):
        return pltpu.make_async_remote_copy(src, dst, send.at[hop], recv.at[hop],
                                            device_id={'sp': self.peer(hop)}, device_id_type=MESH)

    def forward(self, buf, sems, lane, step):
        slot = buf.at[self.own_slot(step)]
        return pltpu.make_async_remote_copy(slot, slot, sems[0].at[lane, step], sems[1].at[lane, step + 1],
                                            device_id={'sp': self.after}, device_id_type=MESH)

    def share(self, buf, sems, lane, step):
        slot = buf.at[self.own_slot(step)]
        return pltpu.make_async_remote_copy(slot, slot, sems[2].at[lane, step], sems[3].at[lane, step],
                                            device_id={'sp': self.partner}, device_id_type=MESH)

    def arrived(self, buf, sems, lane, step):
        slot = buf.at[self.own_slot(step)]
        return pltpu.make_async_remote_copy(slot, slot, sems[0].at[lane, step], sems[1].at[lane, step],
                                            device_id={'sp': self.before}, device_id_type=MESH)

    def shared(self, buf, sems, lane, step):
        slot = buf.at[self.other_slot(step)]
        return pltpu.make_async_remote_copy(slot, slot, sems[2].at[lane, step], sems[3].at[lane, step],
                                            device_id={'sp': self.partner}, device_id_type=MESH)

    def take(self, buf, sems, lane, step):
        @pl.when(step > 0)
        def _():
            self.arrived(buf, sems, lane, step).wait_recv()

        @pl.when(step < self.chips - 1)
        def _():
            self.forward(buf, sems, lane, step).start()
        self.share(buf, sems, lane, step).start()

    def finish(self, buf, sems, lane):
        def body(step, carry):
            @pl.when(step < self.chips - 1)
            def _():
                self.forward(buf, sems, lane, step).wait_send()
            self.share(buf, sems, lane, step).wait_send()
            return carry
        lax.fori_loop(0, self.chips, body, 0)


def gather_kernel(devices, x_ref, gain_ref, dy_ref, pos_ref, wg_ref, wu_ref, wd_ref,
                  n_out, dy_out, pos_out, hid_out, dg_out, du_out, mlp_out, dn_out,
                  n_s, dy_s, pos_s, wg_s, wu_s, wd_s, hid_s, dg_s, du_s, gate_s, up_s, part_s, got_s, mine_s,
                  load_sem, weight_sem, ring_send, ring_recv, pair_send, pair_recv, out_sem, act_sem, swap_send, swap_recv):
    ring = Ring(devices)
    sems = (ring_send, ring_recv, pair_send, pair_recv)
    half = wg_s.shape[1]
    lanes = ((pos_s, pos_ref, pos_out), (n_s, None, n_out), (dy_s, dy_ref, dy_out))
    loads = [pltpu.make_async_copy(src, buf.at[ring.me], load_sem.at[i]) for i, (buf, src, _) in enumerate(lanes) if src is not None]
    columns = pl.ds(pl.multiple_of(ring.core * half, half), half)
    weights = [pltpu.make_async_copy(wg_ref.at[:, columns], wg_s, weight_sem.at[0]),
               pltpu.make_async_copy(wu_ref.at[:, columns], wu_s, weight_sem.at[1]),
               pltpu.make_async_copy(wd_ref.at[columns, :], wd_s, weight_sem.at[2])]
    for copy in loads + weights:
        copy.start()
    n_s[ring.me] = input_norm(x_ref[...].astype(F32), gain_ref[...])
    ring.barrier()
    for copy in loads:
        copy.wait()

    tile = 512
    acts = ((hid_s, hid_out), (dg_s, dg_out), (du_s, du_out))

    def put(lane, slot):
        buf, _, out = lanes[lane]
        return pltpu.make_async_copy(buf.at[slot], out.at[slot], out_sem.at[lane, slot])

    def put_act(i, slot):
        return pltpu.make_async_copy(acts[i][0].at[slot], acts[i][1].at[slot], act_sem.at[i, slot])

    def gate_up(step):
        mine, other = ring.own_slot(step), ring.other_slot(step)

        def body(j, inner):
            cols = pl.ds(pl.multiple_of(j * tile, tile), tile)
            n_rows = jnp.concatenate([n_s[mine], n_s[other]], axis=0)
            gate_s[:, cols] = jnp.dot(n_rows, wg_s[:, cols], preferred_element_type=F32)
            up_s[:, cols] = jnp.dot(n_rows, wu_s[:, cols], preferred_element_type=F32)
            return inner
        lax.fori_loop(0, half // tile, body, 0)

    def hidden(step):
        mine, other = ring.own_slot(step), ring.other_slot(step)

        def body(j, inner):
            cols = pl.ds(pl.multiple_of(j * tile, tile), tile)
            dy_rows = jnp.concatenate([dy_s[mine], dy_s[other]], axis=0)
            d_hidden = times_transposed(dy_rows, wd_s[cols, :]).astype(BF16).astype(F32)
            gate, up = gate_s[:, cols], up_s[:, cols]
            sig = jax.nn.sigmoid(gate)
            silu = gate * sig
            hid = (silu * up).astype(BF16)
            d_up = (d_hidden * silu).astype(BF16)
            d_gate = (d_hidden * up * (sig * (1.0 + gate * (1.0 - sig)))).astype(BF16)
            rows = hid.shape[0] // 2
            for buf, value in ((hid_s, hid), (dg_s, d_gate), (du_s, d_up)):
                buf[mine, :, cols] = value[:rows]
                buf[other, :, cols] = value[rows:]
            return inner
        lax.fori_loop(0, half // tile, body, 0)

    def put_acts(step):
        for i in range(3):
            put_act(i, ring.own_slot(step)).start()
            put_act(i, ring.other_slot(step)).start()

    swap = pltpu.make_async_remote_copy(part_s, got_s, swap_send, swap_recv, device_id={'sp': ring.partner}, device_id_type=MESH)

    def own_tokens(step):
        for k, (slot, keep) in enumerate(((ring.partner, part_s), (ring.me, mine_s))):
            @pl.when(step == 3 * k + 2)
            def _():
                keep[0] = jnp.dot(hid_s[slot], wd_s[...], preferred_element_type=F32)

            @pl.when(step == 3 * k + 3)
            def _():
                keep[1] = times_transposed(dg_s[slot], wg_s[...])

            @pl.when(step == 3 * k + 4)
            def _():
                keep[1] += times_transposed(du_s[slot], wu_s[...])

        @pl.when(step == 5)
        def _():
            swap.start()

    def step_body(step, carry):
        ring.take(n_s, sems, 1, step)
        ring.take(pos_s, sems, 0, step)

        @pl.when(step == 1)
        def _():
            weights[0].wait()
            weights[1].wait()

        @pl.when(step > 0)
        def _():
            gate_up(step - 1)
        ring.take(dy_s, sems, 2, step)

        @pl.when(step == 1)
        def _():
            weights[2].wait()

        @pl.when(step > 0)
        def _():
            hidden(step - 1)

        @pl.when(step > 1)
        def _():
            put_acts(step - 2)
        own_tokens(step)
        for lane in range(3):
            ring.shared(lanes[lane][0], sems, lane, step).wait_recv()
            put(lane, ring.own_slot(step)).start()
            put(lane, ring.other_slot(step)).start()
        return carry

    lax.fori_loop(0, ring.chips, step_body, 0)
    last = ring.chips - 1
    gate_up(last)
    put_acts(last - 1)
    hidden(last)
    own_tokens(last + 1)
    put_acts(last)
    for lane in range(3):
        ring.finish(lanes[lane][0], sems, lane)

    def drain(slot, carry):
        for lane in range(3):
            put(lane, slot).wait()
            put_act(lane, slot).wait()
        return carry
    lax.fori_loop(0, devices, drain, 0)
    swap.wait()
    mlp_out[...] = (mine_s[0] + got_s[0]).astype(BF16)
    dn_out[...] = mine_s[1] + got_s[1]


def backward_kernel(devices, block, dy_ref, n_ref, wo_ref, o_ref, o32_ref, lse_ref, q_ref, k_ref, v_ref, qproj_ref, kproj_ref,
                    qn_ref, kn_ref, cos_ref, sin_ref,
                    rows_out, dw_out, wo_out, gq_ref, gk_ref,
                    dy_s, n_s, w_s, wo_s, do_s, dk_s, dv_s, send_s, got_s, rows_s,
                    load_sem, ring_send, ring_recv, pair_send, pair_recv, out_sem, swap_send, swap_recv):
    ring = Ring(devices)
    sems = (ring_send, ring_recv, pair_send, pair_recv)
    seq_len, head_dim = do_s.shape
    steps = seq_len // block
    scale = head_dim ** -0.5
    share = devices // kn_ref.shape[0]
    w_rows = pl.ds(pl.multiple_of(ring.me * head_dim, head_dim), head_dim)
    loads = [pltpu.make_async_copy(dy_ref, dy_s, load_sem.at[0]), pltpu.make_async_copy(wo_ref.at[w_rows, :], w_s, load_sem.at[1]),
             pltpu.make_async_copy(n_ref, n_s, load_sem.at[2])]
    for copy in loads:
        copy.start()
    ring.barrier()
    dk_s[...] = jnp.zeros_like(dk_s)
    dv_s[...] = jnp.zeros_like(dv_s)
    gq_ref[...] = jnp.zeros_like(gq_ref)
    loads[0].wait()
    wo_s[ring.me] = transposed_times(o_ref[...], dy_s[...]).astype(BF16)
    loads[1].wait()
    do_s[...] = times_transposed(dy_s[...], w_s[...]).astype(BF16)
    ring.take(wo_s, sems, 0, 0)
    causal = lax.broadcasted_iota(jnp.int32, (block, block), 0) >= lax.broadcasted_iota(jnp.int32, (block, block), 1)
    q_weight = qn_ref[ring.me]
    done = 0
    passed = 1
    for i in range(steps):
        rows = pl.ds(i * block, block)
        q_rows, do_rows = q_ref[rows, :], do_s[rows, :]
        delta = jnp.sum(o32_ref[rows, :] * do_rows.astype(F32), axis=-1, keepdims=True)
        lse = lse_ref[rows, :][:, :1]
        dq = jnp.zeros((block, head_dim), F32)
        for j in range(i + 1):
            keys = pl.ds(j * block, block)
            k_rows, v_rows = k_ref[keys, :], v_ref[keys, :]
            probs = jnp.exp(times_transposed(q_rows, k_rows) * scale - lse)
            if i == j:
                probs = jnp.where(causal, probs, 0.0)
            d_probs = times_transposed(do_rows, v_rows).astype(BF16).astype(F32)
            d_score = (probs * (d_probs - delta) * scale).astype(BF16)
            dv_s[keys, :] += transposed_times(probs.astype(BF16), do_rows)
            dk_s[keys, :] += transposed_times(d_score, q_rows)
            dq = dq + jnp.dot(d_score, k_rows, preferred_element_type=F32)
            done += 1
            if done % 2 == 0 and passed < ring.chips - 2:
                ring.take(wo_s, sems, 0, passed)
                passed += 1
        dq_proj, d_weight = head_backward(dq.astype(BF16).astype(F32), qproj_ref[rows, :].astype(F32), q_weight,
                                          cos_ref[rows, :], sin_ref[rows, :])
        rows_s[rows, pl.ds(0, head_dim)] = dq_proj.astype(BF16)
        gq_ref[...] += d_weight

    @pl.when(ring.core == 0)
    def _():
        send_s[...] = dv_s[...].astype(BF16)

    @pl.when(ring.core == 1)
    def _():
        send_s[...] = dk_s[...].astype(BF16)
    while passed < ring.chips - 1:
        ring.take(wo_s, sems, 0, passed)
        passed += 1
    swap = pltpu.make_async_remote_copy(send_s, got_s, swap_send, swap_recv, device_id={'sp': ring.partner}, device_id_type=MESH)
    swap.start()
    loads[2].wait()
    swap.wait()

    @pl.when(ring.core == 0)
    def _():
        total = (dk_s[...].astype(BF16).astype(F32) + got_s[...].astype(F32)).astype(BF16).astype(F32)
        dk_proj, d_weight = head_backward(total, kproj_ref[...].astype(F32), kn_ref[ring.me // share], cos_ref[...], sin_ref[...])
        rows_s[:, head_dim:] = dk_proj.astype(BF16)
        gk_ref[...] = d_weight

    @pl.when(ring.core == 1)
    def _():
        rows_s[:, head_dim:] = (dv_s[...].astype(BF16).astype(F32) + got_s[...].astype(F32)).astype(BF16)
        gk_ref[...] = jnp.zeros_like(gk_ref)
    ring.take(wo_s, sems, 0, passed)
    put_rows = pltpu.make_async_copy(rows_s, rows_out, load_sem.at[3])
    put_rows.start()
    dw_out[...] = transposed_times(n_s[...], rows_s[...]).astype(BF16)

    def put_o(slot):
        rows = pl.ds(pl.multiple_of(slot * head_dim, head_dim), head_dim)
        return pltpu.make_async_copy(wo_s.at[slot], wo_out.at[rows, :], out_sem.at[slot])

    def collect(step, carry):
        ring.shared(wo_s, sems, 0, step).wait_recv()
        put_o(ring.own_slot(step)).start()
        put_o(ring.other_slot(step)).start()
        return carry
    lax.fori_loop(0, ring.chips, collect, 0)
    ring.finish(wo_s, sems, 0)

    def drain(slot, carry):
        put_o(slot).wait()
        return carry
    lax.fori_loop(0, devices, drain, 0)
    put_rows.wait()


def weight_kernel(devices, dwqkv_ref, rows_ref, o_ref, n_ref, dy_ref, hid_ref, dg_ref, du_ref, wq_ref, wk_ref, wv_ref, wo_ref,
                  x_ref, gain_ref, mlp_ref, dn_ref, gq_ref, gk_ref,
                  q_out, k_out, v_out, g_out, u_out, d_out, y_out, dx_out, gain_out, qn_out, kn_out,
                  wqkv_s, n_s, dy_s, nt_s, hid_s, dg_s, du_s, st_g, st_u, st_d, got_s, of_s, df_s, kf_s, vf_s, wq_s, wk_s, wv_s, wo_s, small_s,
                  load_sem, tile_sem, ring_send, ring_recv, pair_send, pair_recv, out_sem, kv_sem,
                  put_sem, swap_send, swap_recv, rows_send, rows_recv, small_send, small_recv):
    ring = Ring(devices)
    sems = (ring_send, ring_recv, pair_send, pair_recv)
    model_dim = n_ref.shape[1]
    local_len, head_dim = o_ref.shape[1:]
    half = hid_ref.shape[1]
    tile = st_g.shape[2]
    tiles = half // tile
    num_kv = kn_out.shape[0]
    share = devices // num_kv
    loads = [pltpu.make_async_copy(dwqkv_ref, wqkv_s.at[ring.me], load_sem.at[0]),
             pltpu.make_async_copy(rows_ref.at[ring.me], got_s.at[ring.me], load_sem.at[1]),
             pltpu.make_async_copy(n_ref, n_s, load_sem.at[2]),
             pltpu.make_async_copy(dy_ref, dy_s, load_sem.at[3])]
    late = [pltpu.make_async_copy(src, dst, load_sem.at[4 + i])
            for i, (src, dst) in enumerate(((wo_ref, wo_s), (wq_ref, wq_s), (wk_ref, wk_s), (wv_ref, wv_s)))]
    tile_bufs = ((hid_ref, hid_s), (dg_ref, dg_s), (du_ref, du_s))

    def fetch(i, t):
        cols = pl.ds(pl.multiple_of(t * tile, tile), tile)
        return pltpu.make_async_copy(tile_bufs[i][0].at[:, cols], tile_bufs[i][1].at[t % 2], tile_sem.at[i, t % 2])

    for copy in loads:
        copy.start()
    for i in range(3):
        fetch(i, 0).start()
    ring.barrier_all()
    loads[0].wait()

    def rows_copy(hop):
        return ring.direct(rows_ref.at[ring.peer(hop)], got_s.at[ring.me], rows_send, rows_recv, hop)

    def rows_from(hop):
        source = lax.rem(ring.me + devices - hop, devices)
        return ring.direct(rows_ref.at[source], got_s.at[source], rows_send, rows_recv, hop)

    def small_copy(hop):
        return ring.direct(small_s.at[ring.me], small_s.at[ring.me], small_send, small_recv, hop)

    def small_from(hop):
        source = lax.rem(ring.me + devices - hop, devices)
        return ring.direct(small_s.at[source], small_s.at[source], small_send, small_recv, hop)

    def each_peer(body):
        def step(hop, carry):
            body(hop)
            return carry
        lax.fori_loop(1, devices, step, 0)

    def put_q(slot):
        cols = pl.ds(pl.multiple_of(slot * head_dim, head_dim), head_dim)
        return pltpu.make_async_copy(wqkv_s.at[slot, :, pl.ds(0, head_dim)], q_out.at[:, cols], out_sem.at[slot])

    def put_kv(slot, out):
        cols = pl.ds(pl.multiple_of(slot // share * head_dim, head_dim), head_dim)
        return pltpu.make_async_copy(wqkv_s.at[slot, :, pl.ds(head_dim, head_dim)], out.at[:, cols], kv_sem.at[slot])

    def store(t, i, core):
        st, out = ((st_g, g_out), (st_u, u_out), (st_d, d_out))[i]
        span = pl.ds(pl.multiple_of(core * half + t * tile, tile), tile)
        return st.at[t], (out.at[span, :] if i == 2 else out.at[:, span])

    def put_tile(t, i):
        src, dst = store(t, i, ring.core)
        return pltpu.make_async_copy(src, dst, put_sem.at[i, t])

    def send_tile(t, i, core):
        src, dst = store(t, i, core)
        return pltpu.make_async_remote_copy(src, dst, swap_send.at[i, t], swap_recv.at[i, t],
                                            device_id={'sp': ring.partner}, device_id_type=MESH)

    def finish_forward():
        late[0].wait()
        for h in range(devices):
            of_s[:, h * head_dim:(h + 1) * head_dim] = o_ref[h]
        attn_out = jnp.dot(of_s[...], wo_s[...], preferred_element_type=F32).astype(BF16)
        y_out[...] = (x_ref[...].astype(F32) + attn_out.astype(F32) + mlp_ref[...].astype(F32)).astype(BF16)

    def finish_backward():
        each_peer(lambda hop: rows_from(hop).wait_recv())
        loads[1].wait()
        for h in range(devices):
            df_s[:, h * head_dim:(h + 1) * head_dim] = got_s[h, :, :head_dim]
        for j in range(num_kv):
            kf_s[:, j * head_dim:(j + 1) * head_dim] = got_s[share * j, :, head_dim:]
            vf_s[:, j * head_dim:(j + 1) * head_dim] = got_s[share * j + 1, :, head_dim:]
        for copy in late[1:]:
            copy.wait()
        d_norm = (times_transposed(df_s[...], wq_s[...]) + times_transposed(kf_s[...], wk_s[...])
                  + times_transposed(vf_s[...], wv_s[...]) + dn_ref[...]).astype(BF16).astype(F32)
        unit, inv_std = head_stats(x_ref[...].astype(F32))
        grad_gain = jnp.sum(d_norm * unit, axis=0, keepdims=True)
        d_unit = d_norm * gain_ref[...]
        mean_d = jnp.mean(d_unit, axis=-1, keepdims=True)
        mean_du = jnp.mean(d_unit * unit, axis=-1, keepdims=True)
        dx = inv_std * (d_unit - mean_d - unit * mean_du)
        own_rows = pl.ds(pl.multiple_of(ring.me * local_len, local_len), local_len)
        dx_out[...] = (dy_s[own_rows, :].astype(F32) + dx).astype(BF16)
        gains = model_dim // head_dim
        parts = [grad_gain[:, c * head_dim:(c + 1) * head_dim] for c in range(gains)] + [gq_ref[...], gk_ref[...]]
        pad = jnp.zeros((small_s.shape[1] - len(parts), head_dim), F32)
        small_s[ring.me] = jnp.concatenate(parts + [pad], axis=0)

    def step_body(step, carry):
        ring.take(wqkv_s, sems, 0, step)

        @pl.when(step == 0)
        def _():
            each_peer(lambda hop: rows_copy(hop).start())
            loads[2].wait()

            def turn(i, inner):
                rows = pl.ds(pl.multiple_of(i * 256, 256), 256)
                nt_s[:, rows] = n_s[rows, :].T
                return inner
            lax.fori_loop(0, n_s.shape[0] // 256, turn, 0)
            loads[3].wait()

        piece = model_dim // 4

        @pl.when(step < tiles)
        def _():
            for i in range(3):
                fetch(i, step).wait()

            @pl.when(step + 1 < tiles)
            def _():
                for i in range(3):
                    fetch(i, step + 1).start()

            def in_weights(i, inner):
                rows = pl.ds(pl.multiple_of(i * piece, piece), piece)
                st_g[step, rows, :] = jnp.dot(nt_s[rows, :], dg_s[step % 2], preferred_element_type=F32).astype(BF16)
                st_u[step, rows, :] = jnp.dot(nt_s[rows, :], du_s[step % 2], preferred_element_type=F32).astype(BF16)
                return inner
            lax.fori_loop(0, 4, in_weights, 0)
            st_d[step] = transposed_times(hid_s[step % 2], dy_s[...]).astype(BF16)

        @pl.when(step == 1)
        def _():
            for copy in late:
                copy.start()

        @pl.when(step == tiles)
        def _():
            finish_forward()

        @pl.when(step == tiles + 1)
        def _():
            finish_backward()

        ring.shared(wqkv_s, sems, 0, step).wait_recv()
        for slot in (ring.own_slot(step), ring.other_slot(step)):
            put_q(slot).start()

            @pl.when(slot % 2 == 0)
            def _():
                put_kv(slot, k_out).start()

            @pl.when(slot % 2 == 1)
            def _():
                put_kv(slot, v_out).start()

        @pl.when(jnp.logical_and(step > 0, step <= tiles))
        def _():
            for i in range(3):
                put_tile(step - 1, i).start()
                send_tile(step - 1, i, ring.core).start()
        return carry

    lax.fori_loop(0, ring.chips, step_body, 0)
    each_peer(lambda hop: small_copy(hop).start())
    ring.finish(wqkv_s, sems, 0)

    def drain(slot, carry):
        put_q(slot).wait()
        put_kv(slot, k_out).wait()
        return carry
    lax.fori_loop(0, devices, drain, 0)

    def drain_tiles(t, carry):
        for i in range(3):
            put_tile(t, i).wait()
            send_tile(t, i, ring.core).wait_send()
            send_tile(t, i, 1 - ring.core).wait_recv()
        return carry
    lax.fori_loop(0, tiles, drain_tiles, 0)
    each_peer(lambda hop: rows_copy(hop).wait_send())
    each_peer(lambda hop: small_from(hop).wait_recv())
    each_peer(lambda hop: small_copy(hop).wait_send())
    gains = model_dim // head_dim
    total = small_s[0, :gains]
    for h in range(1, devices):
        total = total + small_s[h, :gains]
    gain_out[...] = total
    qn_out[...] = jnp.concatenate([small_s[h, gains:gains + 1] for h in range(devices)], axis=0)
    kn_out[...] = jnp.concatenate([small_s[share * j, gains + 1:gains + 2] for j in range(num_kv)], axis=0)


def whole(shape):
    return pl.BlockSpec(shape, lambda *_: (0,) * len(shape))


def solution(mesh):
    group_devices = mesh.shape['sp']
    seq_spec = P('dp', 'sp', None)
    grad_spec = P('dp', None)
    def layer_step(x_in, grad_y, positions, w_q, w_k, w_v, w_o, w_gate, w_up, w_down, norm_gain, q_norm, k_norm):
        batch_rows, local_len, model_dim = x_in.shape
        num_heads, head_dim = q_norm.shape
        num_kv = k_norm.shape[0]
        share = num_heads // num_kv
        ffn_dim = w_gate.shape[1]
        seq_len = local_len * group_devices
        me = lax.axis_index('sp')
        idx = jnp.stack([me, me // share, me % 2]).astype(jnp.int32)
        params = pltpu.CompilerParams(vmem_limit_bytes=VMEM_LIMIT)
        hbm = pl.BlockSpec(memory_space=pl.ANY)

        def call(kernel, name, flops, bytes_accessed, grid, in_specs, out_specs, out_shape, scratch, aliases=None):
            return pl.pallas_call(
                kernel, out_shape=out_shape, name=name, compiler_params=params, input_output_aliases=aliases or {},
                cost_estimate=pl.CostEstimate(flops=flops, bytes_accessed=bytes_accessed, transcendentals=0),
                grid_spec=pltpu.PrefetchScalarGridSpec(num_scalar_prefetch=1, grid=grid, in_specs=in_specs, out_specs=out_specs,
                                                       scratch_shapes=scratch))

        x_rows = x_in.reshape(local_len, model_dim)
        gain_row = norm_gain.reshape(1, model_dim)
        grad_flat = grad_y.reshape(local_len, model_dim)
        half = ffn_dim // 2
        dma = pltpu.SemaphoreType.DMA
        chips = group_devices // 2
        ring_sems = lambda lanes: [dma((lanes, chips))] * 4
        struct = jax.ShapeDtypeStruct
        vmem = pltpu.VMEM
        in_vmem = pl.BlockSpec(memory_space=pltpu.VMEM)
        acts = (group_devices, local_len, half)
        blocks = (group_devices, local_len, model_dim)
        pos_rows = jnp.broadcast_to(positions.reshape(1, local_len), (8, local_len))
        n_all, dy_all, pos_all, hid, d_gate, d_up, mlp_out, d_norm_mlp = pl.pallas_call(
            functools.partial(gather_kernel, group_devices), name="gather_tokens",
            out_shape=[struct(blocks, BF16), struct(blocks, BF16), struct((group_devices, 8, local_len), jnp.int32)]
            + [struct(acts, BF16)] * 3 + [struct((local_len, model_dim), BF16), struct((local_len, model_dim), F32)],
            in_specs=[in_vmem] * 2 + [hbm] * 5, out_specs=[hbm] * 6 + [in_vmem] * 2,
            scratch_shapes=[vmem(blocks, BF16), vmem(blocks, BF16), vmem((group_devices, 8, local_len), jnp.int32),
                            vmem((model_dim, half), BF16), vmem((model_dim, half), BF16), vmem((half, model_dim), BF16)]
            + [vmem(acts, BF16)] * 3 + [vmem((2 * local_len, half), F32)] * 2 + [vmem((2, local_len, model_dim), F32)] * 3
            + [dma((3,)), dma((3,))] + ring_sems(3) + [dma((3, group_devices)), dma((3, group_devices)), dma(()), dma(())],
            compiler_params=pltpu.CompilerParams(collective_id=0, has_side_effects=True, vmem_limit_bytes=VMEM_LIMIT),
            cost_estimate=pl.CostEstimate(flops=40_000_000_000, bytes_accessed=40_000_000, transcendentals=0),
        )(x_rows, gain_row, grad_flat, pos_rows, w_gate, w_up, w_down)
        n_all, dy_all = n_all.reshape(seq_len, model_dim), dy_all.reshape(seq_len, model_dim)
        hid, d_gate, d_up = (act.reshape(seq_len, half) for act in (hid, d_gate, d_up))
        cos_t, sin_t = rope_lanes(pos_all[:, 0].reshape(seq_len), head_dim)

        vec = jax.ShapeDtypeStruct((1, head_dim), F32)
        rows_bf = jax.ShapeDtypeStruct((seq_len, head_dim), BF16)
        rows_f32 = jax.ShapeDtypeStruct((seq_len, head_dim), F32)
        rows = whole((seq_len, head_dim))
        head_cols = pl.BlockSpec((model_dim, head_dim), lambda g, s: (0, s[0]))
        kv_cols = pl.BlockSpec((model_dim, head_dim), lambda g, s: (0, s[1]))
        head_rows = pl.BlockSpec((head_dim, model_dim), lambda g, s: (s[0], 0))
        head_vec = pl.BlockSpec((1, 1, head_dim), lambda g, s: (s[0], 0, 0))
        kv_vec = pl.BlockSpec((1, 1, head_dim), lambda g, s: (s[1], 0, 0))
        tokens = whole((seq_len, model_dim))
        block = 512
        qn3 = q_norm.reshape(num_heads, 1, head_dim)
        kn3 = k_norm.reshape(num_kv, 1, head_dim)

        o_h, o32, lse, q_rot, k_rot, v_h, q_proj, k_proj = call(
            functools.partial(forward_kernel, block), "attention_fwd", 10_000_000_000, 12_000_000, (1,),
            [tokens, head_cols, kv_cols, kv_cols, head_vec, kv_vec, rows, rows], [rows] * 8,
            [rows_bf, rows_f32, rows_f32] + [rows_bf] * 5, [pltpu.VMEM((block, seq_len), F32)],
        )(idx, n_all, w_q, w_k, w_v, qn3, kn3, cos_t, sin_t)

        attn_own = lax.all_to_all(o_h.reshape(group_devices, local_len, head_dim), 'sp', 0, 0, tiled=True)
        d_rows, dwqkv_h, dw_o, gq, gk = pl.pallas_call(
            functools.partial(backward_kernel, group_devices, block), name="attention_bwd",
            out_shape=[struct((seq_len, 2 * head_dim), BF16), struct((model_dim, 2 * head_dim), BF16), struct(w_o.shape, BF16), vec, vec],
            in_specs=[hbm] * 3 + [in_vmem] * 12, out_specs=[hbm, in_vmem, hbm, in_vmem, in_vmem],
            scratch_shapes=[vmem((seq_len, model_dim), BF16)] * 2 + [vmem((head_dim, model_dim), BF16), vmem((group_devices, head_dim, model_dim), BF16)]
            + [vmem((seq_len, head_dim), BF16)] + [vmem((seq_len, head_dim), F32)] * 2 + [vmem((seq_len, head_dim), BF16)] * 2
            + [vmem((seq_len, 2 * head_dim), BF16), dma((4,))] + ring_sems(1) + [dma((group_devices,)), dma(()), dma(())],
            compiler_params=pltpu.CompilerParams(collective_id=2, has_side_effects=True, vmem_limit_bytes=VMEM_LIMIT),
            cost_estimate=pl.CostEstimate(flops=30_000_000_000, bytes_accessed=30_000_000, transcendentals=0),
        )(dy_all, n_all, w_o, o_h, o32, lse, q_rot, k_rot, v_h, q_proj, k_proj, qn3, kn3, cos_t, sin_t)

        tile = 256
        tiles = half // tile
        tile_in = (tiles, model_dim, tile)
        gain_shape = (model_dim // head_dim, head_dim)
        flat = (local_len, num_heads * head_dim)
        flat_kv = (local_len, num_kv * head_dim)
        dw_q, dw_k, dw_v, dw_gate, dw_up, dw_down, y_out, grad_x, grad_gain, grad_q_norm, grad_k_norm = pl.pallas_call(
            functools.partial(weight_kernel, group_devices), name="gather_weights",
            out_shape=[struct(w.shape, BF16) for w in (w_q, w_k, w_v, w_gate, w_up, w_down)]
            + [struct((local_len, model_dim), BF16)] * 2 + [struct(gain_shape, F32), struct(q_norm.shape, F32), struct(k_norm.shape, F32)],
            in_specs=[hbm, hbm, in_vmem] + [hbm] * 9 + [in_vmem] * 6, out_specs=[hbm] * 6 + [in_vmem] * 5,
            scratch_shapes=[vmem((group_devices, model_dim, 2 * head_dim), BF16),
                            vmem((seq_len, model_dim), BF16), vmem((seq_len, model_dim), BF16), vmem((model_dim, seq_len), BF16)]
            + [vmem((2, seq_len, tile), BF16)] * 3 + [vmem(tile_in, BF16), vmem(tile_in, BF16), vmem((tiles, tile, model_dim), BF16)]
            + [vmem((group_devices, local_len, 2 * head_dim), BF16), vmem(flat, BF16), vmem(flat, BF16), vmem(flat_kv, BF16), vmem(flat_kv, BF16)]
            + [vmem(w.shape, BF16) for w in (w_q, w_k, w_v, w_o)] + [vmem((group_devices, 16, head_dim), F32)]
            + [dma((8,)), dma((3, 2))] + ring_sems(1) + [dma((group_devices,))] * 2 + [dma((3, tiles))] * 3 + [dma((group_devices,))] * 4,
            compiler_params=pltpu.CompilerParams(collective_id=1, has_side_effects=True, vmem_limit_bytes=VMEM_LIMIT),
            cost_estimate=pl.CostEstimate(flops=60_000_000_000, bytes_accessed=60_000_000, transcendentals=0),
        )(dwqkv_h, d_rows.reshape(group_devices, local_len, 2 * head_dim), attn_own, n_all, dy_all, hid, d_gate, d_up,
          w_q, w_k, w_v, w_o, x_rows, gain_row, mlp_out, d_norm_mlp, gq, gk)
        grad_gain = grad_gain.reshape(model_dim)
        return (y_out.reshape(x_in.shape), grad_x.reshape(x_in.shape), dw_q, dw_k, dw_v, dw_o, dw_gate, dw_up, dw_down,
                grad_gain, grad_q_norm, grad_k_norm)

    in_specs = (seq_spec, seq_spec, P(('dp', 'sp'))) + (P(),) * 10
    out_specs = (seq_spec, seq_spec) + (grad_spec,) * 7 + (P('dp'), grad_spec, grad_spec)
    return jax.shard_map(layer_step, mesh=mesh, in_specs=in_specs, out_specs=out_specs, check_vma=False)
```

```python
import functools

import jax
import jax.numpy as jnp
from jax import lax
from jax.experimental import pallas as pl
from jax.experimental.pallas import tpu as pltpu
from jax.sharding import PartitionSpec as P

NORM_EPS = 1e-5
ROPE_THETA = 75.0e6
VMEM_LIMIT = 63 * 1024 * 1024
F32 = jnp.float32
BF16 = jnp.bfloat16
MESH = pl.DeviceIdType.MESH


def input_norm(x_f32, norm_gain):
    row_mean = jnp.mean(x_f32, axis=-1, keepdims=True)
    centered = x_f32 - row_mean
    row_var = jnp.mean(centered * centered, axis=-1, keepdims=True)
    return (centered * lax.rsqrt(row_var + NORM_EPS) * norm_gain).astype(BF16)


def swiglu(gate_pre, up_proj):
    return (jax.nn.silu(gate_pre) * up_proj).astype(BF16)


def times_transposed(lhs_mat, rhs_mat):
    return lax.dot_general(lhs_mat, rhs_mat, (((1,), (1,)), ((), ())), preferred_element_type=F32)


def transposed_times(lhs_mat, rhs_mat):
    return lax.dot_general(lhs_mat, rhs_mat, (((0,), (0,)), ((), ())), preferred_element_type=F32)


def rope_lanes(head_dim):
    pair_index = jnp.arange(head_dim, dtype=jnp.int32) // 2
    inv_freq = ROPE_THETA ** (-(pair_index.astype(F32) * 2.0) / head_dim)
    sign = jnp.where(jnp.arange(head_dim) % 2 == 0, -1.0, 1.0).astype(F32)
    return inv_freq[None, :], sign[None, :]


def swap_pairs(rows):
    lane = lax.broadcasted_iota(jnp.int32, rows.shape, 1)
    width = rows.shape[1]
    return jnp.where(lane % 2 == 0, pltpu.roll(rows, width - 1, 1), pltpu.roll(rows, 1, 1))


def head_stats(proj_f32):
    row_mean = jnp.mean(proj_f32, axis=-1, keepdims=True)
    centered = proj_f32 - row_mean
    inv_std = lax.rsqrt(jnp.mean(centered * centered, axis=-1, keepdims=True) + NORM_EPS)
    return centered * inv_std, inv_std


def head_forward(proj_f32, weight, cos_t, sin_t):
    unit, _ = head_stats(proj_f32)
    normed = unit * weight
    return (normed * cos_t + swap_pairs(normed) * sin_t).astype(BF16)


def head_backward(d_rot, proj_f32, weight, cos_t, sin_t):
    unit, inv_std = head_stats(proj_f32)
    d_normed = d_rot * cos_t + swap_pairs(d_rot * sin_t)
    d_weight = jnp.sum(d_normed * unit, axis=0, keepdims=True)
    d_unit = d_normed * weight
    mean_d = jnp.mean(d_unit, axis=-1, keepdims=True)
    mean_du = jnp.mean(d_unit * unit, axis=-1, keepdims=True)
    return inv_std * (d_unit - mean_d - unit * mean_du), d_weight


def forward_kernel(block, idx_ref, n_s, wq_ref, wk_ref, wv_ref, qn_ref, kn_ref, cos_ref, sin_ref,
                   o_ref, o32_ref, lse_ref, q_ref, k_ref, v_ref, qproj_ref, kproj_ref, e_s):
    seq_len, head_dim = o_ref.shape
    steps = seq_len // block
    scale = head_dim ** -0.5

    def project(i, carry):
        rows = pl.ds(pl.multiple_of(i * block, block), block)
        n_rows = n_s[rows, :]
        weights = jnp.concatenate([wq_ref[...], wk_ref[...], wv_ref[...]], axis=1)
        proj = jnp.dot(n_rows, weights, preferred_element_type=F32).astype(BF16)
        q_proj, k_proj = proj[:, :head_dim], proj[:, head_dim:2 * head_dim]
        qproj_ref[rows, :] = q_proj
        kproj_ref[rows, :] = k_proj
        v_ref[rows, :] = proj[:, 2 * head_dim:]
        cos_t, sin_t = cos_ref[rows, :], sin_ref[rows, :]
        q_ref[rows, :] = head_forward(q_proj.astype(F32), qn_ref[0], cos_t, sin_t)
        k_ref[rows, :] = head_forward(k_proj.astype(F32), kn_ref[0], cos_t, sin_t)
        return carry

    lax.fori_loop(0, steps, project, 0)
    causal = lax.broadcasted_iota(jnp.int32, (block, block), 0) >= lax.broadcasted_iota(jnp.int32, (block, block), 1)

    def lanes(op, tile):
        return functools.reduce(op, [tile[:, c:c + 128] for c in range(0, block, 128)])

    def keys_of(j):
        return pl.ds(pl.multiple_of(j * block, block), block)

    def query_block(i, carry):
        rows = keys_of(i)
        q_rows = q_ref[rows, :]

        def score(j, top):
            tile = times_transposed(q_rows, k_ref[keys_of(j), :])
            e_s[:, keys_of(j)] = tile
            return jnp.maximum(top, lanes(jnp.maximum, tile))

        top = lax.fori_loop(0, i, score, jnp.full((block, 128), -1e30, F32))
        diag = jnp.where(causal, times_transposed(q_rows, k_ref[rows, :]), -1e30)
        e_s[:, rows] = diag
        top = jnp.max(jnp.maximum(top, lanes(jnp.maximum, diag)), axis=-1, keepdims=True)

        def exponent(j, total):
            tile = jnp.exp((e_s[:, keys_of(j)] - top) * scale)
            e_s[:, keys_of(j)] = tile
            return total + lanes(jnp.add, tile)

        total = lax.fori_loop(0, i + 1, exponent, jnp.zeros((block, 128), F32))
        total = jnp.sum(total, axis=-1, keepdims=True)
        inv_total = 1.0 / total

        def attend(j, acc):
            probs = (e_s[:, keys_of(j)] * inv_total).astype(BF16)
            return acc + jnp.dot(probs, v_ref[keys_of(j), :], preferred_element_type=F32)

        out = lax.fori_loop(0, i + 1, attend, jnp.zeros((block, head_dim), F32))
        o_ref[rows, :] = out.astype(BF16)
        o32_ref[rows, :] = out
        lse_ref[rows, :] = jnp.broadcast_to(top * scale + jnp.log(total), (block, 128))
        return carry

    lax.fori_loop(0, steps, query_block, 0)


class Ring:
    def __init__(self, devices):
        self.chips = devices // 2
        self.me = lax.axis_index('sp')
        self.z, self.core = self.me // 2, self.me % 2
        self.turn = 1 - 2 * self.core
        self.partner = self.me + self.turn
        self.after = self.device(self.z + self.turn, self.core)
        self.before = self.device(self.z - self.turn, self.core)

    def device(self, z, core):
        return 2 * lax.rem(z + 2 * self.chips, self.chips) + core

    def own_slot(self, step):
        return self.device(self.z - self.turn * step, self.core)

    def other_slot(self, step):
        return self.device(self.z + self.turn * step, 1 - self.core)

    def barrier(self):
        sem = pltpu.get_barrier_semaphore()
        for device in (self.after, self.before, self.partner):
            pl.semaphore_signal(sem, inc=1, device_id={'sp': device}, device_id_type=MESH)
        pl.semaphore_wait(sem, 3)

    def barrier_all(self):
        sem = pltpu.get_barrier_semaphore()

        def signal(hop, carry):
            pl.semaphore_signal(sem, inc=1, device_id={'sp': self.peer(hop)}, device_id_type=MESH)
            return carry
        lax.fori_loop(1, 2 * self.chips, signal, 0)
        pl.semaphore_wait(sem, 2 * self.chips - 1)

    def peer(self, hop):
        return lax.rem(self.me + hop, 2 * self.chips)

    def direct(self, src, dst, send, recv, hop):
        return pltpu.make_async_remote_copy(src, dst, send.at[hop], recv.at[hop],
                                            device_id={'sp': self.peer(hop)}, device_id_type=MESH)

    def part(self, buf, slot, parts, k):
        rows = buf.shape[1] // parts
        return buf.at[slot, pl.ds(k * rows, rows)]

    def forward(self, lane, k, step):
        buf, sems, parts = lane
        piece = self.part(buf, self.own_slot(step), parts, k)
        return pltpu.make_async_remote_copy(piece, piece, sems[0].at[k, step], sems[1].at[k, step + 1],
                                            device_id={'sp': self.after}, device_id_type=MESH)

    def share(self, lane, k, step):
        buf, sems, parts = lane
        piece = self.part(buf, self.own_slot(step), parts, k)
        return pltpu.make_async_remote_copy(piece, piece, sems[2].at[k, step], sems[3].at[k, step],
                                            device_id={'sp': self.partner}, device_id_type=MESH)

    def arrived(self, lane, k, step):
        buf, sems, parts = lane
        piece = self.part(buf, self.own_slot(step), parts, k)
        return pltpu.make_async_remote_copy(piece, piece, sems[0].at[k, step], sems[1].at[k, step],
                                            device_id={'sp': self.before}, device_id_type=MESH)

    def shared(self, lane, step):
        buf, sems, parts = lane
        for k in range(parts):
            piece = self.part(buf, self.other_slot(step), parts, k)
            pltpu.make_async_remote_copy(piece, piece, sems[2].at[k, step], sems[3].at[k, step],
                                         device_id={'sp': self.partner}, device_id_type=MESH).wait_recv()

    def take(self, lane, step, ks=None):
        for k in range(lane[2]) if ks is None else ks:
            @pl.when(step > 0)
            def _():
                self.arrived(lane, k, step).wait_recv()

            @pl.when(step < self.chips - 1)
            def _():
                self.forward(lane, k, step).start()
            self.share(lane, k, step).start()

    def finish(self, lane):
        def body(step, carry):
            for k in range(lane[2]):
                @pl.when(step < self.chips - 1)
                def _():
                    self.forward(lane, k, step).wait_send()
                self.share(lane, k, step).wait_send()
            return carry
        lax.fori_loop(0, self.chips, body, 0)


def gather_kernel(devices, x_ref, gain_ref, freq_ref, sign_ref, dy_ref, pos_ref, wg_ref, wu_ref, wd_ref,
                  n_out, dy_out, cos_out, sin_out, hid_out, dg_out, du_out, mlp_out, dn_out,
                  n_s, dy_s, pos_s, wg_s, wu_s, wd_s, hid_s, dg_s, du_s, gate_s, up_s, part_s, got_s, mine_s,
                  load_sem, weight_sem, *sem_refs):
    ring = Ring(devices)
    out_sem, act_sem, swap_send, swap_recv = sem_refs[12:]
    p_lane, n_lane, dy_lane = ((buf, sem_refs[4 * i:4 * i + 4], parts) for i, (buf, parts) in enumerate(((pos_s, 1), (n_s, 2), (dy_s, 2))))
    half = wg_s.shape[1]
    lanes = ((pos_s, pos_ref, None), (n_s, None, n_out), (dy_s, dy_ref, dy_out))
    loads = [pltpu.make_async_copy(src, buf.at[ring.me], load_sem.at[i]) for i, (buf, src, _) in enumerate(lanes) if src is not None]
    columns = pl.ds(pl.multiple_of(ring.core * half, half), half)
    weights = [pltpu.make_async_copy(wg_ref.at[:, columns], wg_s, weight_sem.at[0]),
               pltpu.make_async_copy(wu_ref.at[:, columns], wu_s, weight_sem.at[1]),
               pltpu.make_async_copy(wd_ref.at[columns, :], wd_s, weight_sem.at[2])]
    for copy in loads + weights:
        copy.start()
    n_s[ring.me] = input_norm(x_ref[...].astype(F32), gain_ref[...])
    ring.barrier()
    for copy in loads:
        copy.wait()

    tile = 512
    acts = ((hid_s, hid_out), (dg_s, dg_out), (du_s, du_out))

    def put(lane, slot):
        buf, _, out = lanes[lane]
        return pltpu.make_async_copy(buf.at[slot], out.at[slot], out_sem.at[lane, slot])

    def put_act(i, slot):
        return pltpu.make_async_copy(acts[i][0].at[slot], acts[i][1].at[slot], act_sem.at[i, slot])

    def gate_up(step):
        mine, other = ring.own_slot(step), ring.other_slot(step)

        def body(j, inner):
            cols = pl.ds(pl.multiple_of(j * tile, tile), tile)
            n_rows = jnp.concatenate([n_s[mine], n_s[other]], axis=0)
            gate_s[:, cols] = jnp.dot(n_rows, wg_s[:, cols], preferred_element_type=F32)
            up_s[:, cols] = jnp.dot(n_rows, wu_s[:, cols], preferred_element_type=F32)
            return inner
        lax.fori_loop(0, half // tile, body, 0)

    def hidden(step):
        mine, other = ring.own_slot(step), ring.other_slot(step)

        def body(j, inner):
            cols = pl.ds(pl.multiple_of(j * tile, tile), tile)
            dy_rows = jnp.concatenate([dy_s[mine], dy_s[other]], axis=0)
            d_hidden = times_transposed(dy_rows, wd_s[cols, :]).astype(BF16).astype(F32)
            gate, up = gate_s[:, cols], up_s[:, cols]
            sig = jax.nn.sigmoid(gate)
            silu = gate * sig
            hid = (silu * up).astype(BF16)
            d_up = (d_hidden * silu).astype(BF16)
            d_gate = (d_hidden * up * (sig * (1.0 + gate * (1.0 - sig)))).astype(BF16)
            rows = hid.shape[0] // 2
            for buf, value in ((hid_s, hid), (dg_s, d_gate), (du_s, d_up)):
                buf[mine, :, cols] = value[:rows]
                buf[other, :, cols] = value[rows:]
            return inner
        lax.fori_loop(0, half // tile, body, 0)

    def tables(step):
        for slot in (ring.own_slot(step), ring.other_slot(step)):
            angles = pos_s[slot].astype(F32).T[:, :1] * freq_ref[...]
            cos_out[slot] = jnp.cos(angles)
            sin_out[slot] = jnp.sin(angles) * sign_ref[...]

    def put_acts(step):
        for i in range(3):
            put_act(i, ring.own_slot(step)).start()
            put_act(i, ring.other_slot(step)).start()

    swap = pltpu.make_async_remote_copy(part_s, got_s, swap_send, swap_recv, device_id={'sp': ring.partner}, device_id_type=MESH)

    def own_tokens(step):
        for k, (slot, keep) in enumerate(((ring.partner, part_s), (ring.me, mine_s))):
            @pl.when(step == 3 * k + 2)
            def _():
                keep[0] = jnp.dot(hid_s[slot], wd_s[...], preferred_element_type=F32)

            @pl.when(step == 3 * k + 3)
            def _():
                keep[1] = times_transposed(dg_s[slot], wg_s[...])

            @pl.when(step == 3 * k + 4)
            def _():
                keep[1] += times_transposed(du_s[slot], wu_s[...])

        @pl.when(step == 5)
        def _():
            swap.start()

    def step_body(step, carry):
        ring.take(n_lane, step)
        ring.take(p_lane, step)

        @pl.when(step == 1)
        def _():
            weights[0].wait()
            weights[1].wait()

        @pl.when(step > 0)
        def _():
            gate_up(step - 1)
        ring.take(dy_lane, step)

        @pl.when(step == 1)
        def _():
            weights[2].wait()

        @pl.when(step > 0)
        def _():
            hidden(step - 1)

        @pl.when(step > 1)
        def _():
            put_acts(step - 2)
            tables(step - 2)
        own_tokens(step)
        for lane in (p_lane, n_lane, dy_lane):
            ring.shared(lane, step)
        for lane in (1, 2):
            put(lane, ring.own_slot(step)).start()
            put(lane, ring.other_slot(step)).start()
        return carry

    lax.fori_loop(0, ring.chips, step_body, 0)
    last = ring.chips - 1
    gate_up(last)
    put_acts(last - 1)
    tables(last - 1)
    hidden(last)
    tables(last)
    own_tokens(last + 1)
    put_acts(last)
    for lane in (p_lane, n_lane, dy_lane):
        ring.finish(lane)

    def drain(slot, carry):
        for lane in (1, 2):
            put(lane, slot).wait()
        for i in range(3):
            put_act(i, slot).wait()
        return carry
    lax.fori_loop(0, devices, drain, 0)
    swap.wait()
    mlp_out[...] = (mine_s[0] + got_s[0]).astype(BF16)
    dn_out[...] = mine_s[1] + got_s[1]


def backward_kernel(devices, block, dy_ref, n_ref, wo_ref, o_ref, o32_ref, lse_ref, q_ref, k_ref, v_ref, qproj_ref, kproj_ref,
                    qn_ref, kn_ref, cos_ref, sin_ref,
                    rows_out, dw_out, wo_out, own_out, gq_ref, gk_ref,
                    dy_s, n_s, w_s, wo_s, do_s, dk_s, dv_s, send_s, got_s, rows_s, own_s,
                    load_sem, ring_send, ring_recv, pair_send, pair_recv, out_sem, swap_send, swap_recv, o_send, o_recv):
    ring = Ring(devices)
    lane = (wo_s, (ring_send, ring_recv, pair_send, pair_recv), 2)
    seq_len, head_dim = do_s.shape
    steps = seq_len // block
    scale = head_dim ** -0.5
    share = devices // kn_ref.shape[0]
    w_rows = pl.ds(pl.multiple_of(ring.me * head_dim, head_dim), head_dim)
    loads = [pltpu.make_async_copy(dy_ref, dy_s, load_sem.at[0]), pltpu.make_async_copy(wo_ref.at[w_rows, :], w_s, load_sem.at[1]),
             pltpu.make_async_copy(n_ref, n_s, load_sem.at[2])]
    for copy in loads:
        copy.start()
    ring.barrier_all()
    local_len = seq_len // devices

    def tokens_of(device):
        return pl.ds(pl.multiple_of(device * local_len, local_len), local_len)

    def o_copy(hop):
        return ring.direct(o_ref.at[tokens_of(ring.peer(hop)), :], own_s.at[ring.me], o_send, o_recv, hop)

    def o_from(hop):
        source = lax.rem(ring.me + devices - hop, devices)
        return ring.direct(o_ref.at[tokens_of(source), :], own_s.at[source], o_send, o_recv, hop)

    def each_peer(body):
        def step(hop, carry):
            body(hop)
            return carry
        lax.fori_loop(1, devices, step, 0)

    each_peer(lambda hop: o_copy(hop).start())
    own_s[ring.me] = o_ref[tokens_of(ring.me), :]
    dk_s[...] = jnp.zeros_like(dk_s)
    dv_s[...] = jnp.zeros_like(dv_s)
    gq_ref[...] = jnp.zeros_like(gq_ref)
    loads[0].wait()
    wo_s[ring.me] = transposed_times(o_ref[...], dy_s[...]).astype(BF16)
    loads[1].wait()
    do_s[...] = times_transposed(dy_s[...], w_s[...]).astype(BF16)
    ring.take(lane, 0)
    causal = lax.broadcasted_iota(jnp.int32, (block, block), 0) >= lax.broadcasted_iota(jnp.int32, (block, block), 1)
    q_weight = qn_ref[ring.me]
    done = 0
    passed = 1
    for i in range(steps):
        rows = pl.ds(i * block, block)
        q_rows, do_rows = q_ref[rows, :], do_s[rows, :]
        delta = jnp.sum(o32_ref[rows, :] * do_rows.astype(F32), axis=-1, keepdims=True)
        lse = lse_ref[rows, :][:, :1]
        dq = jnp.zeros((block, head_dim), F32)
        for j in range(i + 1):
            keys = pl.ds(j * block, block)
            k_rows, v_rows = k_ref[keys, :], v_ref[keys, :]
            probs = jnp.exp(times_transposed(q_rows, k_rows) * scale - lse)
            if i == j:
                probs = jnp.where(causal, probs, 0.0)
            d_probs = times_transposed(do_rows, v_rows).astype(BF16).astype(F32)
            d_score = (probs * (d_probs - delta) * scale).astype(BF16)
            dv_s[keys, :] += transposed_times(probs.astype(BF16), do_rows)
            dk_s[keys, :] += transposed_times(d_score, q_rows)
            dq = dq + jnp.dot(d_score, k_rows, preferred_element_type=F32)
            done += 1
            if done in (3, 5, 8, 10):
                ring.take(lane, passed)
                passed += 1
        dq_proj, d_weight = head_backward(dq.astype(BF16).astype(F32), qproj_ref[rows, :].astype(F32), q_weight,
                                          cos_ref[rows, :], sin_ref[rows, :])
        rows_s[rows, pl.ds(0, head_dim)] = dq_proj.astype(BF16)
        gq_ref[...] += d_weight

    @pl.when(ring.core == 0)
    def _():
        send_s[...] = dv_s[...].astype(BF16)

    @pl.when(ring.core == 1)
    def _():
        send_s[...] = dk_s[...].astype(BF16)
    swap = pltpu.make_async_remote_copy(send_s, got_s, swap_send, swap_recv, device_id={'sp': ring.partner}, device_id_type=MESH)
    swap.start()
    ring.take(lane, passed)
    passed += 1
    loads[2].wait()
    swap.wait()

    @pl.when(ring.core == 0)
    def _():
        total = (dk_s[...].astype(BF16).astype(F32) + got_s[...].astype(F32)).astype(BF16).astype(F32)
        dk_proj, d_weight = head_backward(total, kproj_ref[...].astype(F32), kn_ref[ring.me // share], cos_ref[...], sin_ref[...])
        rows_s[:, head_dim:] = dk_proj.astype(BF16)
        gk_ref[...] = d_weight

    @pl.when(ring.core == 1)
    def _():
        rows_s[:, head_dim:] = (dv_s[...].astype(BF16).astype(F32) + got_s[...].astype(F32)).astype(BF16)
        gk_ref[...] = jnp.zeros_like(gk_ref)
    ring.take(lane, passed)
    passed += 1
    put_rows = pltpu.make_async_copy(rows_s, rows_out, load_sem.at[3])
    put_rows.start()
    dw_out[...] = transposed_times(n_s[...], rows_s[...]).astype(BF16)
    while passed < ring.chips:
        ring.take(lane, passed)
        passed += 1
    each_peer(lambda hop: o_from(hop).wait_recv())
    put_own = pltpu.make_async_copy(own_s, own_out, load_sem.at[4])
    put_own.start()

    def put_o(slot):
        rows = pl.ds(pl.multiple_of(slot * head_dim, head_dim), head_dim)
        return pltpu.make_async_copy(wo_s.at[slot], wo_out.at[rows, :], out_sem.at[slot])

    def collect(step, carry):
        ring.shared(lane, step)
        put_o(ring.own_slot(step)).start()
        put_o(ring.other_slot(step)).start()
        return carry
    lax.fori_loop(0, ring.chips, collect, 0)
    ring.finish(lane)
    each_peer(lambda hop: o_copy(hop).wait_send())

    def drain(slot, carry):
        put_o(slot).wait()
        return carry
    lax.fori_loop(0, devices, drain, 0)
    put_rows.wait()
    put_own.wait()


def weight_kernel(devices, dwqkv_ref, rows_ref, o_ref, n_ref, dy_ref, hid_ref, dg_ref, du_ref, wq_ref, wk_ref, wv_ref, wo_ref,
                  x_ref, gain_ref, mlp_ref, dn_ref, gq_ref, gk_ref,
                  q_out, k_out, v_out, g_out, u_out, d_out, y_out, dx_out, gain_out, qn_out, kn_out,
                  wqkv_s, n_s, dy_s, nt_s, hid_s, dg_s, du_s, st_g, st_u, st_d, got_s, of_s, df_s, kf_s, vf_s, wq_s, wk_s, wv_s, wo_s, small_s,
                  load_sem, tile_sem, ring_send, ring_recv, pair_send, pair_recv, out_sem, kv_sem,
                  put_sem, swap_send, swap_recv, rows_send, rows_recv, small_send, small_recv):
    ring = Ring(devices)
    lane = (wqkv_s, (ring_send, ring_recv, pair_send, pair_recv), 4)
    model_dim = n_ref.shape[1]
    local_len, head_dim = o_ref.shape[1:]
    half = hid_ref.shape[1]
    tile = st_g.shape[2]
    tiles = half // tile
    num_kv = kn_out.shape[0]
    share = devices // num_kv
    loads = [pltpu.make_async_copy(dwqkv_ref, wqkv_s.at[ring.me], load_sem.at[0]),
             pltpu.make_async_copy(rows_ref.at[ring.me], got_s.at[ring.me], load_sem.at[1]),
             pltpu.make_async_copy(n_ref, n_s, load_sem.at[2]),
             pltpu.make_async_copy(dy_ref, dy_s, load_sem.at[3])]
    late = [pltpu.make_async_copy(src, dst, load_sem.at[4 + i])
            for i, (src, dst) in enumerate(((wo_ref, wo_s), (wq_ref, wq_s), (wk_ref, wk_s), (wv_ref, wv_s)))]
    tile_bufs = ((hid_ref, hid_s), (dg_ref, dg_s), (du_ref, du_s))

    def fetch(i, t):
        cols = pl.ds(pl.multiple_of(t * tile, tile), tile)
        return pltpu.make_async_copy(tile_bufs[i][0].at[:, cols], tile_bufs[i][1].at[t % 2], tile_sem.at[i, t % 2])

    for copy in loads:
        copy.start()
    for i in range(3):
        fetch(i, 0).start()
    ring.barrier_all()
    loads[0].wait()

    def rows_copy(hop):
        return ring.direct(rows_ref.at[ring.peer(hop)], got_s.at[ring.me], rows_send, rows_recv, hop)

    def rows_from(hop):
        source = lax.rem(ring.me + devices - hop, devices)
        return ring.direct(rows_ref.at[source], got_s.at[source], rows_send, rows_recv, hop)

    def small_copy(hop):
        return ring.direct(small_s.at[ring.me], small_s.at[ring.me], small_send, small_recv, hop)

    def small_from(hop):
        source = lax.rem(ring.me + devices - hop, devices)
        return ring.direct(small_s.at[source], small_s.at[source], small_send, small_recv, hop)

    def each_peer(body):
        def step(hop, carry):
            body(hop)
            return carry
        lax.fori_loop(1, devices, step, 0)

    def put_q(slot):
        cols = pl.ds(pl.multiple_of(slot * head_dim, head_dim), head_dim)
        return pltpu.make_async_copy(wqkv_s.at[slot, :, pl.ds(0, head_dim)], q_out.at[:, cols], out_sem.at[slot])

    def put_kv(slot, out):
        cols = pl.ds(pl.multiple_of(slot // share * head_dim, head_dim), head_dim)
        return pltpu.make_async_copy(wqkv_s.at[slot, :, pl.ds(head_dim, head_dim)], out.at[:, cols], kv_sem.at[slot])

    def store(t, i, core):
        st, out = ((st_g, g_out), (st_u, u_out), (st_d, d_out))[i]
        span = pl.ds(pl.multiple_of(core * half + t * tile, tile), tile)
        return st.at[t], (out.at[span, :] if i == 2 else out.at[:, span])

    def put_tile(t, i):
        src, dst = store(t, i, ring.core)
        return pltpu.make_async_copy(src, dst, put_sem.at[i, t])

    def send_tile(t, i, core):
        src, dst = store(t, i, core)
        return pltpu.make_async_remote_copy(src, dst, swap_send.at[i, t], swap_recv.at[i, t],
                                            device_id={'sp': ring.partner}, device_id_type=MESH)

    def finish_forward():
        late[0].wait()
        for h in range(devices):
            of_s[:, h * head_dim:(h + 1) * head_dim] = o_ref[h]
        attn_out = jnp.dot(of_s[...], wo_s[...], preferred_element_type=F32).astype(BF16)
        y_out[...] = (x_ref[...].astype(F32) + attn_out.astype(F32) + mlp_ref[...].astype(F32)).astype(BF16)

    def finish_backward():
        each_peer(lambda hop: rows_from(hop).wait_recv())
        loads[1].wait()
        for h in range(devices):
            df_s[:, h * head_dim:(h + 1) * head_dim] = got_s[h, :, :head_dim]
        for j in range(num_kv):
            kf_s[:, j * head_dim:(j + 1) * head_dim] = got_s[share * j, :, head_dim:]
            vf_s[:, j * head_dim:(j + 1) * head_dim] = got_s[share * j + 1, :, head_dim:]
        for copy in late[1:]:
            copy.wait()
        d_norm = (times_transposed(df_s[...], wq_s[...]) + times_transposed(kf_s[...], wk_s[...])
                  + times_transposed(vf_s[...], wv_s[...]) + dn_ref[...]).astype(BF16).astype(F32)
        unit, inv_std = head_stats(x_ref[...].astype(F32))
        grad_gain = jnp.sum(d_norm * unit, axis=0, keepdims=True)
        d_unit = d_norm * gain_ref[...]
        mean_d = jnp.mean(d_unit, axis=-1, keepdims=True)
        mean_du = jnp.mean(d_unit * unit, axis=-1, keepdims=True)
        dx = inv_std * (d_unit - mean_d - unit * mean_du)
        own_rows = pl.ds(pl.multiple_of(ring.me * local_len, local_len), local_len)
        dx_out[...] = (dy_s[own_rows, :].astype(F32) + dx).astype(BF16)
        gains = model_dim // head_dim
        parts = [grad_gain[:, c * head_dim:(c + 1) * head_dim] for c in range(gains)] + [gq_ref[...], gk_ref[...]]
        pad = jnp.zeros((small_s.shape[1] - len(parts), head_dim), F32)
        small_s[ring.me] = jnp.concatenate(parts + [pad], axis=0)

    def step_body(step, carry):
        ring.take(lane, step, (0, 1))

        @pl.when(step == 0)
        def _():
            each_peer(lambda hop: rows_copy(hop).start())
            loads[2].wait()

            def turn(i, inner):
                rows = pl.ds(pl.multiple_of(i * 256, 256), 256)
                nt_s[:, rows] = n_s[rows, :].T
                return inner
            lax.fori_loop(0, n_s.shape[0] // 256, turn, 0)
            loads[3].wait()

        piece = model_dim // 4

        @pl.when(step < tiles)
        def _():
            for i in range(3):
                fetch(i, step).wait()

            @pl.when(step + 1 < tiles)
            def _():
                for i in range(3):
                    fetch(i, step + 1).start()

            def in_weights(i, inner):
                rows = pl.ds(pl.multiple_of(i * piece, piece), piece)
                st_g[step, rows, :] = jnp.dot(nt_s[rows, :], dg_s[step % 2], preferred_element_type=F32).astype(BF16)
                st_u[step, rows, :] = jnp.dot(nt_s[rows, :], du_s[step % 2], preferred_element_type=F32).astype(BF16)
                return inner
            lax.fori_loop(0, 4, in_weights, 0)

        ring.take(lane, step, (2, 3))

        @pl.when(step < tiles)
        def _():
            st_d[step] = transposed_times(hid_s[step % 2], dy_s[...]).astype(BF16)

        @pl.when(step == 1)
        def _():
            for copy in late:
                copy.start()

        @pl.when(step == tiles)
        def _():
            finish_forward()

        @pl.when(step == tiles + 1)
        def _():
            finish_backward()

        ring.shared(lane, step)
        for slot in (ring.own_slot(step), ring.other_slot(step)):
            put_q(slot).start()

            @pl.when(slot % 2 == 0)
            def _():
                put_kv(slot, k_out).start()

            @pl.when(slot % 2 == 1)
            def _():
                put_kv(slot, v_out).start()

        @pl.when(jnp.logical_and(step > 0, step <= tiles))
        def _():
            for i in range(3):
                put_tile(step - 1, i).start()
                send_tile(step - 1, i, ring.core).start()
        return carry

    lax.fori_loop(0, ring.chips, step_body, 0)
    each_peer(lambda hop: small_copy(hop).start())
    ring.finish(lane)

    def drain(slot, carry):
        put_q(slot).wait()
        put_kv(slot, k_out).wait()
        return carry
    lax.fori_loop(0, devices, drain, 0)

    def drain_tiles(t, carry):
        for i in range(3):
            put_tile(t, i).wait()
            send_tile(t, i, ring.core).wait_send()
            send_tile(t, i, 1 - ring.core).wait_recv()
        return carry
    lax.fori_loop(0, tiles, drain_tiles, 0)
    each_peer(lambda hop: rows_copy(hop).wait_send())
    each_peer(lambda hop: small_from(hop).wait_recv())
    each_peer(lambda hop: small_copy(hop).wait_send())
    gains = model_dim // head_dim
    total = small_s[0, :gains]
    for h in range(1, devices):
        total = total + small_s[h, :gains]
    gain_out[...] = total
    qn_out[...] = jnp.concatenate([small_s[h, gains:gains + 1] for h in range(devices)], axis=0)
    kn_out[...] = jnp.concatenate([small_s[share * j, gains + 1:gains + 2] for j in range(num_kv)], axis=0)


def whole(shape):
    return pl.BlockSpec(shape, lambda *_: (0,) * len(shape))


def solution(mesh):
    group_devices = mesh.shape['sp']
    seq_spec = P('dp', 'sp', None)
    grad_spec = P('dp', None)
    def layer_step(x_in, grad_y, positions, w_q, w_k, w_v, w_o, w_gate, w_up, w_down, norm_gain, q_norm, k_norm):
        batch_rows, local_len, model_dim = x_in.shape
        num_heads, head_dim = q_norm.shape
        num_kv = k_norm.shape[0]
        share = num_heads // num_kv
        ffn_dim = w_gate.shape[1]
        seq_len = local_len * group_devices
        me = lax.axis_index('sp')
        idx = jnp.stack([me, me // share, me % 2]).astype(jnp.int32)
        params = pltpu.CompilerParams(vmem_limit_bytes=VMEM_LIMIT)
        hbm = pl.BlockSpec(memory_space=pl.ANY)

        def call(kernel, name, flops, bytes_accessed, grid, in_specs, out_specs, out_shape, scratch, aliases=None):
            return pl.pallas_call(
                kernel, out_shape=out_shape, name=name, compiler_params=params, input_output_aliases=aliases or {},
                cost_estimate=pl.CostEstimate(flops=flops, bytes_accessed=bytes_accessed, transcendentals=0),
                grid_spec=pltpu.PrefetchScalarGridSpec(num_scalar_prefetch=1, grid=grid, in_specs=in_specs, out_specs=out_specs,
                                                       scratch_shapes=scratch))

        x_rows = x_in.reshape(local_len, model_dim)
        gain_row = norm_gain.reshape(1, model_dim)
        grad_flat = grad_y.reshape(local_len, model_dim)
        half = ffn_dim // 2
        dma = pltpu.SemaphoreType.DMA
        chips = group_devices // 2
        ring_sems = lambda lanes: [dma((lanes, chips))] * 4
        struct = jax.ShapeDtypeStruct
        vmem = pltpu.VMEM
        in_vmem = pl.BlockSpec(memory_space=pltpu.VMEM)
        acts = (group_devices, local_len, half)
        blocks = (group_devices, local_len, model_dim)
        pos_rows = jnp.broadcast_to(positions.reshape(1, local_len), (8, local_len))
        freq, sign = rope_lanes(head_dim)
        rope = struct((group_devices, local_len, head_dim), F32)
        n_all, dy_all, cos_t, sin_t, hid, d_gate, d_up, mlp_out, d_norm_mlp = pl.pallas_call(
            functools.partial(gather_kernel, group_devices), name="gather_tokens",
            out_shape=[struct(blocks, BF16), struct(blocks, BF16), rope, rope]
            + [struct(acts, BF16)] * 3 + [struct((local_len, model_dim), BF16), struct((local_len, model_dim), F32)],
            in_specs=[in_vmem] * 4 + [hbm] * 5, out_specs=[hbm] * 2 + [in_vmem] * 2 + [hbm] * 3 + [in_vmem] * 2,
            scratch_shapes=[vmem(blocks, BF16), vmem(blocks, BF16), vmem((group_devices, 8, local_len), jnp.int32),
                            vmem((model_dim, half), BF16), vmem((model_dim, half), BF16), vmem((half, model_dim), BF16)]
            + [vmem(acts, BF16)] * 3 + [vmem((2 * local_len, half), F32)] * 2 + [vmem((2, local_len, model_dim), F32)] * 3
            + [dma((3,)), dma((3,))] + ring_sems(1) + ring_sems(2) * 2 + [dma((3, group_devices)), dma((3, group_devices)), dma(()), dma(())],
            compiler_params=pltpu.CompilerParams(collective_id=0, has_side_effects=True, vmem_limit_bytes=VMEM_LIMIT),
            cost_estimate=pl.CostEstimate(flops=40_000_000_000, bytes_accessed=40_000_000, transcendentals=0),
        )(x_rows, gain_row, freq, sign, grad_flat, pos_rows, w_gate, w_up, w_down)
        n_all, dy_all = n_all.reshape(seq_len, model_dim), dy_all.reshape(seq_len, model_dim)
        hid, d_gate, d_up = (act.reshape(seq_len, half) for act in (hid, d_gate, d_up))
        cos_t, sin_t = cos_t.reshape(seq_len, head_dim), sin_t.reshape(seq_len, head_dim)

        vec = jax.ShapeDtypeStruct((1, head_dim), F32)
        rows_bf = jax.ShapeDtypeStruct((seq_len, head_dim), BF16)
        rows_f32 = jax.ShapeDtypeStruct((seq_len, head_dim), F32)
        rows = whole((seq_len, head_dim))
        head_cols = pl.BlockSpec((model_dim, head_dim), lambda g, s: (0, s[0]))
        kv_cols = pl.BlockSpec((model_dim, head_dim), lambda g, s: (0, s[1]))
        head_rows = pl.BlockSpec((head_dim, model_dim), lambda g, s: (s[0], 0))
        head_vec = pl.BlockSpec((1, 1, head_dim), lambda g, s: (s[0], 0, 0))
        kv_vec = pl.BlockSpec((1, 1, head_dim), lambda g, s: (s[1], 0, 0))
        tokens = whole((seq_len, model_dim))
        block = 512
        qn3 = q_norm.reshape(num_heads, 1, head_dim)
        kn3 = k_norm.reshape(num_kv, 1, head_dim)

        o_h, o32, lse, q_rot, k_rot, v_h, q_proj, k_proj = call(
            functools.partial(forward_kernel, block), "attention_fwd", 10_000_000_000, 12_000_000, (1,),
            [tokens, head_cols, kv_cols, kv_cols, head_vec, kv_vec, rows, rows], [rows] * 8,
            [rows_bf, rows_f32, rows_f32] + [rows_bf] * 5, [pltpu.VMEM((block, seq_len), F32)],
        )(idx, n_all, w_q, w_k, w_v, qn3, kn3, cos_t, sin_t)

        heads = struct((group_devices, local_len, head_dim), BF16)
        d_rows, dwqkv_h, dw_o, attn_own, gq, gk = pl.pallas_call(
            functools.partial(backward_kernel, group_devices, block), name="attention_bwd",
            out_shape=[struct((seq_len, 2 * head_dim), BF16), struct((model_dim, 2 * head_dim), BF16), struct(w_o.shape, BF16), heads, vec, vec],
            in_specs=[hbm] * 3 + [in_vmem] * 12, out_specs=[hbm, in_vmem, hbm, hbm, in_vmem, in_vmem],
            scratch_shapes=[vmem((seq_len, model_dim), BF16)] * 2 + [vmem((head_dim, model_dim), BF16), vmem((group_devices, head_dim, model_dim), BF16)]
            + [vmem((seq_len, head_dim), BF16)] + [vmem((seq_len, head_dim), F32)] * 2 + [vmem((seq_len, head_dim), BF16)] * 2
            + [vmem((seq_len, 2 * head_dim), BF16), vmem(heads.shape, BF16), dma((5,))] + ring_sems(2) + [dma((group_devices,)), dma(()), dma(())] + [dma((group_devices,))] * 2,
            compiler_params=pltpu.CompilerParams(collective_id=2, has_side_effects=True, vmem_limit_bytes=VMEM_LIMIT),
            cost_estimate=pl.CostEstimate(flops=30_000_000_000, bytes_accessed=30_000_000, transcendentals=0),
        )(dy_all, n_all, w_o, o_h, o32, lse, q_rot, k_rot, v_h, q_proj, k_proj, qn3, kn3, cos_t, sin_t)

        tile = 256
        tiles = half // tile
        tile_in = (tiles, model_dim, tile)
        gain_shape = (model_dim // head_dim, head_dim)
        flat = (local_len, num_heads * head_dim)
        flat_kv = (local_len, num_kv * head_dim)
        dw_q, dw_k, dw_v, dw_gate, dw_up, dw_down, y_out, grad_x, grad_gain, grad_q_norm, grad_k_norm = pl.pallas_call(
            functools.partial(weight_kernel, group_devices), name="gather_weights",
            out_shape=[struct(w.shape, BF16) for w in (w_q, w_k, w_v, w_gate, w_up, w_down)]
            + [struct((local_len, model_dim), BF16)] * 2 + [struct(gain_shape, F32), struct(q_norm.shape, F32), struct(k_norm.shape, F32)],
            in_specs=[hbm, hbm, in_vmem] + [hbm] * 9 + [in_vmem] * 6, out_specs=[hbm] * 6 + [in_vmem] * 5,
            scratch_shapes=[vmem((group_devices, model_dim, 2 * head_dim), BF16),
                            vmem((seq_len, model_dim), BF16), vmem((seq_len, model_dim), BF16), vmem((model_dim, seq_len), BF16)]
            + [vmem((2, seq_len, tile), BF16)] * 3 + [vmem(tile_in, BF16), vmem(tile_in, BF16), vmem((tiles, tile, model_dim), BF16)]
            + [vmem((group_devices, local_len, 2 * head_dim), BF16), vmem(flat, BF16), vmem(flat, BF16), vmem(flat_kv, BF16), vmem(flat_kv, BF16)]
            + [vmem(w.shape, BF16) for w in (w_q, w_k, w_v, w_o)] + [vmem((group_devices, 16, head_dim), F32)]
            + [dma((8,)), dma((3, 2))] + ring_sems(4) + [dma((group_devices,))] * 2 + [dma((3, tiles))] * 3 + [dma((group_devices,))] * 4,
            compiler_params=pltpu.CompilerParams(collective_id=1, has_side_effects=True, vmem_limit_bytes=VMEM_LIMIT),
            cost_estimate=pl.CostEstimate(flops=60_000_000_000, bytes_accessed=60_000_000, transcendentals=0),
        )(dwqkv_h, d_rows.reshape(group_devices, local_len, 2 * head_dim), attn_own, n_all, dy_all, hid, d_gate, d_up,
          w_q, w_k, w_v, w_o, x_rows, gain_row, mlp_out, d_norm_mlp, gq, gk)
        grad_gain = grad_gain.reshape(model_dim)
        return (y_out.reshape(x_in.shape), grad_x.reshape(x_in.shape), dw_q, dw_k, dw_v, dw_o, dw_gate, dw_up, dw_down,
                grad_gain, grad_q_norm, grad_k_norm)

    in_specs = (seq_spec, seq_spec, P(('dp', 'sp'))) + (P(),) * 10
    out_specs = (seq_spec, seq_spec) + (grad_spec,) * 7 + (P('dp'), grad_spec, grad_spec)
    return jax.shard_map(layer_step, mesh=mesh, in_specs=in_specs, out_specs=out_specs, check_vma=False)
```

```python
import functools

import jax
import jax.numpy as jnp
from jax import lax
from jax.experimental import pallas as pl
from jax.experimental.pallas import tpu as pltpu
from jax.sharding import PartitionSpec as P

NORM_EPS = 1e-5
ROPE_THETA = 75.0e6
VMEM_LIMIT = 63 * 1024 * 1024
F32 = jnp.float32
BF16 = jnp.bfloat16
MESH = pl.DeviceIdType.MESH


def input_norm(x_f32, norm_gain):
    row_mean = jnp.mean(x_f32, axis=-1, keepdims=True)
    centered = x_f32 - row_mean
    row_var = jnp.mean(centered * centered, axis=-1, keepdims=True)
    return (centered * lax.rsqrt(row_var + NORM_EPS) * norm_gain).astype(BF16)


def swiglu(gate_pre, up_proj):
    return (jax.nn.silu(gate_pre) * up_proj).astype(BF16)


def times_transposed(lhs_mat, rhs_mat):
    return lax.dot_general(lhs_mat, rhs_mat, (((1,), (1,)), ((), ())), preferred_element_type=F32)


def transposed_times(lhs_mat, rhs_mat):
    return lax.dot_general(lhs_mat, rhs_mat, (((0,), (0,)), ((), ())), preferred_element_type=F32)


def rope_lanes(head_dim):
    pair_index = jnp.arange(head_dim, dtype=jnp.int32) // 2
    inv_freq = ROPE_THETA ** (-(pair_index.astype(F32) * 2.0) / head_dim)
    sign = jnp.where(jnp.arange(head_dim) % 2 == 0, -1.0, 1.0).astype(F32)
    return inv_freq[None, :], sign[None, :]


def swap_pairs(rows):
    lane = lax.broadcasted_iota(jnp.int32, rows.shape, 1)
    width = rows.shape[1]
    return jnp.where(lane % 2 == 0, pltpu.roll(rows, width - 1, 1), pltpu.roll(rows, 1, 1))


def head_stats(proj_f32):
    row_mean = jnp.mean(proj_f32, axis=-1, keepdims=True)
    centered = proj_f32 - row_mean
    inv_std = lax.rsqrt(jnp.mean(centered * centered, axis=-1, keepdims=True) + NORM_EPS)
    return centered * inv_std, inv_std


def head_forward(proj_f32, weight, cos_t, sin_t):
    unit, _ = head_stats(proj_f32)
    normed = unit * weight
    return (normed * cos_t + swap_pairs(normed) * sin_t).astype(BF16)


def head_backward(d_rot, proj_f32, weight, cos_t, sin_t):
    unit, inv_std = head_stats(proj_f32)
    d_normed = d_rot * cos_t + swap_pairs(d_rot * sin_t)
    d_weight = jnp.sum(d_normed * unit, axis=0, keepdims=True)
    d_unit = d_normed * weight
    mean_d = jnp.mean(d_unit, axis=-1, keepdims=True)
    mean_du = jnp.mean(d_unit * unit, axis=-1, keepdims=True)
    return inv_std * (d_unit - mean_d - unit * mean_du), d_weight


def forward_kernel(block, idx_ref, n_s, wq_ref, wk_ref, wv_ref, qn_ref, kn_ref, cos_ref, sin_ref,
                   o_ref, o32_ref, lse_ref, q_ref, k_ref, v_ref, qproj_ref, kproj_ref, e_s):
    seq_len, head_dim = o_ref.shape
    steps = seq_len // block
    scale = head_dim ** -0.5

    def project(i, carry):
        rows = pl.ds(pl.multiple_of(i * block, block), block)
        n_rows = n_s[rows, :]
        weights = jnp.concatenate([wq_ref[...], wk_ref[...], wv_ref[...]], axis=1)
        proj = jnp.dot(n_rows, weights, preferred_element_type=F32).astype(BF16)
        q_proj, k_proj = proj[:, :head_dim], proj[:, head_dim:2 * head_dim]
        qproj_ref[rows, :] = q_proj
        kproj_ref[rows, :] = k_proj
        v_ref[rows, :] = proj[:, 2 * head_dim:]
        cos_t, sin_t = cos_ref[rows, :], sin_ref[rows, :]
        q_ref[rows, :] = head_forward(q_proj.astype(F32), qn_ref[0], cos_t, sin_t)
        k_ref[rows, :] = head_forward(k_proj.astype(F32), kn_ref[0], cos_t, sin_t)
        return carry

    lax.fori_loop(0, steps, project, 0)
    causal = lax.broadcasted_iota(jnp.int32, (block, block), 0) >= lax.broadcasted_iota(jnp.int32, (block, block), 1)

    def lanes(op, tile):
        return functools.reduce(op, [tile[:, c:c + 128] for c in range(0, block, 128)])

    def keys_of(j):
        return pl.ds(pl.multiple_of(j * block, block), block)

    def query_block(i, carry):
        rows = keys_of(i)
        q_rows = q_ref[rows, :]

        def score(j, top):
            tile = times_transposed(q_rows, k_ref[keys_of(j), :])
            e_s[:, keys_of(j)] = tile
            return jnp.maximum(top, lanes(jnp.maximum, tile))

        top = lax.fori_loop(0, i, score, jnp.full((block, 128), -1e30, F32))
        diag = jnp.where(causal, times_transposed(q_rows, k_ref[rows, :]), -1e30)
        e_s[:, rows] = diag
        top = jnp.max(jnp.maximum(top, lanes(jnp.maximum, diag)), axis=-1, keepdims=True)

        def exponent(j, total):
            tile = jnp.exp((e_s[:, keys_of(j)] - top) * scale)
            e_s[:, keys_of(j)] = tile
            return total + lanes(jnp.add, tile)

        total = lax.fori_loop(0, i + 1, exponent, jnp.zeros((block, 128), F32))
        total = jnp.sum(total, axis=-1, keepdims=True)
        inv_total = 1.0 / total

        def attend(j, acc):
            probs = (e_s[:, keys_of(j)] * inv_total).astype(BF16)
            return acc + jnp.dot(probs, v_ref[keys_of(j), :], preferred_element_type=F32)

        out = lax.fori_loop(0, i + 1, attend, jnp.zeros((block, head_dim), F32))
        o_ref[rows, :] = out.astype(BF16)
        o32_ref[rows, :] = out
        lse_ref[rows, :] = jnp.broadcast_to(top * scale + jnp.log(total), (block, 128))
        return carry

    lax.fori_loop(0, steps, query_block, 0)


class Ring:
    def __init__(self, devices):
        self.chips = devices // 2
        self.me = lax.axis_index('sp')
        self.z, self.core = self.me // 2, self.me % 2
        self.turn = 1 - 2 * self.core
        self.partner = self.me + self.turn
        self.after = self.device(self.z + self.turn, self.core)
        self.before = self.device(self.z - self.turn, self.core)

    def device(self, z, core):
        return 2 * lax.rem(z + 2 * self.chips, self.chips) + core

    def own_slot(self, step):
        return self.device(self.z - self.turn * step, self.core)

    def other_slot(self, step):
        return self.device(self.z + self.turn * step, 1 - self.core)

    def barrier(self):
        sem = pltpu.get_barrier_semaphore()
        for device in (self.after, self.before, self.partner):
            pl.semaphore_signal(sem, inc=1, device_id={'sp': device}, device_id_type=MESH)
        pl.semaphore_wait(sem, 3)

    def barrier_all(self):
        sem = pltpu.get_barrier_semaphore()

        def signal(hop, carry):
            pl.semaphore_signal(sem, inc=1, device_id={'sp': self.peer(hop)}, device_id_type=MESH)
            return carry
        lax.fori_loop(1, 2 * self.chips, signal, 0)
        pl.semaphore_wait(sem, 2 * self.chips - 1)

    def peer(self, hop):
        return lax.rem(self.me + hop, 2 * self.chips)

    def direct(self, src, dst, send, recv, hop):
        return pltpu.make_async_remote_copy(src, dst, send.at[hop], recv.at[hop],
                                            device_id={'sp': self.peer(hop)}, device_id_type=MESH)

    def part(self, buf, slot, parts, k):
        rows = buf.shape[1] // parts
        return buf.at[slot, pl.ds(k * rows, rows)]

    def forward(self, lane, k, step):
        buf, sems, parts = lane
        piece = self.part(buf, self.own_slot(step), parts, k)
        return pltpu.make_async_remote_copy(piece, piece, sems[0].at[k, step], sems[1].at[k, step + 1],
                                            device_id={'sp': self.after}, device_id_type=MESH)

    def share(self, lane, k, step):
        buf, sems, parts = lane
        piece = self.part(buf, self.own_slot(step), parts, k)
        return pltpu.make_async_remote_copy(piece, piece, sems[2].at[k, step], sems[3].at[k, step],
                                            device_id={'sp': self.partner}, device_id_type=MESH)

    def arrived(self, lane, k, step):
        buf, sems, parts = lane
        piece = self.part(buf, self.own_slot(step), parts, k)
        return pltpu.make_async_remote_copy(piece, piece, sems[0].at[k, step], sems[1].at[k, step],
                                            device_id={'sp': self.before}, device_id_type=MESH)

    def shared(self, lane, step):
        buf, sems, parts = lane
        for k in range(parts):
            piece = self.part(buf, self.other_slot(step), parts, k)
            pltpu.make_async_remote_copy(piece, piece, sems[2].at[k, step], sems[3].at[k, step],
                                         device_id={'sp': self.partner}, device_id_type=MESH).wait_recv()

    def take(self, lane, step, ks=None):
        for k in range(lane[2]) if ks is None else ks:
            @pl.when(step > 0)
            def _():
                self.arrived(lane, k, step).wait_recv()

            @pl.when(step < self.chips - 1)
            def _():
                self.forward(lane, k, step).start()
            self.share(lane, k, step).start()

    def finish(self, lane):
        def body(step, carry):
            for k in range(lane[2]):
                @pl.when(step < self.chips - 1)
                def _():
                    self.forward(lane, k, step).wait_send()
                self.share(lane, k, step).wait_send()
            return carry
        lax.fori_loop(0, self.chips, body, 0)


def gather_kernel(devices, x_ref, gain_ref, freq_ref, sign_ref, dy_ref, pos_ref, wg_ref, wu_ref, wd_ref,
                  n_out, dy_out, cos_out, sin_out, hid_out, dg_out, du_out, mlp_out, dn_out,
                  n_s, dy_s, pos_s, wg_s, wu_s, wd_s, hid_s, dg_s, du_s, gate_s, up_s, part_s, got_s, mine_s,
                  load_sem, weight_sem, *sem_refs):
    ring = Ring(devices)
    out_sem, act_sem, swap_send, swap_recv = sem_refs[12:]
    p_lane, n_lane, dy_lane = ((buf, sem_refs[4 * i:4 * i + 4], parts) for i, (buf, parts) in enumerate(((pos_s, 1), (n_s, 2), (dy_s, 2))))
    half = wg_s.shape[1]
    lanes = ((pos_s, pos_ref, None), (n_s, None, n_out), (dy_s, dy_ref, dy_out))
    loads = [pltpu.make_async_copy(src, buf.at[ring.me], load_sem.at[i]) for i, (buf, src, _) in enumerate(lanes) if src is not None]
    columns = pl.ds(pl.multiple_of(ring.core * half, half), half)
    weights = [pltpu.make_async_copy(wg_ref.at[:, columns], wg_s, weight_sem.at[0]),
               pltpu.make_async_copy(wu_ref.at[:, columns], wu_s, weight_sem.at[1]),
               pltpu.make_async_copy(wd_ref.at[columns, :], wd_s, weight_sem.at[2])]
    for copy in loads + weights:
        copy.start()
    n_s[ring.me] = input_norm(x_ref[...].astype(F32), gain_ref[...])
    ring.barrier()
    for copy in loads:
        copy.wait()

    tile = 512
    acts = ((hid_s, hid_out), (dg_s, dg_out), (du_s, du_out))

    def put(lane, slot):
        buf, _, out = lanes[lane]
        return pltpu.make_async_copy(buf.at[slot], out.at[slot], out_sem.at[lane, slot])

    def put_act(i, slot):
        return pltpu.make_async_copy(acts[i][0].at[slot], acts[i][1].at[slot], act_sem.at[i, slot])

    def gate_up(step):
        mine, other = ring.own_slot(step), ring.other_slot(step)

        def body(j, inner):
            cols = pl.ds(pl.multiple_of(j * tile, tile), tile)
            n_rows = jnp.concatenate([n_s[mine], n_s[other]], axis=0)
            gate_s[:, cols] = jnp.dot(n_rows, wg_s[:, cols], preferred_element_type=F32)
            up_s[:, cols] = jnp.dot(n_rows, wu_s[:, cols], preferred_element_type=F32)
            return inner
        lax.fori_loop(0, half // tile, body, 0)

    def hidden(step):
        mine, other = ring.own_slot(step), ring.other_slot(step)

        def body(j, inner):
            cols = pl.ds(pl.multiple_of(j * tile, tile), tile)
            dy_rows = jnp.concatenate([dy_s[mine], dy_s[other]], axis=0)
            d_hidden = times_transposed(dy_rows, wd_s[cols, :]).astype(BF16).astype(F32)
            gate, up = gate_s[:, cols], up_s[:, cols]
            sig = jax.nn.sigmoid(gate)
            silu = gate * sig
            hid = (silu * up).astype(BF16)
            d_up = (d_hidden * silu).astype(BF16)
            d_gate = (d_hidden * up * (sig * (1.0 + gate * (1.0 - sig)))).astype(BF16)
            rows = hid.shape[0] // 2
            for buf, value in ((hid_s, hid), (dg_s, d_gate), (du_s, d_up)):
                buf[mine, :, cols] = value[:rows]
                buf[other, :, cols] = value[rows:]
            return inner
        lax.fori_loop(0, half // tile, body, 0)

    def tables(step):
        for slot in (ring.own_slot(step), ring.other_slot(step)):
            angles = pos_s[slot].astype(F32).T[:, :1] * freq_ref[...]
            cos_out[slot] = jnp.cos(angles)
            sin_out[slot] = jnp.sin(angles) * sign_ref[...]

    def put_acts(step):
        for i in range(3):
            put_act(i, ring.own_slot(step)).start()
            put_act(i, ring.other_slot(step)).start()

    swap = pltpu.make_async_remote_copy(part_s, got_s, swap_send, swap_recv, device_id={'sp': ring.partner}, device_id_type=MESH)

    def own_tokens(step):
        for k, (slot, keep) in enumerate(((ring.partner, part_s), (ring.me, mine_s))):
            @pl.when(step == 3 * k + 2)
            def _():
                keep[0] = jnp.dot(hid_s[slot], wd_s[...], preferred_element_type=F32)

            @pl.when(step == 3 * k + 3)
            def _():
                keep[1] = times_transposed(dg_s[slot], wg_s[...])

            @pl.when(step == 3 * k + 4)
            def _():
                keep[1] += times_transposed(du_s[slot], wu_s[...])

        @pl.when(step == 5)
        def _():
            swap.start()

    def settle(lane, i, step):
        ring.shared(lane, step)
        put(i, ring.own_slot(step)).start()
        put(i, ring.other_slot(step)).start()

    def step_body(step, carry):
        ring.take(n_lane, step)
        ring.take(p_lane, step)

        @pl.when(step == 1)
        def _():
            weights[0].wait()
            weights[1].wait()

        @pl.when(step > 0)
        def _():
            settle(n_lane, 1, step - 1)
            gate_up(step - 1)
            ring.shared(p_lane, step - 1)
            tables(step - 1)

        @pl.when(step > 1)
        def _():
            put_acts(step - 2)
        ring.take(dy_lane, step)

        @pl.when(step == 1)
        def _():
            weights[2].wait()

        @pl.when(step > 0)
        def _():
            settle(dy_lane, 2, step - 1)
            hidden(step - 1)
        own_tokens(step)
        return carry

    lax.fori_loop(0, ring.chips, step_body, 0)
    last = ring.chips - 1
    settle(n_lane, 1, last)
    gate_up(last)
    put_acts(last - 1)
    settle(dy_lane, 2, last)
    hidden(last)
    ring.shared(p_lane, last)
    tables(last)
    own_tokens(last + 1)
    put_acts(last)
    for lane in (p_lane, n_lane, dy_lane):
        ring.finish(lane)

    def drain(slot, carry):
        for lane in (1, 2):
            put(lane, slot).wait()
        for i in range(3):
            put_act(i, slot).wait()
        return carry
    lax.fori_loop(0, devices, drain, 0)
    swap.wait()
    mlp_out[...] = (mine_s[0] + got_s[0]).astype(BF16)
    dn_out[...] = mine_s[1] + got_s[1]


def backward_kernel(devices, block, dy_ref, n_ref, wo_ref, o_ref, o32_ref, lse_ref, q_ref, k_ref, v_ref, qproj_ref, kproj_ref,
                    qn_ref, kn_ref, cos_ref, sin_ref,
                    rows_out, dw_out, wo_out, own_out, gq_ref, gk_ref,
                    dy_s, n_s, w_s, wo_s, do_s, dk_s, dv_s, send_s, got_s, rows_s, own_s,
                    load_sem, ring_send, ring_recv, pair_send, pair_recv, out_sem, swap_send, swap_recv, o_send, o_recv):
    ring = Ring(devices)
    lane = (wo_s, (ring_send, ring_recv, pair_send, pair_recv), 4)
    seq_len, head_dim = do_s.shape
    steps = seq_len // block
    scale = head_dim ** -0.5
    share = devices // kn_ref.shape[0]
    w_rows = pl.ds(pl.multiple_of(ring.me * head_dim, head_dim), head_dim)
    loads = [pltpu.make_async_copy(dy_ref, dy_s, load_sem.at[0]), pltpu.make_async_copy(wo_ref.at[w_rows, :], w_s, load_sem.at[1]),
             pltpu.make_async_copy(n_ref, n_s, load_sem.at[2])]
    for copy in loads:
        copy.start()
    ring.barrier_all()
    local_len = seq_len // devices

    def tokens_of(device):
        return pl.ds(pl.multiple_of(device * local_len, local_len), local_len)

    def o_copy(hop):
        return ring.direct(o_ref.at[tokens_of(ring.peer(hop)), :], own_s.at[ring.me], o_send, o_recv, hop)

    def o_from(hop):
        source = lax.rem(ring.me + devices - hop, devices)
        return ring.direct(o_ref.at[tokens_of(source), :], own_s.at[source], o_send, o_recv, hop)

    def each_peer(body):
        def step(hop, carry):
            body(hop)
            return carry
        lax.fori_loop(1, devices, step, 0)

    each_peer(lambda hop: o_copy(hop).start())
    own_s[ring.me] = o_ref[tokens_of(ring.me), :]
    dk_s[...] = jnp.zeros_like(dk_s)
    dv_s[...] = jnp.zeros_like(dv_s)
    gq_ref[...] = jnp.zeros_like(gq_ref)
    loads[0].wait()
    wo_s[ring.me] = transposed_times(o_ref[...], dy_s[...]).astype(BF16)
    loads[1].wait()
    do_s[...] = times_transposed(dy_s[...], w_s[...]).astype(BF16)
    ring.take(lane, 0)
    causal = lax.broadcasted_iota(jnp.int32, (block, block), 0) >= lax.broadcasted_iota(jnp.int32, (block, block), 1)
    q_weight = qn_ref[ring.me]
    done = 0
    passed = 1
    for i in range(steps):
        rows = pl.ds(i * block, block)
        q_rows, do_rows = q_ref[rows, :], do_s[rows, :]
        delta = jnp.sum(o32_ref[rows, :] * do_rows.astype(F32), axis=-1, keepdims=True)
        lse = lse_ref[rows, :][:, :1]
        dq = jnp.zeros((block, head_dim), F32)
        for j in range(i + 1):
            keys = pl.ds(j * block, block)
            k_rows, v_rows = k_ref[keys, :], v_ref[keys, :]
            probs = jnp.exp(times_transposed(q_rows, k_rows) * scale - lse)
            if i == j:
                probs = jnp.where(causal, probs, 0.0)
            d_probs = times_transposed(do_rows, v_rows).astype(BF16).astype(F32)
            d_score = (probs * (d_probs - delta) * scale).astype(BF16)
            dv_s[keys, :] += transposed_times(probs.astype(BF16), do_rows)
            dk_s[keys, :] += transposed_times(d_score, q_rows)
            dq = dq + jnp.dot(d_score, k_rows, preferred_element_type=F32)
            done += 1
            if done % 2 == 0:
                ring.take(lane, passed)
                passed += 1
        dq_proj, d_weight = head_backward(dq.astype(BF16).astype(F32), qproj_ref[rows, :].astype(F32), q_weight,
                                          cos_ref[rows, :], sin_ref[rows, :])
        rows_s[rows, pl.ds(0, head_dim)] = dq_proj.astype(BF16)
        gq_ref[...] += d_weight

    @pl.when(ring.core == 0)
    def _():
        send_s[...] = dv_s[...].astype(BF16)

    @pl.when(ring.core == 1)
    def _():
        send_s[...] = dk_s[...].astype(BF16)
    swap = pltpu.make_async_remote_copy(send_s, got_s, swap_send, swap_recv, device_id={'sp': ring.partner}, device_id_type=MESH)
    swap.start()
    ring.take(lane, passed)
    passed += 1
    loads[2].wait()
    swap.wait()

    @pl.when(ring.core == 0)
    def _():
        total = (dk_s[...].astype(BF16).astype(F32) + got_s[...].astype(F32)).astype(BF16).astype(F32)
        dk_proj, d_weight = head_backward(total, kproj_ref[...].astype(F32), kn_ref[ring.me // share], cos_ref[...], sin_ref[...])
        rows_s[:, head_dim:] = dk_proj.astype(BF16)
        gk_ref[...] = d_weight

    @pl.when(ring.core == 1)
    def _():
        rows_s[:, head_dim:] = (dv_s[...].astype(BF16).astype(F32) + got_s[...].astype(F32)).astype(BF16)
        gk_ref[...] = jnp.zeros_like(gk_ref)
    ring.take(lane, passed)
    passed += 1
    put_rows = pltpu.make_async_copy(rows_s, rows_out, load_sem.at[3])
    put_rows.start()
    dw_out[...] = transposed_times(n_s[...], rows_s[...]).astype(BF16)
    while passed < ring.chips:
        ring.take(lane, passed)
        passed += 1
    each_peer(lambda hop: o_from(hop).wait_recv())
    put_own = pltpu.make_async_copy(own_s, own_out, load_sem.at[4])
    put_own.start()

    def put_o(slot):
        rows = pl.ds(pl.multiple_of(slot * head_dim, head_dim), head_dim)
        return pltpu.make_async_copy(wo_s.at[slot], wo_out.at[rows, :], out_sem.at[slot])

    def collect(step, carry):
        ring.shared(lane, step)
        put_o(ring.own_slot(step)).start()
        put_o(ring.other_slot(step)).start()
        return carry
    lax.fori_loop(0, ring.chips, collect, 0)
    ring.finish(lane)
    each_peer(lambda hop: o_copy(hop).wait_send())

    def drain(slot, carry):
        put_o(slot).wait()
        return carry
    lax.fori_loop(0, devices, drain, 0)
    put_rows.wait()
    put_own.wait()


def weight_kernel(devices, dwqkv_ref, rows_ref, o_ref, n_ref, dy_ref, hid_ref, dg_ref, du_ref, wq_ref, wk_ref, wv_ref, wo_ref,
                  x_ref, gain_ref, mlp_ref, dn_ref, gq_ref, gk_ref,
                  q_out, k_out, v_out, g_out, u_out, d_out, y_out, dx_out, gain_out, qn_out, kn_out,
                  wqkv_s, n_s, dy_s, nt_s, hid_s, dg_s, du_s, st_g, st_u, st_d, got_s, of_s, df_s, kf_s, vf_s, wq_s, wk_s, wv_s, wo_s, small_s,
                  load_sem, tile_sem, ring_send, ring_recv, pair_send, pair_recv, out_sem, kv_sem,
                  put_sem, swap_send, swap_recv, rows_send, rows_recv, small_send, small_recv):
    ring = Ring(devices)
    lane = (wqkv_s, (ring_send, ring_recv, pair_send, pair_recv), 4)
    model_dim = n_ref.shape[1]
    local_len, head_dim = o_ref.shape[1:]
    half = hid_ref.shape[1]
    tile = st_g.shape[2]
    tiles = half // tile
    num_kv = kn_out.shape[0]
    share = devices // num_kv
    loads = [pltpu.make_async_copy(dwqkv_ref, wqkv_s.at[ring.me], load_sem.at[0]),
             pltpu.make_async_copy(rows_ref.at[ring.me], got_s.at[ring.me], load_sem.at[1]),
             pltpu.make_async_copy(n_ref, n_s, load_sem.at[2]),
             pltpu.make_async_copy(dy_ref, dy_s, load_sem.at[3])]
    late = [pltpu.make_async_copy(src, dst, load_sem.at[4 + i])
            for i, (src, dst) in enumerate(((wo_ref, wo_s), (wq_ref, wq_s), (wk_ref, wk_s), (wv_ref, wv_s)))]
    tile_bufs = ((hid_ref, hid_s), (dg_ref, dg_s), (du_ref, du_s))

    def fetch(i, t):
        cols = pl.ds(pl.multiple_of(t * tile, tile), tile)
        return pltpu.make_async_copy(tile_bufs[i][0].at[:, cols], tile_bufs[i][1].at[t % 2], tile_sem.at[i, t % 2])

    for copy in loads:
        copy.start()
    for i in range(3):
        fetch(i, 0).start()
    ring.barrier_all()
    loads[0].wait()

    def rows_copy(hop):
        return ring.direct(rows_ref.at[ring.peer(hop)], got_s.at[ring.me], rows_send, rows_recv, hop)

    def rows_from(hop):
        source = lax.rem(ring.me + devices - hop, devices)
        return ring.direct(rows_ref.at[source], got_s.at[source], rows_send, rows_recv, hop)

    def small_copy(hop):
        return ring.direct(small_s.at[ring.me], small_s.at[ring.me], small_send, small_recv, hop)

    def small_from(hop):
        source = lax.rem(ring.me + devices - hop, devices)
        return ring.direct(small_s.at[source], small_s.at[source], small_send, small_recv, hop)

    def each_peer(body):
        def step(hop, carry):
            body(hop)
            return carry
        lax.fori_loop(1, devices, step, 0)

    def put_q(slot):
        cols = pl.ds(pl.multiple_of(slot * head_dim, head_dim), head_dim)
        return pltpu.make_async_copy(wqkv_s.at[slot, :, pl.ds(0, head_dim)], q_out.at[:, cols], out_sem.at[slot])

    def put_kv(slot, out):
        cols = pl.ds(pl.multiple_of(slot // share * head_dim, head_dim), head_dim)
        return pltpu.make_async_copy(wqkv_s.at[slot, :, pl.ds(head_dim, head_dim)], out.at[:, cols], kv_sem.at[slot])

    def store(t, i, core):
        st, out = ((st_g, g_out), (st_u, u_out), (st_d, d_out))[i]
        span = pl.ds(pl.multiple_of(core * half + t * tile, tile), tile)
        return st.at[t], (out.at[span, :] if i == 2 else out.at[:, span])

    def put_tile(t, i):
        src, dst = store(t, i, ring.core)
        return pltpu.make_async_copy(src, dst, put_sem.at[i, t])

    def send_tile(t, i, core):
        src, dst = store(t, i, core)
        return pltpu.make_async_remote_copy(src, dst, swap_send.at[i, t], swap_recv.at[i, t],
                                            device_id={'sp': ring.partner}, device_id_type=MESH)

    def finish_forward():
        late[0].wait()
        for h in range(devices):
            of_s[:, h * head_dim:(h + 1) * head_dim] = o_ref[h]
        attn_out = jnp.dot(of_s[...], wo_s[...], preferred_element_type=F32).astype(BF16)
        y_out[...] = (x_ref[...].astype(F32) + attn_out.astype(F32) + mlp_ref[...].astype(F32)).astype(BF16)

    def finish_backward():
        each_peer(lambda hop: rows_from(hop).wait_recv())
        loads[1].wait()
        for h in range(devices):
            df_s[:, h * head_dim:(h + 1) * head_dim] = got_s[h, :, :head_dim]
        for j in range(num_kv):
            kf_s[:, j * head_dim:(j + 1) * head_dim] = got_s[share * j, :, head_dim:]
            vf_s[:, j * head_dim:(j + 1) * head_dim] = got_s[share * j + 1, :, head_dim:]
        for copy in late[1:]:
            copy.wait()
        d_norm = (times_transposed(df_s[...], wq_s[...]) + times_transposed(kf_s[...], wk_s[...])
                  + times_transposed(vf_s[...], wv_s[...]) + dn_ref[...]).astype(BF16).astype(F32)
        unit, inv_std = head_stats(x_ref[...].astype(F32))
        grad_gain = jnp.sum(d_norm * unit, axis=0, keepdims=True)
        d_unit = d_norm * gain_ref[...]
        mean_d = jnp.mean(d_unit, axis=-1, keepdims=True)
        mean_du = jnp.mean(d_unit * unit, axis=-1, keepdims=True)
        dx = inv_std * (d_unit - mean_d - unit * mean_du)
        own_rows = pl.ds(pl.multiple_of(ring.me * local_len, local_len), local_len)
        dx_out[...] = (dy_s[own_rows, :].astype(F32) + dx).astype(BF16)
        gains = model_dim // head_dim
        parts = [grad_gain[:, c * head_dim:(c + 1) * head_dim] for c in range(gains)] + [gq_ref[...], gk_ref[...]]
        pad = jnp.zeros((small_s.shape[1] - len(parts), head_dim), F32)
        small_s[ring.me] = jnp.concatenate(parts + [pad], axis=0)

    def settle(step):
        ring.shared(lane, step)
        for slot in (ring.own_slot(step), ring.other_slot(step)):
            put_q(slot).start()

            @pl.when(slot % 2 == 0)
            def _():
                put_kv(slot, k_out).start()

            @pl.when(slot % 2 == 1)
            def _():
                put_kv(slot, v_out).start()

    def step_body(step, carry):
        ring.take(lane, step, (0, 1))

        @pl.when(step == 0)
        def _():
            each_peer(lambda hop: rows_copy(hop).start())
            loads[2].wait()

            def turn(i, inner):
                rows = pl.ds(pl.multiple_of(i * 256, 256), 256)
                nt_s[:, rows] = n_s[rows, :].T
                return inner
            lax.fori_loop(0, n_s.shape[0] // 256, turn, 0)
            loads[3].wait()

        piece = model_dim // 4

        @pl.when(step < tiles)
        def _():
            for i in range(3):
                fetch(i, step).wait()

            @pl.when(step + 1 < tiles)
            def _():
                for i in range(3):
                    fetch(i, step + 1).start()

            def in_weights(i, inner):
                rows = pl.ds(pl.multiple_of(i * piece, piece), piece)
                st_g[step, rows, :] = jnp.dot(nt_s[rows, :], dg_s[step % 2], preferred_element_type=F32).astype(BF16)
                st_u[step, rows, :] = jnp.dot(nt_s[rows, :], du_s[step % 2], preferred_element_type=F32).astype(BF16)
                return inner
            lax.fori_loop(0, 4, in_weights, 0)

        ring.take(lane, step, (2, 3))

        @pl.when(step < tiles)
        def _():
            st_d[step] = transposed_times(hid_s[step % 2], dy_s[...]).astype(BF16)

        @pl.when(step == 1)
        def _():
            for copy in late:
                copy.start()

        @pl.when(step == tiles)
        def _():
            finish_forward()

        @pl.when(step == tiles + 1)
        def _():
            finish_backward()

        @pl.when(step > 0)
        def _():
            settle(step - 1)

        @pl.when(jnp.logical_and(step > 0, step <= tiles))
        def _():
            for i in range(3):
                put_tile(step - 1, i).start()
                send_tile(step - 1, i, ring.core).start()
        return carry

    lax.fori_loop(0, ring.chips, step_body, 0)
    each_peer(lambda hop: small_copy(hop).start())
    settle(ring.chips - 1)
    ring.finish(lane)

    def drain(slot, carry):
        put_q(slot).wait()
        put_kv(slot, k_out).wait()
        return carry
    lax.fori_loop(0, devices, drain, 0)

    def drain_tiles(t, carry):
        for i in range(3):
            put_tile(t, i).wait()
            send_tile(t, i, ring.core).wait_send()
            send_tile(t, i, 1 - ring.core).wait_recv()
        return carry
    lax.fori_loop(0, tiles, drain_tiles, 0)
    each_peer(lambda hop: rows_copy(hop).wait_send())
    each_peer(lambda hop: small_from(hop).wait_recv())
    each_peer(lambda hop: small_copy(hop).wait_send())
    gains = model_dim // head_dim
    total = small_s[0, :gains]
    for h in range(1, devices):
        total = total + small_s[h, :gains]
    gain_out[...] = total
    qn_out[...] = jnp.concatenate([small_s[h, gains:gains + 1] for h in range(devices)], axis=0)
    kn_out[...] = jnp.concatenate([small_s[share * j, gains + 1:gains + 2] for j in range(num_kv)], axis=0)


def whole(shape):
    return pl.BlockSpec(shape, lambda *_: (0,) * len(shape))


def solution(mesh):
    group_devices = mesh.shape['sp']
    seq_spec = P('dp', 'sp', None)
    grad_spec = P('dp', None)
    def layer_step(x_in, grad_y, positions, w_q, w_k, w_v, w_o, w_gate, w_up, w_down, norm_gain, q_norm, k_norm):
        batch_rows, local_len, model_dim = x_in.shape
        num_heads, head_dim = q_norm.shape
        num_kv = k_norm.shape[0]
        share = num_heads // num_kv
        ffn_dim = w_gate.shape[1]
        seq_len = local_len * group_devices
        me = lax.axis_index('sp')
        idx = jnp.stack([me, me // share, me % 2]).astype(jnp.int32)
        params = pltpu.CompilerParams(vmem_limit_bytes=VMEM_LIMIT)
        hbm = pl.BlockSpec(memory_space=pl.ANY)

        def call(kernel, name, flops, bytes_accessed, grid, in_specs, out_specs, out_shape, scratch, aliases=None):
            return pl.pallas_call(
                kernel, out_shape=out_shape, name=name, compiler_params=params, input_output_aliases=aliases or {},
                cost_estimate=pl.CostEstimate(flops=flops, bytes_accessed=bytes_accessed, transcendentals=0),
                grid_spec=pltpu.PrefetchScalarGridSpec(num_scalar_prefetch=1, grid=grid, in_specs=in_specs, out_specs=out_specs,
                                                       scratch_shapes=scratch))

        x_rows = x_in.reshape(local_len, model_dim)
        gain_row = norm_gain.reshape(1, model_dim)
        grad_flat = grad_y.reshape(local_len, model_dim)
        half = ffn_dim // 2
        dma = pltpu.SemaphoreType.DMA
        chips = group_devices // 2
        ring_sems = lambda lanes: [dma((lanes, chips))] * 4
        struct = jax.ShapeDtypeStruct
        vmem = pltpu.VMEM
        in_vmem = pl.BlockSpec(memory_space=pltpu.VMEM)
        acts = (group_devices, local_len, half)
        blocks = (group_devices, local_len, model_dim)
        pos_rows = jnp.broadcast_to(positions.reshape(1, local_len), (8, local_len))
        freq, sign = rope_lanes(head_dim)
        rope = struct((group_devices, local_len, head_dim), F32)
        n_all, dy_all, cos_t, sin_t, hid, d_gate, d_up, mlp_out, d_norm_mlp = pl.pallas_call(
            functools.partial(gather_kernel, group_devices), name="gather_tokens",
            out_shape=[struct(blocks, BF16), struct(blocks, BF16), rope, rope]
            + [struct(acts, BF16)] * 3 + [struct((local_len, model_dim), BF16), struct((local_len, model_dim), F32)],
            in_specs=[in_vmem] * 4 + [hbm] * 5, out_specs=[hbm] * 2 + [in_vmem] * 2 + [hbm] * 3 + [in_vmem] * 2,
            scratch_shapes=[vmem(blocks, BF16), vmem(blocks, BF16), vmem((group_devices, 8, local_len), jnp.int32),
                            vmem((model_dim, half), BF16), vmem((model_dim, half), BF16), vmem((half, model_dim), BF16)]
            + [vmem(acts, BF16)] * 3 + [vmem((2 * local_len, half), F32)] * 2 + [vmem((2, local_len, model_dim), F32)] * 3
            + [dma((3,)), dma((3,))] + ring_sems(1) + ring_sems(2) * 2 + [dma((3, group_devices)), dma((3, group_devices)), dma(()), dma(())],
            compiler_params=pltpu.CompilerParams(collective_id=0, has_side_effects=True, vmem_limit_bytes=VMEM_LIMIT),
            cost_estimate=pl.CostEstimate(flops=40_000_000_000, bytes_accessed=40_000_000, transcendentals=0),
        )(x_rows, gain_row, freq, sign, grad_flat, pos_rows, w_gate, w_up, w_down)
        n_all, dy_all = n_all.reshape(seq_len, model_dim), dy_all.reshape(seq_len, model_dim)
        hid, d_gate, d_up = (act.reshape(seq_len, half) for act in (hid, d_gate, d_up))
        cos_t, sin_t = cos_t.reshape(seq_len, head_dim), sin_t.reshape(seq_len, head_dim)

        vec = jax.ShapeDtypeStruct((1, head_dim), F32)
        rows_bf = jax.ShapeDtypeStruct((seq_len, head_dim), BF16)
        rows_f32 = jax.ShapeDtypeStruct((seq_len, head_dim), F32)
        rows = whole((seq_len, head_dim))
        head_cols = pl.BlockSpec((model_dim, head_dim), lambda g, s: (0, s[0]))
        kv_cols = pl.BlockSpec((model_dim, head_dim), lambda g, s: (0, s[1]))
        head_rows = pl.BlockSpec((head_dim, model_dim), lambda g, s: (s[0], 0))
        head_vec = pl.BlockSpec((1, 1, head_dim), lambda g, s: (s[0], 0, 0))
        kv_vec = pl.BlockSpec((1, 1, head_dim), lambda g, s: (s[1], 0, 0))
        tokens = whole((seq_len, model_dim))
        block = 512
        qn3 = q_norm.reshape(num_heads, 1, head_dim)
        kn3 = k_norm.reshape(num_kv, 1, head_dim)

        o_h, o32, lse, q_rot, k_rot, v_h, q_proj, k_proj = call(
            functools.partial(forward_kernel, block), "attention_fwd", 10_000_000_000, 12_000_000, (1,),
            [tokens, head_cols, kv_cols, kv_cols, head_vec, kv_vec, rows, rows], [rows] * 8,
            [rows_bf, rows_f32, rows_f32] + [rows_bf] * 5, [pltpu.VMEM((block, seq_len), F32)],
        )(idx, n_all, w_q, w_k, w_v, qn3, kn3, cos_t, sin_t)

        heads = struct((group_devices, local_len, head_dim), BF16)
        d_rows, dwqkv_h, dw_o, attn_own, gq, gk = pl.pallas_call(
            functools.partial(backward_kernel, group_devices, block), name="attention_bwd",
            out_shape=[struct((seq_len, 2 * head_dim), BF16), struct((model_dim, 2 * head_dim), BF16), struct(w_o.shape, BF16), heads, vec, vec],
            in_specs=[hbm] * 3 + [in_vmem] * 12, out_specs=[hbm, in_vmem, hbm, hbm, in_vmem, in_vmem],
            scratch_shapes=[vmem((seq_len, model_dim), BF16)] * 2 + [vmem((head_dim, model_dim), BF16), vmem((group_devices, head_dim, model_dim), BF16)]
            + [vmem((seq_len, head_dim), BF16)] + [vmem((seq_len, head_dim), F32)] * 2 + [vmem((seq_len, head_dim), BF16)] * 2
            + [vmem((seq_len, 2 * head_dim), BF16), vmem(heads.shape, BF16), dma((5,))] + ring_sems(4) + [dma((group_devices,)), dma(()), dma(())] + [dma((group_devices,))] * 2,
            compiler_params=pltpu.CompilerParams(collective_id=2, has_side_effects=True, vmem_limit_bytes=VMEM_LIMIT),
            cost_estimate=pl.CostEstimate(flops=30_000_000_000, bytes_accessed=30_000_000, transcendentals=0),
        )(dy_all, n_all, w_o, o_h, o32, lse, q_rot, k_rot, v_h, q_proj, k_proj, qn3, kn3, cos_t, sin_t)

        tile = 256
        tiles = half // tile
        tile_in = (tiles, model_dim, tile)
        gain_shape = (model_dim // head_dim, head_dim)
        flat = (local_len, num_heads * head_dim)
        flat_kv = (local_len, num_kv * head_dim)
        dw_q, dw_k, dw_v, dw_gate, dw_up, dw_down, y_out, grad_x, grad_gain, grad_q_norm, grad_k_norm = pl.pallas_call(
            functools.partial(weight_kernel, group_devices), name="gather_weights",
            out_shape=[struct(w.shape, BF16) for w in (w_q, w_k, w_v, w_gate, w_up, w_down)]
            + [struct((local_len, model_dim), BF16)] * 2 + [struct(gain_shape, F32), struct(q_norm.shape, F32), struct(k_norm.shape, F32)],
            in_specs=[hbm, hbm, in_vmem] + [hbm] * 9 + [in_vmem] * 6, out_specs=[hbm] * 6 + [in_vmem] * 5,
            scratch_shapes=[vmem((group_devices, model_dim, 2 * head_dim), BF16),
                            vmem((seq_len, model_dim), BF16), vmem((seq_len, model_dim), BF16), vmem((model_dim, seq_len), BF16)]
            + [vmem((2, seq_len, tile), BF16)] * 3 + [vmem(tile_in, BF16), vmem(tile_in, BF16), vmem((tiles, tile, model_dim), BF16)]
            + [vmem((group_devices, local_len, 2 * head_dim), BF16), vmem(flat, BF16), vmem(flat, BF16), vmem(flat_kv, BF16), vmem(flat_kv, BF16)]
            + [vmem(w.shape, BF16) for w in (w_q, w_k, w_v, w_o)] + [vmem((group_devices, 16, head_dim), F32)]
            + [dma((8,)), dma((3, 2))] + ring_sems(4) + [dma((group_devices,))] * 2 + [dma((3, tiles))] * 3 + [dma((group_devices,))] * 4,
            compiler_params=pltpu.CompilerParams(collective_id=1, has_side_effects=True, vmem_limit_bytes=VMEM_LIMIT),
            cost_estimate=pl.CostEstimate(flops=60_000_000_000, bytes_accessed=60_000_000, transcendentals=0),
        )(dwqkv_h, d_rows.reshape(group_devices, local_len, 2 * head_dim), attn_own, n_all, dy_all, hid, d_gate, d_up,
          w_q, w_k, w_v, w_o, x_rows, gain_row, mlp_out, d_norm_mlp, gq, gk)
        grad_gain = grad_gain.reshape(model_dim)
        return (y_out.reshape(x_in.shape), grad_x.reshape(x_in.shape), dw_q, dw_k, dw_v, dw_o, dw_gate, dw_up, dw_down,
                grad_gain, grad_q_norm, grad_k_norm)

    in_specs = (seq_spec, seq_spec, P(('dp', 'sp'))) + (P(),) * 10
    out_specs = (seq_spec, seq_spec) + (grad_spec,) * 7 + (P('dp'), grad_spec, grad_spec)
    return jax.shard_map(layer_step, mesh=mesh, in_specs=in_specs, out_specs=out_specs, check_vma=False)
```

```python
import functools

import jax
import jax.numpy as jnp
from jax import lax
from jax.experimental import pallas as pl
from jax.experimental.pallas import tpu as pltpu
from jax.sharding import PartitionSpec as P

NORM_EPS = 1e-5
ROPE_THETA = 75.0e6
VMEM_LIMIT = 63 * 1024 * 1024
F32 = jnp.float32
BF16 = jnp.bfloat16
MESH = pl.DeviceIdType.MESH


def input_norm(x_f32, norm_gain):
    row_mean = jnp.mean(x_f32, axis=-1, keepdims=True)
    centered = x_f32 - row_mean
    row_var = jnp.mean(centered * centered, axis=-1, keepdims=True)
    return (centered * lax.rsqrt(row_var + NORM_EPS) * norm_gain).astype(BF16)


def swiglu(gate_pre, up_proj):
    return (jax.nn.silu(gate_pre) * up_proj).astype(BF16)


def times_transposed(lhs_mat, rhs_mat):
    return lax.dot_general(lhs_mat, rhs_mat, (((1,), (1,)), ((), ())), preferred_element_type=F32)


def transposed_times(lhs_mat, rhs_mat):
    return lax.dot_general(lhs_mat, rhs_mat, (((0,), (0,)), ((), ())), preferred_element_type=F32)


def rope_lanes(head_dim):
    pair_index = jnp.arange(head_dim, dtype=jnp.int32) // 2
    inv_freq = ROPE_THETA ** (-(pair_index.astype(F32) * 2.0) / head_dim)
    sign = jnp.where(jnp.arange(head_dim) % 2 == 0, -1.0, 1.0).astype(F32)
    return inv_freq[None, :], sign[None, :]


def swap_pairs(rows):
    lane = lax.broadcasted_iota(jnp.int32, rows.shape, 1)
    width = rows.shape[1]
    return jnp.where(lane % 2 == 0, pltpu.roll(rows, width - 1, 1), pltpu.roll(rows, 1, 1))


def head_stats(proj_f32):
    row_mean = jnp.mean(proj_f32, axis=-1, keepdims=True)
    centered = proj_f32 - row_mean
    inv_std = lax.rsqrt(jnp.mean(centered * centered, axis=-1, keepdims=True) + NORM_EPS)
    return centered * inv_std, inv_std


def head_forward(proj_f32, weight, cos_t, sin_t):
    unit, _ = head_stats(proj_f32)
    normed = unit * weight
    return (normed * cos_t + swap_pairs(normed) * sin_t).astype(BF16)


def head_backward(d_rot, proj_f32, weight, cos_t, sin_t):
    unit, inv_std = head_stats(proj_f32)
    d_normed = d_rot * cos_t + swap_pairs(d_rot * sin_t)
    d_weight = jnp.sum(d_normed * unit, axis=0, keepdims=True)
    d_unit = d_normed * weight
    mean_d = jnp.mean(d_unit, axis=-1, keepdims=True)
    mean_du = jnp.mean(d_unit * unit, axis=-1, keepdims=True)
    return inv_std * (d_unit - mean_d - unit * mean_du), d_weight


def forward_kernel(block, idx_ref, n_s, wq_ref, wk_ref, wv_ref, qn_ref, kn_ref, cos_ref, sin_ref,
                   o_ref, o32_ref, lse_ref, q_ref, k_ref, v_ref, qproj_ref, kproj_ref, e_s):
    seq_len, head_dim = o_ref.shape
    steps = seq_len // block
    scale = head_dim ** -0.5

    def project(i, carry):
        rows = pl.ds(pl.multiple_of(i * block, block), block)
        n_rows = n_s[rows, :]
        weights = jnp.concatenate([wq_ref[...], wk_ref[...], wv_ref[...]], axis=1)
        proj = jnp.dot(n_rows, weights, preferred_element_type=F32).astype(BF16)
        q_proj, k_proj = proj[:, :head_dim], proj[:, head_dim:2 * head_dim]
        qproj_ref[rows, :] = q_proj
        kproj_ref[rows, :] = k_proj
        v_ref[rows, :] = proj[:, 2 * head_dim:]
        cos_t, sin_t = cos_ref[rows, :], sin_ref[rows, :]
        q_ref[rows, :] = head_forward(q_proj.astype(F32), qn_ref[0], cos_t, sin_t)
        k_ref[rows, :] = head_forward(k_proj.astype(F32), kn_ref[0], cos_t, sin_t)
        return carry

    lax.fori_loop(0, steps, project, 0)
    causal = lax.broadcasted_iota(jnp.int32, (block, block), 0) >= lax.broadcasted_iota(jnp.int32, (block, block), 1)

    def lanes(op, tile):
        return functools.reduce(op, [tile[:, c:c + 128] for c in range(0, block, 128)])

    def keys_of(j):
        return pl.ds(pl.multiple_of(j * block, block), block)

    def query_block(i, carry):
        rows = keys_of(i)
        q_rows = q_ref[rows, :]

        def score(j, top):
            tile = times_transposed(q_rows, k_ref[keys_of(j), :])
            e_s[:, keys_of(j)] = tile
            return jnp.maximum(top, lanes(jnp.maximum, tile))

        top = lax.fori_loop(0, i, score, jnp.full((block, 128), -1e30, F32))
        diag = jnp.where(causal, times_transposed(q_rows, k_ref[rows, :]), -1e30)
        e_s[:, rows] = diag
        top = jnp.max(jnp.maximum(top, lanes(jnp.maximum, diag)), axis=-1, keepdims=True)

        def exponent(j, total):
            tile = jnp.exp((e_s[:, keys_of(j)] - top) * scale)
            e_s[:, keys_of(j)] = tile
            return total + lanes(jnp.add, tile)

        total = lax.fori_loop(0, i + 1, exponent, jnp.zeros((block, 128), F32))
        total = jnp.sum(total, axis=-1, keepdims=True)
        inv_total = 1.0 / total

        def attend(j, acc):
            probs = (e_s[:, keys_of(j)] * inv_total).astype(BF16)
            return acc + jnp.dot(probs, v_ref[keys_of(j), :], preferred_element_type=F32)

        out = lax.fori_loop(0, i + 1, attend, jnp.zeros((block, head_dim), F32))
        o_ref[rows, :] = out.astype(BF16)
        o32_ref[rows, :] = out
        lse_ref[rows, :] = jnp.broadcast_to(top * scale + jnp.log(total), (block, 128))
        return carry

    lax.fori_loop(0, steps, query_block, 0)


class Ring:
    def __init__(self, devices):
        self.chips = devices // 2
        self.me = lax.axis_index('sp')
        self.z, self.core = self.me // 2, self.me % 2
        self.turn = 1 - 2 * self.core
        self.partner = self.me + self.turn
        self.after = self.device(self.z + self.turn, self.core)
        self.before = self.device(self.z - self.turn, self.core)

    def device(self, z, core):
        return 2 * lax.rem(z + 2 * self.chips, self.chips) + core

    def way(self, k):
        return self.turn if k % 2 == 0 else -self.turn

    def own_slot(self, step, k):
        return self.device(self.z - self.way(k) * step, self.core)

    def other_slot(self, step, k):
        return self.device(self.z + self.way(k) * step, 1 - self.core)

    def slots(self, step, k):
        return self.own_slot(step, k), self.other_slot(step, k)

    def barrier(self):
        sem = pltpu.get_barrier_semaphore()
        for device in (self.after, self.before, self.partner):
            pl.semaphore_signal(sem, inc=1, device_id={'sp': device}, device_id_type=MESH)
        pl.semaphore_wait(sem, 3)

    def barrier_all(self):
        sem = pltpu.get_barrier_semaphore()

        def signal(hop, carry):
            pl.semaphore_signal(sem, inc=1, device_id={'sp': self.peer(hop)}, device_id_type=MESH)
            return carry
        lax.fori_loop(1, 2 * self.chips, signal, 0)
        pl.semaphore_wait(sem, 2 * self.chips - 1)

    def peer(self, hop):
        return lax.rem(self.me + hop, 2 * self.chips)

    def direct(self, src, dst, send, recv, hop):
        return pltpu.make_async_remote_copy(src, dst, send.at[hop], recv.at[hop],
                                            device_id={'sp': self.peer(hop)}, device_id_type=MESH)

    def part(self, buf, slot, parts, k):
        rows = buf.shape[1] // parts
        return buf.at[slot, pl.ds(k * rows, rows)]

    def forward(self, lane, k, step):
        buf, sems, parts = lane
        piece = self.part(buf, self.own_slot(step, k), parts, k)
        return pltpu.make_async_remote_copy(piece, piece, sems[0].at[k, step], sems[1].at[k, step + 1],
                                            device_id={'sp': self.device(self.z + self.way(k), self.core)}, device_id_type=MESH)

    def share(self, lane, k, step):
        buf, sems, parts = lane
        piece = self.part(buf, self.own_slot(step, k), parts, k)
        return pltpu.make_async_remote_copy(piece, piece, sems[2].at[k, step], sems[3].at[k, step],
                                            device_id={'sp': self.partner}, device_id_type=MESH)

    def arrived(self, lane, k, step):
        buf, sems, parts = lane
        piece = self.part(buf, self.own_slot(step, k), parts, k)
        return pltpu.make_async_remote_copy(piece, piece, sems[0].at[k, step], sems[1].at[k, step],
                                            device_id={'sp': self.before}, device_id_type=MESH)

    def shared(self, lane, step):
        buf, sems, parts = lane
        for k in range(parts):
            piece = self.part(buf, self.other_slot(step, k), parts, k)
            pltpu.make_async_remote_copy(piece, piece, sems[2].at[k, step], sems[3].at[k, step],
                                         device_id={'sp': self.partner}, device_id_type=MESH).wait_recv()

    def take(self, lane, step, ks=None):
        for k in range(lane[2]) if ks is None else ks:
            @pl.when(step > 0)
            def _():
                self.arrived(lane, k, step).wait_recv()

            @pl.when(step < self.chips - 1)
            def _():
                self.forward(lane, k, step).start()
            self.share(lane, k, step).start()

    def finish(self, lane):
        def body(step, carry):
            for k in range(lane[2]):
                @pl.when(step < self.chips - 1)
                def _():
                    self.forward(lane, k, step).wait_send()
                self.share(lane, k, step).wait_send()
            return carry
        lax.fori_loop(0, self.chips, body, 0)


def gather_kernel(devices, x_ref, gain_ref, freq_ref, sign_ref, dy_ref, pos_ref, wg_ref, wu_ref, wd_ref,
                  n_out, dy_out, cos_out, sin_out, hid_out, dg_out, du_out, mlp_out, dn_out,
                  n_s, dy_s, pos_s, wg_s, wu_s, wd_s, hid_s, dg_s, du_s, gate_s, up_s, part_s, got_s, mine_s,
                  load_sem, weight_sem, *sem_refs):
    ring = Ring(devices)
    out_sem, act_sem, swap_send, swap_recv = sem_refs[12:]
    p_lane, n_lane, dy_lane = ((buf, sem_refs[4 * i:4 * i + 4], parts) for i, (buf, parts) in enumerate(((pos_s, 1), (n_s, 2), (dy_s, 2))))
    half = wg_s.shape[1]
    lanes = ((pos_s, pos_ref, None), (n_s, None, n_out), (dy_s, dy_ref, dy_out))
    loads = [pltpu.make_async_copy(src, buf.at[ring.me], load_sem.at[i]) for i, (buf, src, _) in enumerate(lanes) if src is not None]
    columns = pl.ds(pl.multiple_of(ring.core * half, half), half)
    weights = [pltpu.make_async_copy(wg_ref.at[:, columns], wg_s, weight_sem.at[0]),
               pltpu.make_async_copy(wu_ref.at[:, columns], wu_s, weight_sem.at[1]),
               pltpu.make_async_copy(wd_ref.at[columns, :], wd_s, weight_sem.at[2])]
    for copy in loads + weights:
        copy.start()
    n_s[ring.me] = input_norm(x_ref[...].astype(F32), gain_ref[...])
    ring.barrier()
    for copy in loads:
        copy.wait()

    tile = 512
    acts = ((hid_s, hid_out), (dg_s, dg_out), (du_s, du_out))

    halves = 2
    piece = n_s.shape[1] // halves

    def span(h):
        return pl.ds(h * piece, piece)

    def pieces(step):
        return [(slot, h) for h in range(halves) for slot in ring.slots(step, h)]

    def put(lane, slot, h):
        buf, _, out = lanes[lane]
        return pltpu.make_async_copy(buf.at[slot, span(h)], out.at[slot, span(h)], out_sem.at[lane, h, slot])

    def put_act(i, slot, h):
        return pltpu.make_async_copy(acts[i][0].at[slot, span(h)], acts[i][1].at[slot, span(h)], act_sem.at[i, h, slot])

    def gate_up(step):
        def body(j, inner):
            cols = pl.ds(pl.multiple_of(j * tile, tile), tile)
            n_rows = jnp.concatenate([n_s[slot, span(h)] for slot, h in pieces(step)], axis=0)
            gate_s[:, cols] = jnp.dot(n_rows, wg_s[:, cols], preferred_element_type=F32)
            up_s[:, cols] = jnp.dot(n_rows, wu_s[:, cols], preferred_element_type=F32)
            return inner
        lax.fori_loop(0, half // tile, body, 0)

    def hidden(step):
        def body(j, inner):
            cols = pl.ds(pl.multiple_of(j * tile, tile), tile)
            dy_rows = jnp.concatenate([dy_s[slot, span(h)] for slot, h in pieces(step)], axis=0)
            d_hidden = times_transposed(dy_rows, wd_s[cols, :]).astype(BF16).astype(F32)
            gate, up = gate_s[:, cols], up_s[:, cols]
            sig = jax.nn.sigmoid(gate)
            silu = gate * sig
            hid = (silu * up).astype(BF16)
            d_up = (d_hidden * silu).astype(BF16)
            d_gate = (d_hidden * up * (sig * (1.0 + gate * (1.0 - sig)))).astype(BF16)
            for buf, value in ((hid_s, hid), (dg_s, d_gate), (du_s, d_up)):
                for i, (slot, h) in enumerate(pieces(step)):
                    buf[slot, span(h), cols] = value[i * piece:(i + 1) * piece]
            return inner
        lax.fori_loop(0, half // tile, body, 0)

    def tables(step):
        for slot in ring.slots(step, 0):
            angles = pos_s[slot].astype(F32).T[:, :1] * freq_ref[...]
            cos_out[slot] = jnp.cos(angles)
            sin_out[slot] = jnp.sin(angles) * sign_ref[...]

    def put_acts(step):
        for i in range(3):
            for slot, h in pieces(step):
                put_act(i, slot, h).start()

    swap = pltpu.make_async_remote_copy(part_s, got_s, swap_send, swap_recv, device_id={'sp': ring.partner}, device_id_type=MESH)

    def own_tokens(step):
        for k, (slot, keep) in enumerate(((ring.partner, part_s), (ring.me, mine_s))):
            @pl.when(step == 3 * k + 2)
            def _():
                keep[0] = jnp.dot(hid_s[slot], wd_s[...], preferred_element_type=F32)

            @pl.when(step == 3 * k + 3)
            def _():
                keep[1] = times_transposed(dg_s[slot], wg_s[...])

            @pl.when(step == 3 * k + 4)
            def _():
                keep[1] += times_transposed(du_s[slot], wu_s[...])

        @pl.when(step == 5)
        def _():
            swap.start()

    def settle(lane, i, step):
        ring.shared(lane, step)
        for slot, h in pieces(step):
            put(i, slot, h).start()

    def step_body(step, carry):
        ring.take(n_lane, step)
        ring.take(p_lane, step)

        @pl.when(step == 1)
        def _():
            weights[0].wait()
            weights[1].wait()

        @pl.when(step > 0)
        def _():
            settle(n_lane, 1, step - 1)
            gate_up(step - 1)
            ring.shared(p_lane, step - 1)
            tables(step - 1)

        @pl.when(step > 1)
        def _():
            put_acts(step - 2)
        ring.take(dy_lane, step)

        @pl.when(step == 1)
        def _():
            weights[2].wait()

        @pl.when(step > 0)
        def _():
            settle(dy_lane, 2, step - 1)
            hidden(step - 1)
        own_tokens(step)
        return carry

    lax.fori_loop(0, ring.chips, step_body, 0)
    last = ring.chips - 1
    settle(n_lane, 1, last)
    gate_up(last)
    put_acts(last - 1)
    settle(dy_lane, 2, last)
    hidden(last)
    ring.shared(p_lane, last)
    tables(last)
    own_tokens(last + 1)
    put_acts(last)
    for lane in (p_lane, n_lane, dy_lane):
        ring.finish(lane)

    def drain(slot, carry):
        for h in range(halves):
            for lane in (1, 2):
                put(lane, slot, h).wait()
            for i in range(3):
                put_act(i, slot, h).wait()
        return carry
    lax.fori_loop(0, devices, drain, 0)
    swap.wait()
    mlp_out[...] = (mine_s[0] + got_s[0]).astype(BF16)
    dn_out[...] = mine_s[1] + got_s[1]


def backward_kernel(devices, block, dy_ref, n_ref, wo_ref, o_ref, o32_ref, lse_ref, q_ref, k_ref, v_ref, qproj_ref, kproj_ref,
                    qn_ref, kn_ref, cos_ref, sin_ref,
                    rows_out, dw_out, wo_out, own_out, gq_ref, gk_ref,
                    dy_s, n_s, w_s, wo_s, do_s, dk_s, dv_s, send_s, got_s, rows_s, own_s,
                    load_sem, ring_send, ring_recv, pair_send, pair_recv, out_sem, swap_send, swap_recv, o_send, o_recv):
    ring = Ring(devices)
    lane = (wo_s, (ring_send, ring_recv, pair_send, pair_recv), 4)
    seq_len, head_dim = do_s.shape
    steps = seq_len // block
    scale = head_dim ** -0.5
    share = devices // kn_ref.shape[0]
    w_rows = pl.ds(pl.multiple_of(ring.me * head_dim, head_dim), head_dim)
    loads = [pltpu.make_async_copy(dy_ref, dy_s, load_sem.at[0]), pltpu.make_async_copy(wo_ref.at[w_rows, :], w_s, load_sem.at[1]),
             pltpu.make_async_copy(n_ref, n_s, load_sem.at[2])]
    for copy in loads:
        copy.start()
    ring.barrier_all()
    local_len = seq_len // devices

    def tokens_of(device):
        return pl.ds(pl.multiple_of(device * local_len, local_len), local_len)

    def o_copy(hop):
        return ring.direct(o_ref.at[tokens_of(ring.peer(hop)), :], own_s.at[ring.me], o_send, o_recv, hop)

    def o_from(hop):
        source = lax.rem(ring.me + devices - hop, devices)
        return ring.direct(o_ref.at[tokens_of(source), :], own_s.at[source], o_send, o_recv, hop)

    def each_peer(body):
        def step(hop, carry):
            body(hop)
            return carry
        lax.fori_loop(1, devices, step, 0)

    each_peer(lambda hop: o_copy(hop).start())
    own_s[ring.me] = o_ref[tokens_of(ring.me), :]
    dk_s[...] = jnp.zeros_like(dk_s)
    dv_s[...] = jnp.zeros_like(dv_s)
    gq_ref[...] = jnp.zeros_like(gq_ref)
    loads[0].wait()
    wo_s[ring.me] = transposed_times(o_ref[...], dy_s[...]).astype(BF16)
    loads[1].wait()
    do_s[...] = times_transposed(dy_s[...], w_s[...]).astype(BF16)
    ring.take(lane, 0)
    causal = lax.broadcasted_iota(jnp.int32, (block, block), 0) >= lax.broadcasted_iota(jnp.int32, (block, block), 1)
    q_weight = qn_ref[ring.me]
    done = 0
    passed = 1
    for i in range(steps):
        rows = pl.ds(i * block, block)
        q_rows, do_rows = q_ref[rows, :], do_s[rows, :]
        delta = jnp.sum(o32_ref[rows, :] * do_rows.astype(F32), axis=-1, keepdims=True)
        lse = lse_ref[rows, :][:, :1]
        dq = jnp.zeros((block, head_dim), F32)
        for j in range(i + 1):
            keys = pl.ds(j * block, block)
            k_rows, v_rows = k_ref[keys, :], v_ref[keys, :]
            probs = jnp.exp(times_transposed(q_rows, k_rows) * scale - lse)
            if i == j:
                probs = jnp.where(causal, probs, 0.0)
            d_probs = times_transposed(do_rows, v_rows).astype(BF16).astype(F32)
            d_score = (probs * (d_probs - delta) * scale).astype(BF16)
            dv_s[keys, :] += transposed_times(probs.astype(BF16), do_rows)
            dk_s[keys, :] += transposed_times(d_score, q_rows)
            dq = dq + jnp.dot(d_score, k_rows, preferred_element_type=F32)
            done += 1
            if done % 2 == 0:
                ring.take(lane, passed)
                passed += 1
        dq_proj, d_weight = head_backward(dq.astype(BF16).astype(F32), qproj_ref[rows, :].astype(F32), q_weight,
                                          cos_ref[rows, :], sin_ref[rows, :])
        rows_s[rows, pl.ds(0, head_dim)] = dq_proj.astype(BF16)
        gq_ref[...] += d_weight

    @pl.when(ring.core == 0)
    def _():
        send_s[...] = dv_s[...].astype(BF16)

    @pl.when(ring.core == 1)
    def _():
        send_s[...] = dk_s[...].astype(BF16)
    swap = pltpu.make_async_remote_copy(send_s, got_s, swap_send, swap_recv, device_id={'sp': ring.partner}, device_id_type=MESH)
    swap.start()
    ring.take(lane, passed)
    passed += 1
    loads[2].wait()
    swap.wait()

    @pl.when(ring.core == 0)
    def _():
        total = (dk_s[...].astype(BF16).astype(F32) + got_s[...].astype(F32)).astype(BF16).astype(F32)
        dk_proj, d_weight = head_backward(total, kproj_ref[...].astype(F32), kn_ref[ring.me // share], cos_ref[...], sin_ref[...])
        rows_s[:, head_dim:] = dk_proj.astype(BF16)
        gk_ref[...] = d_weight

    @pl.when(ring.core == 1)
    def _():
        rows_s[:, head_dim:] = (dv_s[...].astype(BF16).astype(F32) + got_s[...].astype(F32)).astype(BF16)
        gk_ref[...] = jnp.zeros_like(gk_ref)
    ring.take(lane, passed)
    passed += 1
    put_rows = pltpu.make_async_copy(rows_s, rows_out, load_sem.at[3])
    put_rows.start()
    dw_out[...] = transposed_times(n_s[...], rows_s[...]).astype(BF16)
    while passed < ring.chips:
        ring.take(lane, passed)
        passed += 1
    each_peer(lambda hop: o_from(hop).wait_recv())
    put_own = pltpu.make_async_copy(own_s, own_out, load_sem.at[4])
    put_own.start()

    def put_o(slot, k):
        width = head_dim // lane[2]
        rows = pl.ds(pl.multiple_of(slot * head_dim + k * width, width), width)
        return pltpu.make_async_copy(wo_s.at[slot, pl.ds(k * width, width)], wo_out.at[rows, :], out_sem.at[k, slot])

    def collect(step, carry):
        ring.shared(lane, step)
        for k in range(lane[2]):
            for slot in ring.slots(step, k):
                put_o(slot, k).start()
        return carry
    lax.fori_loop(0, ring.chips, collect, 0)
    ring.finish(lane)
    each_peer(lambda hop: o_copy(hop).wait_send())

    def drain(slot, carry):
        for k in range(lane[2]):
            put_o(slot, k).wait()
        return carry
    lax.fori_loop(0, devices, drain, 0)
    put_rows.wait()
    put_own.wait()


def weight_kernel(devices, dwqkv_ref, rows_ref, o_ref, n_ref, dy_ref, hid_ref, dg_ref, du_ref, wq_ref, wk_ref, wv_ref, wo_ref,
                  x_ref, gain_ref, mlp_ref, dn_ref, gq_ref, gk_ref,
                  q_out, k_out, v_out, g_out, u_out, d_out, y_out, dx_out, gain_out, qn_out, kn_out,
                  wqkv_s, n_s, dy_s, nt_s, hid_s, dg_s, du_s, st_g, st_u, st_d, got_s, of_s, df_s, kf_s, vf_s, wq_s, wk_s, wv_s, wo_s, small_s,
                  load_sem, tile_sem, ring_send, ring_recv, pair_send, pair_recv, out_sem, kv_sem,
                  put_sem, swap_send, swap_recv, rows_send, rows_recv, small_send, small_recv):
    ring = Ring(devices)
    lane = (wqkv_s, (ring_send, ring_recv, pair_send, pair_recv), 4)
    model_dim = n_ref.shape[1]
    local_len, head_dim = o_ref.shape[1:]
    half = hid_ref.shape[1]
    tile = st_g.shape[2]
    tiles = half // tile
    num_kv = kn_out.shape[0]
    share = devices // num_kv
    loads = [pltpu.make_async_copy(dwqkv_ref, wqkv_s.at[ring.me], load_sem.at[0]),
             pltpu.make_async_copy(rows_ref.at[ring.me], got_s.at[ring.me], load_sem.at[1]),
             pltpu.make_async_copy(n_ref, n_s, load_sem.at[2]),
             pltpu.make_async_copy(dy_ref, dy_s, load_sem.at[3])]
    late = [pltpu.make_async_copy(src, dst, load_sem.at[4 + i])
            for i, (src, dst) in enumerate(((wo_ref, wo_s), (wq_ref, wq_s), (wk_ref, wk_s), (wv_ref, wv_s)))]
    tile_bufs = ((hid_ref, hid_s), (dg_ref, dg_s), (du_ref, du_s))

    def fetch(i, t):
        cols = pl.ds(pl.multiple_of(t * tile, tile), tile)
        return pltpu.make_async_copy(tile_bufs[i][0].at[:, cols], tile_bufs[i][1].at[t % 2], tile_sem.at[i, t % 2])

    for copy in loads:
        copy.start()
    for i in range(3):
        fetch(i, 0).start()
    ring.barrier_all()
    loads[0].wait()

    def rows_copy(hop):
        return ring.direct(rows_ref.at[ring.peer(hop)], got_s.at[ring.me], rows_send, rows_recv, hop)

    def rows_from(hop):
        source = lax.rem(ring.me + devices - hop, devices)
        return ring.direct(rows_ref.at[source], got_s.at[source], rows_send, rows_recv, hop)

    def small_copy(hop):
        return ring.direct(small_s.at[ring.me], small_s.at[ring.me], small_send, small_recv, hop)

    def small_from(hop):
        source = lax.rem(ring.me + devices - hop, devices)
        return ring.direct(small_s.at[source], small_s.at[source], small_send, small_recv, hop)

    def each_peer(body):
        def step(hop, carry):
            body(hop)
            return carry
        lax.fori_loop(1, devices, step, 0)

    def part_rows(k):
        return pl.ds(k * (model_dim // lane[2]), model_dim // lane[2])

    def put_q(slot, k):
        cols = pl.ds(pl.multiple_of(slot * head_dim, head_dim), head_dim)
        return pltpu.make_async_copy(wqkv_s.at[slot, part_rows(k), pl.ds(0, head_dim)], q_out.at[part_rows(k), cols], out_sem.at[k, slot])

    def put_kv(slot, k, out):
        cols = pl.ds(pl.multiple_of(slot // share * head_dim, head_dim), head_dim)
        return pltpu.make_async_copy(wqkv_s.at[slot, part_rows(k), pl.ds(head_dim, head_dim)], out.at[part_rows(k), cols], kv_sem.at[k, slot])

    def store(t, i, core):
        st, out = ((st_g, g_out), (st_u, u_out), (st_d, d_out))[i]
        span = pl.ds(pl.multiple_of(core * half + t * tile, tile), tile)
        return st.at[t], (out.at[span, :] if i == 2 else out.at[:, span])

    def put_tile(t, i):
        src, dst = store(t, i, ring.core)
        return pltpu.make_async_copy(src, dst, put_sem.at[i, t])

    def send_tile(t, i, core):
        src, dst = store(t, i, core)
        return pltpu.make_async_remote_copy(src, dst, swap_send.at[i, t], swap_recv.at[i, t],
                                            device_id={'sp': ring.partner}, device_id_type=MESH)

    def finish_forward():
        late[0].wait()
        for h in range(devices):
            of_s[:, h * head_dim:(h + 1) * head_dim] = o_ref[h]
        attn_out = jnp.dot(of_s[...], wo_s[...], preferred_element_type=F32).astype(BF16)
        y_out[...] = (x_ref[...].astype(F32) + attn_out.astype(F32) + mlp_ref[...].astype(F32)).astype(BF16)

    def finish_backward():
        each_peer(lambda hop: rows_from(hop).wait_recv())
        loads[1].wait()
        for h in range(devices):
            df_s[:, h * head_dim:(h + 1) * head_dim] = got_s[h, :, :head_dim]
        for j in range(num_kv):
            kf_s[:, j * head_dim:(j + 1) * head_dim] = got_s[share * j, :, head_dim:]
            vf_s[:, j * head_dim:(j + 1) * head_dim] = got_s[share * j + 1, :, head_dim:]
        for copy in late[1:]:
            copy.wait()
        d_norm = (times_transposed(df_s[...], wq_s[...]) + times_transposed(kf_s[...], wk_s[...])
                  + times_transposed(vf_s[...], wv_s[...]) + dn_ref[...]).astype(BF16).astype(F32)
        unit, inv_std = head_stats(x_ref[...].astype(F32))
        grad_gain = jnp.sum(d_norm * unit, axis=0, keepdims=True)
        d_unit = d_norm * gain_ref[...]
        mean_d = jnp.mean(d_unit, axis=-1, keepdims=True)
        mean_du = jnp.mean(d_unit * unit, axis=-1, keepdims=True)
        dx = inv_std * (d_unit - mean_d - unit * mean_du)
        own_rows = pl.ds(pl.multiple_of(ring.me * local_len, local_len), local_len)
        dx_out[...] = (dy_s[own_rows, :].astype(F32) + dx).astype(BF16)
        gains = model_dim // head_dim
        parts = [grad_gain[:, c * head_dim:(c + 1) * head_dim] for c in range(gains)] + [gq_ref[...], gk_ref[...]]
        pad = jnp.zeros((small_s.shape[1] - len(parts), head_dim), F32)
        small_s[ring.me] = jnp.concatenate(parts + [pad], axis=0)

    def settle(step):
        ring.shared(lane, step)
        for k in range(lane[2]):
            for slot in ring.slots(step, k):
                put_q(slot, k).start()

                @pl.when(slot % 2 == 0)
                def _():
                    put_kv(slot, k, k_out).start()

                @pl.when(slot % 2 == 1)
                def _():
                    put_kv(slot, k, v_out).start()

    def step_body(step, carry):
        ring.take(lane, step, (0, 1))

        @pl.when(step == 0)
        def _():
            each_peer(lambda hop: rows_copy(hop).start())
            loads[2].wait()

            def turn(i, inner):
                rows = pl.ds(pl.multiple_of(i * 256, 256), 256)
                nt_s[:, rows] = n_s[rows, :].T
                return inner
            lax.fori_loop(0, n_s.shape[0] // 256, turn, 0)
            loads[3].wait()

        piece = model_dim // 4

        @pl.when(step < tiles)
        def _():
            for i in range(3):
                fetch(i, step).wait()

            @pl.when(step + 1 < tiles)
            def _():
                for i in range(3):
                    fetch(i, step + 1).start()

            def in_weights(i, inner):
                rows = pl.ds(pl.multiple_of(i * piece, piece), piece)
                st_g[step, rows, :] = jnp.dot(nt_s[rows, :], dg_s[step % 2], preferred_element_type=F32).astype(BF16)
                st_u[step, rows, :] = jnp.dot(nt_s[rows, :], du_s[step % 2], preferred_element_type=F32).astype(BF16)
                return inner
            lax.fori_loop(0, 4, in_weights, 0)

        ring.take(lane, step, (2, 3))

        @pl.when(step < tiles)
        def _():
            st_d[step] = transposed_times(hid_s[step % 2], dy_s[...]).astype(BF16)

        @pl.when(step == 1)
        def _():
            for copy in late:
                copy.start()

        @pl.when(step == tiles)
        def _():
            finish_forward()

        @pl.when(step == tiles + 1)
        def _():
            finish_backward()

        @pl.when(step > 0)
        def _():
            settle(step - 1)

        @pl.when(jnp.logical_and(step > 0, step <= tiles))
        def _():
            for i in range(3):
                put_tile(step - 1, i).start()
                send_tile(step - 1, i, ring.core).start()
        return carry

    lax.fori_loop(0, ring.chips, step_body, 0)
    each_peer(lambda hop: small_copy(hop).start())
    settle(ring.chips - 1)
    ring.finish(lane)

    def drain(slot, carry):
        for k in range(lane[2]):
            put_q(slot, k).wait()
            put_kv(slot, k, k_out).wait()
        return carry
    lax.fori_loop(0, devices, drain, 0)

    def drain_tiles(t, carry):
        for i in range(3):
            put_tile(t, i).wait()
            send_tile(t, i, ring.core).wait_send()
            send_tile(t, i, 1 - ring.core).wait_recv()
        return carry
    lax.fori_loop(0, tiles, drain_tiles, 0)
    each_peer(lambda hop: rows_copy(hop).wait_send())
    each_peer(lambda hop: small_from(hop).wait_recv())
    each_peer(lambda hop: small_copy(hop).wait_send())
    gains = model_dim // head_dim
    total = small_s[0, :gains]
    for h in range(1, devices):
        total = total + small_s[h, :gains]
    gain_out[...] = total
    qn_out[...] = jnp.concatenate([small_s[h, gains:gains + 1] for h in range(devices)], axis=0)
    kn_out[...] = jnp.concatenate([small_s[share * j, gains + 1:gains + 2] for j in range(num_kv)], axis=0)


def whole(shape):
    return pl.BlockSpec(shape, lambda *_: (0,) * len(shape))


def solution(mesh):
    group_devices = mesh.shape['sp']
    seq_spec = P('dp', 'sp', None)
    grad_spec = P('dp', None)
    def layer_step(x_in, grad_y, positions, w_q, w_k, w_v, w_o, w_gate, w_up, w_down, norm_gain, q_norm, k_norm):
        batch_rows, local_len, model_dim = x_in.shape
        num_heads, head_dim = q_norm.shape
        num_kv = k_norm.shape[0]
        share = num_heads // num_kv
        ffn_dim = w_gate.shape[1]
        seq_len = local_len * group_devices
        me = lax.axis_index('sp')
        idx = jnp.stack([me, me // share, me % 2]).astype(jnp.int32)
        params = pltpu.CompilerParams(vmem_limit_bytes=VMEM_LIMIT)
        hbm = pl.BlockSpec(memory_space=pl.ANY)

        def call(kernel, name, flops, bytes_accessed, grid, in_specs, out_specs, out_shape, scratch, aliases=None):
            return pl.pallas_call(
                kernel, out_shape=out_shape, name=name, compiler_params=params, input_output_aliases=aliases or {},
                cost_estimate=pl.CostEstimate(flops=flops, bytes_accessed=bytes_accessed, transcendentals=0),
                grid_spec=pltpu.PrefetchScalarGridSpec(num_scalar_prefetch=1, grid=grid, in_specs=in_specs, out_specs=out_specs,
                                                       scratch_shapes=scratch))

        x_rows = x_in.reshape(local_len, model_dim)
        gain_row = norm_gain.reshape(1, model_dim)
        grad_flat = grad_y.reshape(local_len, model_dim)
        half = ffn_dim // 2
        dma = pltpu.SemaphoreType.DMA
        chips = group_devices // 2
        ring_sems = lambda lanes: [dma((lanes, chips))] * 4
        struct = jax.ShapeDtypeStruct
        vmem = pltpu.VMEM
        in_vmem = pl.BlockSpec(memory_space=pltpu.VMEM)
        acts = (group_devices, local_len, half)
        blocks = (group_devices, local_len, model_dim)
        pos_rows = jnp.broadcast_to(positions.reshape(1, local_len), (8, local_len))
        freq, sign = rope_lanes(head_dim)
        rope = struct((group_devices, local_len, head_dim), F32)
        n_all, dy_all, cos_t, sin_t, hid, d_gate, d_up, mlp_out, d_norm_mlp = pl.pallas_call(
            functools.partial(gather_kernel, group_devices), name="gather_tokens",
            out_shape=[struct(blocks, BF16), struct(blocks, BF16), rope, rope]
            + [struct(acts, BF16)] * 3 + [struct((local_len, model_dim), BF16), struct((local_len, model_dim), F32)],
            in_specs=[in_vmem] * 4 + [hbm] * 5, out_specs=[hbm] * 2 + [in_vmem] * 2 + [hbm] * 3 + [in_vmem] * 2,
            scratch_shapes=[vmem(blocks, BF16), vmem(blocks, BF16), vmem((group_devices, 8, local_len), jnp.int32),
                            vmem((model_dim, half), BF16), vmem((model_dim, half), BF16), vmem((half, model_dim), BF16)]
            + [vmem(acts, BF16)] * 3 + [vmem((2 * local_len, half), F32)] * 2 + [vmem((2, local_len, model_dim), F32)] * 3
            + [dma((3,)), dma((3,))] + ring_sems(1) + ring_sems(2) * 2 + [dma((3, 2, group_devices)), dma((3, 2, group_devices)), dma(()), dma(())],
            compiler_params=pltpu.CompilerParams(collective_id=0, has_side_effects=True, vmem_limit_bytes=VMEM_LIMIT),
            cost_estimate=pl.CostEstimate(flops=40_000_000_000, bytes_accessed=40_000_000, transcendentals=0),
        )(x_rows, gain_row, freq, sign, grad_flat, pos_rows, w_gate, w_up, w_down)
        n_all, dy_all = n_all.reshape(seq_len, model_dim), dy_all.reshape(seq_len, model_dim)
        hid, d_gate, d_up = (act.reshape(seq_len, half) for act in (hid, d_gate, d_up))
        cos_t, sin_t = cos_t.reshape(seq_len, head_dim), sin_t.reshape(seq_len, head_dim)

        vec = jax.ShapeDtypeStruct((1, head_dim), F32)
        rows_bf = jax.ShapeDtypeStruct((seq_len, head_dim), BF16)
        rows_f32 = jax.ShapeDtypeStruct((seq_len, head_dim), F32)
        rows = whole((seq_len, head_dim))
        head_cols = pl.BlockSpec((model_dim, head_dim), lambda g, s: (0, s[0]))
        kv_cols = pl.BlockSpec((model_dim, head_dim), lambda g, s: (0, s[1]))
        head_rows = pl.BlockSpec((head_dim, model_dim), lambda g, s: (s[0], 0))
        head_vec = pl.BlockSpec((1, 1, head_dim), lambda g, s: (s[0], 0, 0))
        kv_vec = pl.BlockSpec((1, 1, head_dim), lambda g, s: (s[1], 0, 0))
        tokens = whole((seq_len, model_dim))
        block = 512
        qn3 = q_norm.reshape(num_heads, 1, head_dim)
        kn3 = k_norm.reshape(num_kv, 1, head_dim)

        o_h, o32, lse, q_rot, k_rot, v_h, q_proj, k_proj = call(
            functools.partial(forward_kernel, block), "attention_fwd", 10_000_000_000, 12_000_000, (1,),
            [tokens, head_cols, kv_cols, kv_cols, head_vec, kv_vec, rows, rows], [rows] * 8,
            [rows_bf, rows_f32, rows_f32] + [rows_bf] * 5, [pltpu.VMEM((block, seq_len), F32)],
        )(idx, n_all, w_q, w_k, w_v, qn3, kn3, cos_t, sin_t)

        heads = struct((group_devices, local_len, head_dim), BF16)
        d_rows, dwqkv_h, dw_o, attn_own, gq, gk = pl.pallas_call(
            functools.partial(backward_kernel, group_devices, block), name="attention_bwd",
            out_shape=[struct((seq_len, 2 * head_dim), BF16), struct((model_dim, 2 * head_dim), BF16), struct(w_o.shape, BF16), heads, vec, vec],
            in_specs=[hbm] * 3 + [in_vmem] * 12, out_specs=[hbm, in_vmem, hbm, hbm, in_vmem, in_vmem],
            scratch_shapes=[vmem((seq_len, model_dim), BF16)] * 2 + [vmem((head_dim, model_dim), BF16), vmem((group_devices, head_dim, model_dim), BF16)]
            + [vmem((seq_len, head_dim), BF16)] + [vmem((seq_len, head_dim), F32)] * 2 + [vmem((seq_len, head_dim), BF16)] * 2
            + [vmem((seq_len, 2 * head_dim), BF16), vmem(heads.shape, BF16), dma((5,))] + ring_sems(4) + [dma((4, group_devices)), dma(()), dma(())] + [dma((group_devices,))] * 2,
            compiler_params=pltpu.CompilerParams(collective_id=2, has_side_effects=True, vmem_limit_bytes=VMEM_LIMIT),
            cost_estimate=pl.CostEstimate(flops=30_000_000_000, bytes_accessed=30_000_000, transcendentals=0),
        )(dy_all, n_all, w_o, o_h, o32, lse, q_rot, k_rot, v_h, q_proj, k_proj, qn3, kn3, cos_t, sin_t)

        tile = 256
        tiles = half // tile
        tile_in = (tiles, model_dim, tile)
        gain_shape = (model_dim // head_dim, head_dim)
        flat = (local_len, num_heads * head_dim)
        flat_kv = (local_len, num_kv * head_dim)
        dw_q, dw_k, dw_v, dw_gate, dw_up, dw_down, y_out, grad_x, grad_gain, grad_q_norm, grad_k_norm = pl.pallas_call(
            functools.partial(weight_kernel, group_devices), name="gather_weights",
            out_shape=[struct(w.shape, BF16) for w in (w_q, w_k, w_v, w_gate, w_up, w_down)]
            + [struct((local_len, model_dim), BF16)] * 2 + [struct(gain_shape, F32), struct(q_norm.shape, F32), struct(k_norm.shape, F32)],
            in_specs=[hbm, hbm, in_vmem] + [hbm] * 9 + [in_vmem] * 6, out_specs=[hbm] * 6 + [in_vmem] * 5,
            scratch_shapes=[vmem((group_devices, model_dim, 2 * head_dim), BF16),
                            vmem((seq_len, model_dim), BF16), vmem((seq_len, model_dim), BF16), vmem((model_dim, seq_len), BF16)]
            + [vmem((2, seq_len, tile), BF16)] * 3 + [vmem(tile_in, BF16), vmem(tile_in, BF16), vmem((tiles, tile, model_dim), BF16)]
            + [vmem((group_devices, local_len, 2 * head_dim), BF16), vmem(flat, BF16), vmem(flat, BF16), vmem(flat_kv, BF16), vmem(flat_kv, BF16)]
            + [vmem(w.shape, BF16) for w in (w_q, w_k, w_v, w_o)] + [vmem((group_devices, 16, head_dim), F32)]
            + [dma((8,)), dma((3, 2))] + ring_sems(4) + [dma((4, group_devices))] * 2 + [dma((3, tiles))] * 3 + [dma((group_devices,))] * 4,
            compiler_params=pltpu.CompilerParams(collective_id=1, has_side_effects=True, vmem_limit_bytes=VMEM_LIMIT),
            cost_estimate=pl.CostEstimate(flops=60_000_000_000, bytes_accessed=60_000_000, transcendentals=0),
        )(dwqkv_h, d_rows.reshape(group_devices, local_len, 2 * head_dim), attn_own, n_all, dy_all, hid, d_gate, d_up,
          w_q, w_k, w_v, w_o, x_rows, gain_row, mlp_out, d_norm_mlp, gq, gk)
        grad_gain = grad_gain.reshape(model_dim)
        return (y_out.reshape(x_in.shape), grad_x.reshape(x_in.shape), dw_q, dw_k, dw_v, dw_o, dw_gate, dw_up, dw_down,
                grad_gain, grad_q_norm, grad_k_norm)

    in_specs = (seq_spec, seq_spec, P(('dp', 'sp'))) + (P(),) * 10
    out_specs = (seq_spec, seq_spec) + (grad_spec,) * 7 + (P('dp'), grad_spec, grad_spec)
    return jax.shard_map(layer_step, mesh=mesh, in_specs=in_specs, out_specs=out_specs, check_vma=False)
```
